256 devices in a mesh: dp: 4 (over y_lo, core), sp: 8 (over y_hi, x), tp: 8 (over z).
Axes of the slice: x: 4, y: 4 (y_hi: 2, y_lo: 2; y = y_hi * 2 + y_lo), z: 8, core: 2. Of those that a mesh axis runs over, the one named last changes fastest.
Arguments:
- query: bfloat16 [4, 3072, 3072], P('dp', 'sp', 'tp'), may hold values from -110 to 110
- key: bfloat16 [4, 3072, 3072], P('dp', 'sp', 'tp'), may hold values from -8 to 8
- value: bfloat16 [4, 3072, 3072], P('dp', 'sp', 'tp'), may hold values from -6 to 6
- text_key: bfloat16 [4, 256, 3072], P('dp', None, 'tp'), may hold values from -6 to 6
- text_value: bfloat16 [4, 256, 3072], P('dp', None, 'tp'), may hold values from -6 to 6
- grad_out: bfloat16 [4, 3072, 3072], P('dp', 'sp', 'tp'), may hold values from -6 to 6
- gate: bfloat16 [4, 3072], P('dp'), may hold values from 0.5 to 1.5
- out_weight: bfloat16 [3072, 3072], P('tp', 'dp'), may hold values from -0.109375 to 0.109375
- windows: int32 [8, 2], P('sp'), may hold values from 0 to 2, as said below
- tile_map: int32 [8, 1], replicated, may hold values from 0 to 2, as said below
- text_count: int32 [4], P('dp'), may hold values from 1 to 256
Outputs:
- grad_query: bfloat16 [4, 3072, 3072], P('dp', 'sp', 'tp')
- grad_key: bfloat16 [4, 3072, 3072], P('dp', 'sp', 'tp')
- grad_value: bfloat16 [4, 3072, 3072], P('dp', 'sp', 'tp')
- grad_text_key: bfloat16 [4, 256, 3072], P('dp', None, 'tp')
- grad_text_value: bfloat16 [4, 256, 3072], P('dp', None, 'tp')
- grad_weight: float32 [3072, 3072], P('tp', 'dp')
The draws below stay inside these ranges and needn't reach their ends.
Inputs may be any that keep to these rules, and one draw needn't show every extreme that they name: `tile_map`: the positions within each row are distinct. `windows`: the time reach is 0 or 1; the first tile of every time slab has time reach 1 and spatial reach 2.
All inputs are finite; a program needn't handle non-finite values.
Results may differ from the reference program's by a relative error of at most 0.024.
Values may be sent and summed in bfloat16 or wider, within the bound.
A program may use at most 64 MiB of HBM per device.

```python
import jax
import jax.numpy as jnp
from jax import lax

D = 3072
HD = 128
TILE = 384
TILES_DEV = 1
TXT = 256
VTOK = 3072
SAMPLES = 4
NTILES = 8
N_SP = 8


def base_keys(key):
    raw = jax.random.normal(jax.random.fold_in(key, 11), (SAMPLES, VTOK, D), jnp.float32)
    return jnp.clip(raw, -6.0, 6.0)


def draw_key(key, part):
    keys = base_keys(key)
    return keys.astype(jnp.bfloat16)


def draw_query(key, part):
    fresh = jnp.clip(jax.random.normal(jax.random.fold_in(key, 13), (SAMPLES, VTOK, D), jnp.float32), -6.0, 6.0)
    return fresh.astype(jnp.bfloat16)


def draw_tile_map(key, part):
    streams = jax.random.split(jax.random.fold_in(key, 21), N_SP)
    orders = jax.vmap(lambda stream: jax.random.permutation(stream, 3 * TILES_DEV)[:TILES_DEV])(streams)
    orders = orders.astype(jnp.int32)
    highest = 3 * TILES_DEV - 1
    first_row = orders[0]
    has_lowest = jnp.any(first_row == 0)
    first_row = first_row.at[0].set(jnp.where(has_lowest, first_row[0], 0))
    orders = orders.at[0].set(first_row)
    last_row = orders[N_SP - 1]
    has_highest = jnp.any(last_row == highest)
    last_row = last_row.at[0].set(jnp.where(has_highest, last_row[0], highest))
    orders = orders.at[N_SP - 1].set(last_row)
    return orders.astype(jnp.int32)


def draw_windows(key, part):
    time_reach = jax.random.randint(jax.random.fold_in(key, 31), (NTILES,), 0, 2)
    space_reach = jax.random.randint(jax.random.fold_in(key, 32), (NTILES,), 0, 3 * TILES_DEV)
    first = jnp.arange(NTILES) % TILES_DEV == 0
    time_reach = jnp.where(first, 1, time_reach)
    space_reach = jnp.where(first, 3 * TILES_DEV - 1, space_reach)
    return jnp.stack([time_reach, space_reach], axis=1).astype(jnp.int32)


def place_ends(result, stream_key, least, top_value):
    longest = result.shape.index(max(result.shape))
    spots = []
    for shift in (0, 1):
        where = [jax.random.randint(jax.random.fold_in(stream_key, axis), (), 0, length) for axis, length in enumerate(result.shape)]
        where[longest] = (where[longest] + shift) % result.shape[longest]
        spots.append(tuple(where))
    return result.at[spots[0]].set(least).at[spots[1]].set(top_value)


def steps_of(own_key, shape, cuts, low, largest):
    level = 1.0
    for position, blocks in cuts:
        steps = jax.random.uniform(jax.random.fold_in(jax.random.fold_in(own_key, 6), position), (blocks,), jnp.float32, low / len(cuts), largest / len(cuts))
        level = level * jnp.repeat(jnp.exp(steps), shape[position] // blocks).reshape((-1,) + (1,) * (len(shape) - 1 - position))
    return level


def normal_values(own_key, dims, width, most, cuts=(), held_as=jnp.bfloat16):
    values = width * jax.random.normal(own_key, dims, jnp.float32)
    if cuts:
        values = values * steps_of(own_key, dims, cuts, -0.22, 0.18)
    return jnp.clip(values, -most, most).astype(held_as)


def setup_inputs(seed: int = 0) -> dict:
    streams_of = jax.random.split(jax.random.key(seed), 12)
    return {
        "query": draw_query(jax.random.fold_in(streams_of[11], 71), 0),
        "key": draw_key(jax.random.fold_in(streams_of[11], 71), 0),
        "value": normal_values(streams_of[2], (SAMPLES, VTOK, D), 1.0, 6.0, ((0, 4), (1, 8), (2, 8))),
        "text_key": normal_values(streams_of[3], (SAMPLES, TXT, D), 1.0, 6.0, ((0, 4), (2, 8))),
        "text_value": normal_values(streams_of[4], (SAMPLES, TXT, D), 1.0, 6.0, ((0, 4), (2, 8))),
        "grad_out": normal_values(streams_of[5], (SAMPLES, VTOK, D), 1.0, 6.0, ((0, 4), (1, 8), (2, 8))),
        "gate": jnp.clip(0.5 + 1.0 * jax.random.uniform(streams_of[6], (SAMPLES, D), jnp.float32) ** steps_of(streams_of[6], (SAMPLES, D), ((0, 4),), -0.2, 0.2), 0.5, 1.5).astype(jnp.bfloat16),
        "out_weight": normal_values(streams_of[7], (D, D), D ** -0.5, 0.109375, ((0, 8), (1, 4))),
        "windows": draw_windows(jax.random.fold_in(streams_of[11], 71), 0),
        "tile_map": draw_tile_map(jax.random.fold_in(streams_of[11], 71), 0),
        "text_count": place_ends(jax.random.randint(streams_of[10], (SAMPLES,), 1, TXT + 1), jax.random.fold_in(streams_of[10], 1), 1, TXT).astype(jnp.int32),
    }


def window_mask(own_map, side_maps, valid, spans, text_live):
    reach = jnp.abs(jnp.arange(3, dtype=jnp.int32) - 1)
    near_time = reach[None, :, None] <= spans[:, 0][:, None, None]
    near_space = jnp.abs(own_map[:, None, None] - side_maps[None, :, :]) <= spans[:, 1][:, None, None]
    allowed = near_time & near_space & valid[None, :, None]
    count = own_map.shape[0]
    tiles = allowed.reshape(count, 3 * count)
    video = jnp.broadcast_to(tiles[:, None, :, None], (count, TILE, 3 * count, TILE))
    video = video.reshape(count * TILE, 3 * count * TILE)
    text = jnp.broadcast_to(text_live[None, :], (count * TILE, text_live.shape[0]))
    return jnp.concatenate([video, text], axis=1)


def tile_attention(query, keys, values, grad_attn, allowed):
    factor = HD ** -0.5
    scores = factor * jnp.dot(query, keys.T, preferred_element_type=jnp.float32)
    scores = jnp.where(allowed, scores, -1e30)
    top = jnp.max(scores, axis=1, keepdims=True)
    weights = jnp.exp(scores - top)
    weights = weights / jnp.sum(weights, axis=1, keepdims=True)
    probs = weights.astype(jnp.bfloat16)
    attended = jnp.dot(probs, values, preferred_element_type=jnp.float32).astype(jnp.bfloat16)
    delta = jnp.sum(grad_attn.astype(jnp.float32) * attended.astype(jnp.float32), axis=1, keepdims=True)
    grad_probs = jnp.dot(grad_attn, values.T, preferred_element_type=jnp.float32)
    grad_scores = (weights * (grad_probs - delta)).astype(jnp.bfloat16)
    grad_query = factor * jnp.dot(grad_scores, keys, preferred_element_type=jnp.float32)
    grad_keys = factor * jnp.dot(grad_scores.T, query, preferred_element_type=jnp.float32)
    grad_values = jnp.dot(probs.T, grad_attn, preferred_element_type=jnp.float32)
    return attended, grad_query, grad_keys, grad_values


def gather_back(parts, slabs, tok):
    video = parts[:, :3 * tok].reshape(slabs, 3, tok, HD)
    empty = jnp.zeros((1, tok, HD), jnp.float32)
    total = video[:, 1] + jnp.concatenate([video[1:, 0], empty], axis=0)
    total = total + jnp.concatenate([empty, video[:-1, 2]], axis=0)
    return total.reshape(slabs * tok, HD), jnp.sum(parts[:, 3 * tok:], axis=0)


def reference(query, key, value, text_key, text_value, grad_out, gate, out_weight, windows, tile_map, text_count):
    slabs = N_SP
    tok = TILE * TILES_DEV
    heads = D // HD
    blank = jnp.zeros((1, TILES_DEV), jnp.int32)
    padded_map = jnp.concatenate([blank, tile_map.astype(jnp.int32), blank], axis=0)
    weight_grad = jnp.zeros((D, D), jnp.float32)
    outs = [[], [], [], [], []]
    for sample in range(SAMPLES):
        scaled = (grad_out[sample].astype(jnp.float32) * gate[sample].astype(jnp.float32)[None, :]).astype(jnp.bfloat16)
        grad_attn = jnp.dot(scaled, out_weight.T, preferred_element_type=jnp.float32).astype(jnp.bfloat16)
        text_live = jnp.arange(TXT, dtype=jnp.int32) < text_count[sample]

        def one_head(head):
            start = (head * HD).astype(jnp.int32)

            def cut(array):
                return lax.dynamic_slice_in_dim(array, start, HD, 1)

            queries = cut(query[sample]).reshape(slabs, tok, HD)
            grads = cut(grad_attn).reshape(slabs, tok, HD)
            zero_slab = jnp.zeros((1, tok, HD), jnp.bfloat16)
            keys = jnp.concatenate([zero_slab, cut(key[sample]).reshape(slabs, tok, HD), zero_slab], axis=0)
            vals = jnp.concatenate([zero_slab, cut(value[sample]).reshape(slabs, tok, HD), zero_slab], axis=0)
            text_k = cut(text_key[sample])
            text_v = cut(text_value[sample])

            def one_slab(slab):
                slab = slab.astype(jnp.int32)
                near_k = lax.dynamic_slice_in_dim(keys, slab, 3, 0).reshape(3 * tok, HD)
                near_v = lax.dynamic_slice_in_dim(vals, slab, 3, 0).reshape(3 * tok, HD)
                all_k = jnp.concatenate([near_k, text_k], axis=0)
                all_v = jnp.concatenate([near_v, text_v], axis=0)
                own_map = lax.dynamic_index_in_dim(tile_map.astype(jnp.int32), slab, 0, keepdims=False)
                side_maps = lax.dynamic_slice_in_dim(padded_map, slab, 3, 0)
                others = slab + jnp.arange(3, dtype=jnp.int32) - 1
                valid = (others >= 0) & (others < slabs)
                spans = lax.dynamic_slice_in_dim(windows.astype(jnp.int32), slab * TILES_DEV, TILES_DEV, 0)
                allowed = window_mask(own_map, side_maps, valid, spans, text_live)
                qs = lax.dynamic_index_in_dim(queries, slab, 0, keepdims=False)
                gs = lax.dynamic_index_in_dim(grads, slab, 0, keepdims=False)
                return tile_attention(qs, all_k, all_v, gs, allowed)

            attended, grad_q, grad_k, grad_v = lax.map(one_slab, jnp.arange(slabs, dtype=jnp.int32))
            video_k, text_gk = gather_back(grad_k, slabs, tok)
            video_v, text_gv = gather_back(grad_v, slabs, tok)
            return attended.reshape(slabs * tok, HD), grad_q.reshape(slabs * tok, HD), video_k, video_v, text_gk, text_gv

        results = lax.map(one_head, jnp.arange(heads, dtype=jnp.int32))

        def joined(stacked):
            return jnp.transpose(stacked, (1, 0, 2)).reshape(stacked.shape[1], D)

        attended = joined(results[0])
        weight_grad = weight_grad + jnp.dot(attended.T, scaled, preferred_element_type=jnp.float32)
        for place in range(5):
            outs[place].append(joined(results[place + 1]).astype(jnp.bfloat16))
    stacked = [jnp.stack(items, axis=0) for items in outs]
    return stacked[0], stacked[1], stacked[2], stacked[3], stacked[4], weight_grad
```

```python
import functools

import jax
import jax.numpy as jnp
from jax import lax
from jax.experimental import pallas as pl
from jax.experimental.pallas import tpu as pltpu
from jax.sharding import PartitionSpec as P

HD = 128
VMEM = 67043328
MESH = pl.DeviceIdType.MESH

NT = (((1,), (1,)), ((), ()))
NN = (((1,), (0,)), ((), ()))
TN = (((0,), (0,)), ((), ()))

bf16, f32 = jnp.bfloat16, jnp.float32


def mm(a, b, dims):
    return lax.dot_general(a, b, dims, preferred_element_type=f32)


def item_k(h):
    return 3 * h


def item_v(h):
    return 3 * h + 1


def item_q(h):
    return 3 * h + 2


def kernel(
    names,
    *refs,
):
    r_ = dict(zip(names, refs, strict=True))
    q_ref, k_ref, v_ref, tk_ref, tv_ref = (r_[n] for n in ("q", "k", "v", "tk", "tv"))
    s_ref, w_ref, gate_ref, win_ref = (r_[n] for n in ("s", "w", "gate", "win"))
    map_ref, live_ref = r_["map"], r_["live"]
    keys, vals, qf, gaf = r_["keys"], r_["vals"], r_["qf"], r_["gaf"]
    st_out, st_in, dl_out, dl_in = r_["st_out"], r_["st_in"], r_["dl_out"], r_["dl_in"]
    raw, nat, w_all, acc = r_["raw"], r_["nat"], r_["w_all"], r_["acc"]
    ga_t, att_t, wts, wfar, gs_buf = r_["ga_t"], r_["att_t"], r_["wts"], r_["wfar"], r_["gs_buf"]
    parts, g1_out, g1_in = r_["parts"], r_["g1_out"], r_["g1_in"]
    gy_out, gy_in, gx_out, gx_in = r_["gy_out"], r_["gy_in"], r_["gx_out"], r_["gx_in"]
    ag_out, gfin = r_["ag_out"], r_["gfin"]
    tx_out, tx_in, tg = r_["tx_out"], r_["tx_in"], r_["tg"]
    gk_sum, gv_sum = r_["gk_sum"], r_["gv_sum"]

    factor = HD ** (-0.5)
    tok, width = q_ref.shape
    text = tk_ref.shape[0]
    heads = width // HD
    near = tok + text
    n_tp = n_sp = 8
    me_sp = lax.axis_index("sp")
    me_dp = lax.axis_index("dp")
    me_tp = lax.axis_index("tp")
    x = me_sp & 3
    yh = me_sp >> 2
    core = me_dp & 1
    yl = me_dp >> 1
    w = s_ref.shape[1]
    piece = width // n_sp
    half = width // 2
    has = [me_sp >= 1, me_sp + 1 < n_sp]
    side_sp = [me_sp - 1, me_sp + 1]

    partners = [{"tp": (me_tp + 1) & 7}, {"tp": (me_tp + 7) & 7}]
    partners += [{"dp": me_dp ^ 1}, {"dp": me_dp ^ 2}, {"dp": me_dp ^ 2, "sp": me_sp ^ 4}]
    partners += [{"sp": me_sp ^ j} for j in range(1, n_sp)]
    barrier = pltpu.get_barrier_semaphore()
    for where in partners:
        pl.semaphore_signal(barrier, inc=1, device_id=where, device_id_type=MESH)
    pl.semaphore_wait(barrier, len(partners))

    def remote(src, dst, send, recv, where):
        return pltpu.make_async_remote_copy(
            src_ref=src,
            dst_ref=dst,
            send_sem=send,
            recv_sem=recv,
            device_id=where,
            device_id_type=MESH,
        )

    chunk = tok // 2

    def crow(c):
        return pl.ds(c * chunk, chunk)

    def z_copy(up, t, c):
        r = (8 - t) % 8 if up else t
        to = (r + 7) % 8 if up else (r + 1) % 8
        src = s_ref.at[crow(c)] if t == 0 else raw.at[r, crow(c)]
        send = r_["zs"].at[0 if up else 1, t, c]
        recv = r_["zr"].at[0 if up else 1, t, c]
        where = {"tp": (me_tp + (1 if up else 7)) & 7}
        return remote(src, raw.at[to, crow(c)], send, recv, where)

    def z_exists(up, t, c):
        return t < 3 or (t == 3 and c == (0 if up else 1))

    def z_arrive(t, c):
        for up in (True, False):
            if z_exists(up, t, c):
                z_copy(up, t, c).wait_recv()
                if t < 3 and z_exists(up, t + 1, c):
                    z_copy(up, t + 1, c).start()

    def w_core():
        return remote(w_ref, w_all.at[me_dp], r_["ws"].at[0], r_["wr"].at[0], {"dp": me_dp ^ 1})

    def w_y(i):
        rows = pl.ds(i * half, half)
        where = {"dp": me_dp ^ 2, "sp": me_sp ^ (4 * i)}
        return remote(
            w_ref.at[rows], w_all.at[me_dp, rows], r_["ws"].at[1 + i], r_["wr"].at[1 + i], where
        )

    def w_fwd():
        block = w_all.at[me_dp ^ 2]
        return remote(block, block, r_["ws"].at[3], r_["wr"].at[3], {"dp": me_dp ^ 1})

    def halo(side, item):
        there = 1 - side
        region = pl.ds(near + there * tok, tok)
        if item < 3 * heads:
            h, kind = divmod(item, 3)
            c = pl.ds(h * HD, HD)
            src = (k_ref, v_ref, q_ref)[kind].at[:, c]
            dst = (keys.at[region, c], vals.at[region, c], qf.at[there, :, c])[kind]
        elif item < 4 * heads:
            c = pl.ds((item - 3 * heads) * HD, HD)
            src, dst = ga_t.at[c], gaf.at[there, c]
        elif item == 4 * heads:
            src, dst = st_out.at[side], st_in.at[there]
        else:
            src, dst = dl_out, dl_in.at[there]
        return remote(
            src, dst, r_["hs"].at[side, item], r_["hr"].at[there, item], {"sp": side_sp[side]}
        )

    def halo_start(items):
        for side in (0, 1):

            @pl.when(has[side])
            def _():
                for item in items:
                    halo(side, item).start()

    def halo_wait(side, items):
        for item in items:
            c = halo(1 - side, item)
            c.wait_recv()

    def halo_wait_both(items):
        for side in (0, 1):

            @pl.when(has[side])
            def _():
                halo_wait(side, items)

    for c in (0, 1):
        z_copy(True, 0, c).start()
        z_copy(False, 0, c).start()
    w_core().start()
    w_y(0).start()
    w_y(1).start()
    for h in range(heads):
        halo_start([item_k(h), item_v(h)])
    for h in range(heads):
        halo_start([item_q(h)])

    keys[:tok] = k_ref[...]
    keys[tok:near] = tk_ref[...]
    vals[:tok] = v_ref[...]
    vals[tok:near] = tv_ref[...]
    w_all[me_dp] = w_ref[...]
    for side in (0, 1):

        @pl.when(jnp.logical_not(has[side]))
        def _():
            region = slice(near + side * tok, near + (side + 1) * tok)
            keys[region] = jnp.zeros((tok, width), bf16)
            vals[region] = jnp.zeros((tok, width), bf16)

    def blk(r):
        return (me_tp + r) & 7

    def scale(r):
        gate = gate_ref[:, pl.ds(pl.multiple_of(blk(r) * w, HD), w)].astype(f32)
        src = s_ref[...] if r == 0 else raw[r]
        nat[r] = (src.astype(f32) * gate).astype(bf16)

    def ga_add(r, first=False):
        at = pl.multiple_of((blk(r) & 1) * w, HD)
        term = mm(w_all[blk(r) >> 1, :, pl.ds(at, w)], nat[r], NT)
        if first:
            acc[...] = term
        else:
            acc[...] += term

    place = map_ref[me_sp, 0]
    side_bias = []
    for side in (0, 1):
        other = map_ref[jnp.clip(side_sp[side], 0, n_sp - 1), 0]
        seen = (win_ref[0:1, 0:1] >= 1) & (win_ref[0:1, 1:2] >= jnp.abs(place - other))
        edge = jnp.where(has[side], 0.0, -1e30).astype(f32)
        side_bias.append(jnp.minimum(jnp.where(seen, 0.0, -1e30).astype(f32), edge))
    place_of = lax.broadcasted_iota(jnp.int32, (text, 1), 0)
    words = jnp.where(place_of < live_ref[0], 0.0, -1e30).astype(f32)
    bias_ref = r_["bias"]
    bias_ref[:tok] = jnp.zeros((tok, 1), f32)
    bias_ref[tok:near] = words
    for side in (0, 1):
        region = slice(near + side * tok, near + (side + 1) * tok)
        bias_ref[region] = jnp.broadcast_to(side_bias[side], (tok, 1))

    def cols(h):
        return slice(h * HD, (h + 1) * HD)

    def forward(h):
        c = cols(h)
        scores = factor * mm(keys[:, c], q_ref[:, c], NT) + bias_ref[...]
        top = jnp.max(scores, axis=0, keepdims=True)
        e = jnp.exp(scores - top)
        inv = 1.0 / jnp.sum(e, axis=0, keepdims=True)
        weights = e * inv
        wts[h] = weights
        att_t[c, :] = mm(vals[:, c], weights.astype(bf16), TN).astype(bf16)
        for side in (0, 1):
            st_out[side, h : h + 1, :] = top - side_bias[side]
            st_out[side, heads + h : heads + h + 1, :] = inv

    def far_weights(side, h):
        c = cols(h)
        scores = factor * mm(keys[:tok, c], qf[side, :, c], NT)
        e = jnp.exp(scores - st_in[side, h : h + 1, :])
        wfar[side, h] = e * st_in[side, heads + h : heads + h + 1, :]

    def core_owns(r):
        return ((blk(r) >> 1) & 1) == core

    def mine(r):
        return (blk(r) >> 1) == me_dp

    def core_only(r):
        return core_owns(r) & ((blk(r) >> 2) != yl)

    def s1_copy(r):
        return remote(
            g1_out.at[r], g1_in.at[r], r_["s1s"].at[r], r_["s1r"].at[r], {"dp": me_dp ^ 1}
        )

    def gy_over(r, i):
        rows = pl.ds(i * half, half)
        return remote(
            gy_out.at[r, rows],
            gy_in.at[r, yh],
            r_["gys"].at[r, i],
            r_["gyr"].at[r, yh],
            {"dp": me_dp ^ 2, "sp": x + 4 * i},
        )

    def gy_across(r):
        rows = pl.ds(pl.multiple_of((1 - yh) * half, half), half)
        return remote(
            gy_out.at[r, rows],
            gy_in.at[r, 2],
            r_["gys"].at[r, 2],
            r_["gyr"].at[r, 2],
            {"sp": me_sp ^ 4},
        )

    def gx_copy(r, j):
        rows = pl.ds(pl.multiple_of((x ^ j) * piece, piece), piece)
        return remote(
            gx_out.at[r, rows],
            gx_in.at[r, j - 1],
            r_["gxs"].at[r, j - 1],
            r_["gxr"].at[r, j - 1],
            {"sp": me_sp ^ j},
        )

    def ag_copy(r, j):
        rows = pl.ds(pl.multiple_of(me_sp * piece, piece), piece)
        return remote(
            ag_out.at[r],
            gfin.at[blk(r) & 1, rows],
            r_["ags"].at[r, j - 1],
            r_["agr"].at[r, j - 1],
            {"sp": me_sp ^ j},
        )

    def gw_part(r):
        parts[r] = mm(att_t[...], nat[r], NN)

        @pl.when(jnp.logical_not(core_owns(r)))
        def _():
            g1_out[r] = parts[r].astype(bf16)
            s1_copy(r).start()

    def gw_s1(r):
        @pl.when(core_owns(r))
        def _():
            s1_copy(r).wait_recv()
            total = parts[r] + g1_in[r].astype(f32)
            parts[r] = total
            gy_out[r] = total.astype(bf16)

        @pl.when(core_only(r))
        def _():
            gy_over(r, 0).start()
            gy_over(r, 1).start()

        @pl.when(mine(r))
        def _():
            gy_across(r).start()

    def gw_sy(r):
        @pl.when(mine(r))
        def _():
            for i in range(3):
                remote(
                    gy_out.at[r, pl.ds(0, half)],
                    gy_in.at[r, i],
                    r_["gys"].at[r, i],
                    r_["gyr"].at[r, i],
                    {"sp": me_sp ^ 4},
                ).wait_recv()
            total = parts[r, pl.ds(pl.multiple_of(yh * half, half), half), :]
            for i in range(3):
                total = total + gy_in[r, i].astype(f32)
            parts[r, :half, :] = total
            gx_out[r] = total.astype(bf16)
            for j in range(1, 4):
                gx_copy(r, j).start()

    def gw_sx(r):
        @pl.when(mine(r))
        def _():
            for j in range(1, 4):
                gx_copy(r, j).wait_recv()
            total = parts[r, pl.ds(pl.multiple_of(x * piece, piece), piece), :]
            for j in range(3):
                total = total + gx_in[r, j].astype(f32)
            ag_out[r] = total.astype(bf16)
            gfin[blk(r) & 1, pl.ds(pl.multiple_of(me_sp * piece, piece), piece), :] = total.astype(
                bf16
            )
            for j in range(1, n_sp):
                ag_copy(r, j).start()

    gw_v = r_["gw_v"]

    def gw_ag(r):
        @pl.when(mine(r))
        def _():
            for j in range(1, n_sp):
                ag_copy(r, j).wait_recv()
            at = pl.ds(pl.multiple_of((blk(r) & 1) * w, HD), w)
            gw_v[:, at] = gfin[blk(r) & 1].astype(f32)

    trow = text // n_sp

    def tx_copy(j):
        return remote(
            tx_out.at[me_sp ^ j],
            tx_in.at[j - 1],
            r_["txs"].at[j - 1],
            r_["txr"].at[j - 1],
            {"sp": me_sp ^ j},
        )

    def tg_copy(j):
        return remote(
            tg.at[me_sp],
            tg.at[me_sp],
            r_["tgs"].at[j - 1],
            r_["tgr"].at[j - 1],
            {"sp": me_sp ^ j},
        )

    gq_v, gk_v, gv_v, gtk_v, gtv_v = (r_[n] for n in ("gq_v", "gk_v", "gv_v", "gtk_v", "gtv_v"))

    def text_part(h):
        c = cols(h)
        ga = ga_t[c, :]
        wt = wts[h, tok:near, :]
        gp = mm(vals[tok:near, c], ga, NN)
        gs = (wt * (gp - dl_out[h : h + 1, :])).astype(bf16)
        gs_buf[h, tok:near, :] = gs
        gk = (factor * mm(gs, q_ref[:, c], NN)).astype(bf16)
        gv = mm(wt.astype(bf16), ga, NT).astype(bf16)
        for j in range(n_sp):
            rows = slice(j * trow, (j + 1) * trow)
            tx_out[j, :trow, c] = gk[rows]
            tx_out[j, trow:, c] = gv[rows]

    def own_part(h):
        c = cols(h)
        ga = ga_t[c, :]
        delta = dl_out[h : h + 1, :]
        for lo, hi in ((0, tok), (near, near + 2 * tok)):
            gp = mm(vals[lo:hi, c], ga, NN)
            gs_buf[h, lo:hi, :] = (wts[h, lo:hi, :] * (gp - delta)).astype(bf16)
        gq_v[:, c] = (factor * mm(keys[:, c], gs_buf[h], TN)).T.astype(bf16)
        gk_sum[:, c] = mm(gs_buf[h, :tok, :], q_ref[:, c], NN)
        gv_sum[:, c] = mm(wts[h, :tok, :].astype(bf16), ga, NT)

    def far_part(side, h):
        c = cols(h)
        ga = gaf[side, c, :]
        weights = wfar[side, h]
        gp = mm(vals[:tok, c], ga, NN)
        gs = (weights * (gp - dl_in[side, h : h + 1, :])).astype(bf16)
        gk_sum[:, c] += mm(gs, qf[side, :, c], NN)
        gv_sum[:, c] += mm(weights.astype(bf16), ga, NT)

    scale(0)
    z_arrive(0, 0)
    w_core().wait_recv()
    z_arrive(0, 1)
    w_y(0).wait_recv()
    w_y(1).wait_recv()
    w_fwd().start()
    scale(1)
    scale(7)
    halo_wait_both([item_k(0), item_v(0)])
    forward(0)
    w_fwd().wait_recv()
    ga_add(0, True)
    z_arrive(1, 0)
    halo_wait_both([item_k(1), item_v(1)])
    forward(1)
    ga_add(1)
    ga_add(7)
    z_arrive(1, 1)
    scale(2)
    scale(6)
    halo_wait_both([item_k(2), item_v(2)])
    forward(2)
    halo_start([4 * heads])
    z_arrive(2, 0)
    for r in (0, 1, 7):
        gw_part(r)
    ga_add(2)
    ga_add(6)
    for r in (0, 1, 7):
        gw_s1(r)
    for r in (2, 6):
        gw_part(r)
    z_arrive(2, 1)
    scale(3)
    scale(5)
    for r in (3, 5):
        gw_part(r)
    for r in (2, 6):
        gw_s1(r)
    ga_add(3)
    ga_add(5)
    for r in (0, 1, 7):
        gw_sy(r)
    halo_wait_both([4 * heads])
    for h in range(heads):
        halo_wait_both([item_q(h)])
        for side in (0, 1):
            pl.when(has[side])(functools.partial(far_weights, side, h))
    for r in (3, 5):
        gw_s1(r)
    for r in (2, 6):
        gw_sy(r)
    for r in (0, 1, 7):
        gw_sx(r)
    z_arrive(3, 0)
    z_arrive(3, 1)
    scale(4)
    ga_add(4)
    ga_t[...] = acc[...].astype(bf16)
    for h in range(heads):
        c = cols(h)
        dl_out[h : h + 1, :] = jnp.sum(
            ga_t[c, :].astype(f32) * att_t[c, :].astype(f32), axis=0, keepdims=True
        )
    gw_part(4)
    for h in range(heads):
        text_part(h)
    for j in range(1, n_sp):
        tx_copy(j).start()
    halo_start([4 * heads + 1] + [3 * heads + h for h in range(heads)])
    gw_s1(4)
    own_part(0)
    for r in (3, 5):
        gw_sy(r)
    for r in (2, 6):
        gw_sx(r)
    own_part(1)
    gw_sy(4)
    for r in (3, 5):
        gw_sx(r)
    own_part(2)
    gq_store = pltpu.make_async_copy(gq_v, r_["gq_out"], r_["os"].at[0])
    gq_store.start()
    for j in range(1, n_sp):
        tx_copy(j).wait_recv()
    total = tx_out[me_sp].astype(f32)
    for j in range(n_sp - 1):
        total = total + tx_in[j].astype(f32)
    tg[me_sp] = total.astype(bf16)
    for j in range(1, n_sp):
        tg_copy(j).start()
    gw_sx(4)
    for r in (0, 1, 7, 2, 6, 3, 5):
        gw_ag(r)
    halo_wait_both([4 * heads + 1])
    for h in range(heads):
        halo_wait_both([3 * heads + h])
        for side in (0, 1):
            pl.when(has[side])(functools.partial(far_part, side, h))
        c = cols(h)
        gk_v[:, c] = (factor * gk_sum[:, c]).astype(bf16)
        gv_v[:, c] = gv_sum[:, c].astype(bf16)
    stored = [
        pltpu.make_async_copy(gk_v, r_["gk_out"], r_["os"].at[1]),
        pltpu.make_async_copy(gv_v, r_["gv_out"], r_["os"].at[2]),
    ]
    for c in stored:
        c.start()
    for j in range(1, n_sp):
        remote(
            tg.at[me_sp],
            tg.at[me_sp ^ j],
            r_["tgs"].at[j - 1],
            r_["tgr"].at[j - 1],
            {"sp": me_sp ^ j},
        ).wait_recv()
    for j in range(n_sp):
        rows = slice(j * trow, (j + 1) * trow)
        gtk_v[rows] = tg[j, :trow]
        gtv_v[rows] = tg[j, trow:]
    late = [
        pltpu.make_async_copy(gtk_v, r_["gtk_out"], r_["os"].at[3]),
        pltpu.make_async_copy(gtv_v, r_["gtv_out"], r_["os"].at[4]),
    ]
    for c in late:
        c.start()
    gw_ag(4)
    gw_store = pltpu.make_async_copy(gw_v, r_["gw_out"], r_["os"].at[5])
    gw_store.start()

    for up in (True, False):
        for t in range(4):
            for c in (0, 1):
                if z_exists(up, t, c):
                    z_copy(up, t, c).wait_send()
    w_core().wait_send()
    w_y(0).wait_send()
    w_y(1).wait_send()
    w_fwd().wait_send()
    for side in (0, 1):

        @pl.when(has[side])
        def _():
            for item in range(4 * heads + 2):
                halo(side, item).wait_send()

    for r in range(n_tp):

        @pl.when(jnp.logical_not(core_owns(r)))
        def _():
            s1_copy(r).wait_send()

        @pl.when(core_only(r))
        def _():
            gy_over(r, 0).wait_send()
            gy_over(r, 1).wait_send()

        @pl.when(mine(r))
        def _():
            gy_across(r).wait_send()
            for j in range(1, 4):
                gx_copy(r, j).wait_send()
            for j in range(1, n_sp):
                ag_copy(r, j).wait_send()

    for j in range(1, n_sp):
        tx_copy(j).wait_send()
        tg_copy(j).wait_send()
    for c in [gq_store] + stored + late + [gw_store]:
        c.wait()


def call(q, k, v, tk, tv, s, w, gate, windows, tile_map, text_count):
    tok, width = q.shape
    text = tk.shape[0]
    heads = width // HD
    cols = w.shape[1]
    total = 3 * tok + text
    block = s.shape[1]
    piece, half = width // 8, width // 2
    sm = pl.BlockSpec(memory_space=pltpu.SMEM)
    vm = pl.BlockSpec(memory_space=pltpu.VMEM)
    outs = [
        ("gq", (tok, width), bf16),
        ("gk", (tok, width), bf16),
        ("gv", (tok, width), bf16),
        ("gtk", (text, width), bf16),
        ("gtv", (text, width), bf16),
        ("gw", (width, cols), f32),
    ]
    scratch = [(n + "_v", a, b) for n, a, b in outs] + [
        ("keys", (total, width), bf16),
        ("vals", (total, width), bf16),
        ("qf", (2, tok, width), bf16),
        ("gaf", (2, width, tok), bf16),
        ("st_out", (2, 8, tok), f32),
        ("st_in", (2, 8, tok), f32),
        ("dl_out", (8, tok), f32),
        ("dl_in", (2, 8, tok), f32),
        ("bias", (total, 1), f32),
        ("raw", (8, tok, block), bf16),
        ("nat", (8, tok, block), bf16),
        ("w_all", (4, width, cols), bf16),
        ("acc", (width, tok), f32),
        ("ga_t", (width, tok), bf16),
        ("att_t", (width, tok), bf16),
        ("wts", (heads, total, tok), f32),
        ("wfar", (2, heads, tok, tok), f32),
        ("gs_buf", (heads, total, tok), bf16),
        ("gk_sum", (tok, width), f32),
        ("gv_sum", (tok, width), f32),
        ("parts", (8, width, block), f32),
        ("g1_out", (8, width, block), bf16),
        ("g1_in", (8, width, block), bf16),
        ("gy_out", (8, width, block), bf16),
        ("gy_in", (8, 3, half, block), bf16),
        ("gx_out", (8, half, block), bf16),
        ("gx_in", (8, 3, piece, block), bf16),
        ("ag_out", (8, piece, block), bf16),
        ("gfin", (2, width, block), bf16),
        ("tx_out", (8, text // 4, width), bf16),
        ("tx_in", (7, text // 4, width), bf16),
        ("tg", (8, text // 4, width), bf16),
    ]
    items = 4 * heads + 2
    sems = [
        ("zs", (2, 4, 2)),
        ("zr", (2, 4, 2)),
        ("ws", (4,)),
        ("wr", (4,)),
        ("hs", (2, items)),
        ("hr", (2, items)),
        ("s1s", (8,)),
        ("s1r", (8,)),
        ("gys", (8, 3)),
        ("gyr", (8, 3)),
        ("gxs", (8, 3)),
        ("gxr", (8, 3)),
        ("ags", (8, 7)),
        ("agr", (8, 7)),
        ("txs", (7,)),
        ("txr", (7,)),
        ("tgs", (7,)),
        ("tgr", (7,)),
        ("os", (6,)),
    ]
    args = ["q", "k", "v", "tk", "tv", "s", "w", "gate", "win", "map", "live"]
    names = args + [n + "_out" for n, _, _ in outs] + [n for n, _, _ in scratch]
    names += [n for n, _ in sems]
    return pl.pallas_call(
        functools.partial(kernel, tuple(names)),
        out_shape=[jax.ShapeDtypeStruct(a, b) for _, a, b in outs],
        in_specs=[vm] * 9 + [sm] * 2,
        out_specs=[pl.BlockSpec(memory_space=pl.ANY)] * len(outs),
        scratch_shapes=[pltpu.VMEM(a, b) for _, a, b in scratch]
        + [pltpu.SemaphoreType.DMA(n) for _, n in sems],
        compiler_params=pltpu.CompilerParams(
            collective_id=0, has_side_effects=True, vmem_limit_bytes=VMEM
        ),
        name="attention_backward",
    )(q, k, v, tk, tv, s, w, gate, windows, tile_map, text_count)


def copy_kernel(n, *refs):
    srcs, dsts, held = refs[:n], refs[n : 2 * n], refs[2 * n : 3 * n]
    in_sem, out_sem = refs[3 * n :]
    loads = [pltpu.make_async_copy(srcs[i], held[i], in_sem.at[i]) for i in range(n)]
    stores = [pltpu.make_async_copy(held[i], dsts[i], out_sem.at[i]) for i in range(n)]
    for c in loads:
        c.start()
    for i in range(n):
        loads[i].wait()
        stores[i].start()
    for c in stores:
        c.wait()


def copy_call(arrays):
    n = len(arrays)
    hbm = pl.BlockSpec(memory_space=pltpu.HBM)
    return pl.pallas_call(
        functools.partial(copy_kernel, n),
        out_shape=[jax.ShapeDtypeStruct(a.shape, a.dtype) for a in arrays],
        in_specs=[hbm] * n,
        out_specs=[hbm] * n,
        scratch_shapes=[pltpu.VMEM(a.shape, a.dtype) for a in arrays]
        + [pltpu.SemaphoreType.DMA((n,))] * 2,
        compiler_params=pltpu.CompilerParams(vmem_limit_bytes=VMEM),
        name="results",
    )(*arrays)


def per_device(
    query,
    key,
    value,
    text_key,
    text_value,
    grad_out,
    gate,
    out_weight,
    windows,
    tile_map,
    text_count,
):
    outs = call(
        query[0],
        key[0],
        value[0],
        text_key[0],
        text_value[0],
        grad_out[0],
        out_weight,
        gate,
        windows,
        tile_map,
        text_count,
    )
    outs = copy_call(outs)
    return tuple(o[None] for o in outs[:5]) + (outs[5],)


def solution(mesh):
    placed = (
        P("dp", "sp", "tp"),
        P("dp", "sp", "tp"),
        P("dp", "sp", "tp"),
        P("dp", None, "tp"),
        P("dp", None, "tp"),
        P("dp", "sp", "tp"),
        P("dp", None),
        P("tp", "dp"),
        P("sp", None),
        P(),
        P("dp"),
    )
    return jax.shard_map(
        per_device,
        mesh=mesh,
        in_specs=placed,
        out_specs=(
            P("dp", "sp", "tp"),
            P("dp", "sp", "tp"),
            P("dp", "sp", "tp"),
            P("dp", None, "tp"),
            P("dp", None, "tp"),
            P("tp", "dp"),
        ),
        check_vma=False,
    )
```

```python
import functools

import jax
import jax.numpy as jnp
from jax import lax
from jax.experimental import pallas as pl
from jax.experimental.pallas import tpu as pltpu
from jax.sharding import PartitionSpec as P

HD = 128
VMEM = 67043328
MESH = pl.DeviceIdType.MESH

NT = (((1,), (1,)), ((), ()))
NN = (((1,), (0,)), ((), ()))
TN = (((0,), (0,)), ((), ()))

bf16, f32 = jnp.bfloat16, jnp.float32


def mm(a, b, dims):
    return lax.dot_general(a, b, dims, preferred_element_type=f32)


def item_k(h):
    return 3 * h


def item_v(h):
    return 3 * h + 1


def item_q(h):
    return 3 * h + 2


def kernel(
    names,
    *refs,
):
    r_ = dict(zip(names, refs, strict=True))
    q_ref, k_ref, v_ref, tk_ref, tv_ref = (r_[n] for n in ("q", "k", "v", "tk", "tv"))
    s_ref, w_ref, gate_ref, win_ref = (r_[n] for n in ("s", "w", "gate", "win"))
    map_ref, live_ref = r_["map"], r_["live"]
    keys, vals, qf, gaf = r_["keys"], r_["vals"], r_["qf"], r_["gaf"]
    st_out, st_in, dl_out, dl_in = r_["st_out"], r_["st_in"], r_["dl_out"], r_["dl_in"]
    raw, nat, w_all, acc = r_["raw"], r_["nat"], r_["w_all"], r_["acc"]
    ga_t, att_t, wts, wfar, gs_buf = r_["ga_t"], r_["att_t"], r_["wts"], r_["wfar"], r_["gs_buf"]
    parts, g1_out, g1_in = r_["parts"], r_["g1_out"], r_["g1_in"]
    gy_out, gy_in, gx_out, gx_in = r_["gy_out"], r_["gy_in"], r_["gx_out"], r_["gx_in"]
    fin_out, gfin = r_["fin_out"], r_["gfin"]
    tx_out, tx_in, tg = r_["tx_out"], r_["tx_in"], r_["tg"]
    gk_sum, gv_sum = r_["gk_sum"], r_["gv_sum"]

    factor = HD ** (-0.5)
    tok, width = q_ref.shape
    text = tk_ref.shape[0]
    heads = width // HD
    near = tok + text
    n_tp = n_sp = 8
    me_sp = lax.axis_index("sp")
    me_dp = lax.axis_index("dp")
    me_tp = lax.axis_index("tp")
    x = me_sp & 3
    yh = me_sp >> 2
    core = me_dp & 1
    yl = me_dp >> 1
    w = s_ref.shape[1]
    piece = width // 16
    y = 2 * yh + yl
    half = width // 2
    has = [me_sp >= 1, me_sp + 1 < n_sp]
    side_sp = [me_sp - 1, me_sp + 1]

    partners = [{"tp": (me_tp + 1) & 7}, {"tp": (me_tp + 7) & 7}]
    partners += [{"dp": me_dp ^ 1}, {"dp": me_dp ^ 2}, {"dp": me_dp ^ 2, "sp": me_sp ^ 4}]
    partners += [{"sp": me_sp ^ j} for j in range(1, n_sp)]
    barrier = pltpu.get_barrier_semaphore()
    for where in partners:
        pl.semaphore_signal(barrier, inc=1, device_id=where, device_id_type=MESH)
    pl.semaphore_wait(barrier, len(partners))

    def remote(src, dst, send, recv, where):
        return pltpu.make_async_remote_copy(
            src_ref=src,
            dst_ref=dst,
            send_sem=send,
            recv_sem=recv,
            device_id=where,
            device_id_type=MESH,
        )

    chunk = tok // 2

    def crow(c):
        return pl.ds(c * chunk, chunk)

    def z_copy(up, t, c):
        r = (8 - t) % 8 if up else t
        to = (r + 7) % 8 if up else (r + 1) % 8
        src = s_ref.at[crow(c)] if t == 0 else raw.at[r, crow(c)]
        send = r_["zs"].at[0]
        recv = r_["zr"].at[0 if up else 1, t, c]
        where = {"tp": (me_tp + (1 if up else 7)) & 7}
        return remote(src, raw.at[to, crow(c)], send, recv, where)

    def z_exists(up, t, c):
        return t < 3 or (t == 3 and c == (0 if up else 1))

    def z_arrive(t, c):
        for up in (True, False):
            if z_exists(up, t, c):
                z_copy(up, t, c).wait_recv()
                if t < 3 and z_exists(up, t + 1, c):
                    z_copy(up, t + 1, c).start()

    def w_core():
        return remote(w_ref, w_all.at[me_dp], r_["ws"].at[0], r_["wr"].at[0], {"dp": me_dp ^ 1})

    ends = (x == 0) | (x == 3)
    gives = jnp.where(x == 0, yh == 1, yh == 0)

    def w_y(i, j):
        rows = pl.ds(j * half, half)
        where = {"dp": me_dp ^ 2, "sp": me_sp ^ (4 * i)}
        return remote(
            w_ref.at[rows],
            w_all.at[me_dp, rows],
            r_["ws"].at[1],
            r_["wr"].at[1],
            where,
        )

    def w_y_all(n):
        held = w_all.at[pl.ds(0, n)]
        return remote(held, held, r_["ws"].at[1], r_["wr"].at[1], {"dp": me_dp ^ 2})

    def w_fwd():
        block = w_all.at[me_dp ^ 2]
        return remote(block, block, r_["ws"].at[2], r_["wr"].at[2], {"dp": me_dp ^ 1})

    def halo(side, item):
        there = 1 - side
        region = pl.ds(near + there * tok, tok)
        if item < 3 * heads:
            h, kind = divmod(item, 3)
            c = pl.ds(h * HD, HD)
            src = (k_ref, v_ref, q_ref)[kind].at[:, c]
            dst = (keys.at[region, c], vals.at[region, c], qf.at[there, :, c])[kind]
        elif item < 4 * heads:
            c = pl.ds((item - 3 * heads) * HD, HD)
            src, dst = ga_t.at[c], gaf.at[there, c]
        elif item == 4 * heads:
            src, dst = st_out.at[side], st_in.at[there]
        else:
            src, dst = dl_out, dl_in.at[there]
        if item < 4 * heads:
            send = 0
            got = (h if kind < 2 else heads) if item < 3 * heads else item - 2 * heads + 1
        else:
            send = 1 + item - 4 * heads
            got = item - 2 * heads + 1
        return remote(
            src, dst, r_["hs"].at[side, send], r_["hr"].at[there, got], {"sp": side_sp[side]}
        )

    def halo_start(items):
        for side in (0, 1):

            @pl.when(has[side])
            def _():
                for item in items:
                    halo(side, item).start()

    def halo_wait(side, what):
        kind, h = what
        if kind in ("st", "dl"):
            halo(1 - side, 4 * heads + (kind == "dl")).wait_recv()
        elif kind == "ga":
            halo(1 - side, 3 * heads + h).wait_recv()
        else:
            some = keys.at[pl.ds(0, 2 * tok), pl.ds(0, HD)] if kind == "kv" else qf.at[side]
            got = r_["hr"].at[side, h if kind == "kv" else heads]
            remote(some, some, r_["hs"].at[side, 0], got, {"sp": me_sp ^ 1}).wait_recv()

    def halo_wait_both(*whats):
        for side in (0, 1):

            @pl.when(has[side])
            def _():
                for what in whats:
                    halo_wait(side, what)

    for c in (0, 1):
        z_copy(True, 0, c).start()
        z_copy(False, 0, c).start()
    w_core().start()

    @pl.when(jnp.logical_not(ends))
    def _():
        w_y(0, 0).start()
        w_y(1, 1).start()

    @pl.when(ends & gives)
    def _():
        for i in (0, 1):
            for j in (0, 1):
                w_y(i, j).start()

    for h in range(heads):
        halo_start([item_k(h), item_v(h)])
    for h in range(heads):
        halo_start([item_q(h)])

    keys[:tok] = k_ref[...]
    keys[tok:near] = tk_ref[...]
    vals[:tok] = v_ref[...]
    vals[tok:near] = tv_ref[...]
    w_all[me_dp] = w_ref[...]
    for side in (0, 1):

        @pl.when(jnp.logical_not(has[side]))
        def _():
            region = slice(near + side * tok, near + (side + 1) * tok)
            keys[region] = jnp.zeros((tok, width), bf16)
            vals[region] = jnp.zeros((tok, width), bf16)

    def blk(r):
        return (me_tp + r) & 7

    def scale(r):
        gate = gate_ref[:, pl.ds(pl.multiple_of(blk(r) * w, HD), w)].astype(f32)
        src = s_ref[...] if r == 0 else raw[r]
        nat[r] = (src.astype(f32) * gate).astype(bf16)

    def ga_add(r, first=False):
        at = pl.multiple_of((blk(r) & 1) * w, HD)
        term = mm(w_all[blk(r) >> 1, :, pl.ds(at, w)], nat[r], NT)
        if first:
            acc[...] = term
        else:
            acc[...] += term

    slab_of = lax.broadcasted_iota(jnp.int32, (1, n_sp), 1)

    def place_of_slab(slab):
        here = jnp.where(slab_of == slab, map_ref[...].astype(f32), 0.0)
        return jnp.sum(here, axis=1, keepdims=True)

    place = place_of_slab(me_sp)
    reach = win_ref[...].astype(f32)
    side_bias = []
    for side in (0, 1):
        apart = jnp.abs(place - place_of_slab(side_sp[side]))
        seen = (reach[0:1, 0:1] >= 1.0) & (reach[0:1, 1:2] >= apart)
        edge = jnp.where(has[side], 0.0, -1e30).astype(f32)
        side_bias.append(jnp.minimum(jnp.where(seen, 0.0, -1e30).astype(f32), edge))
    place_of = lax.broadcasted_iota(jnp.int32, (text, 1), 0)
    words = jnp.where(place_of < live_ref[0], 0.0, -1e30).astype(f32)
    bias_ref = r_["bias"]
    bias_ref[:tok] = jnp.zeros((tok, 1), f32)
    bias_ref[tok:near] = words
    for side in (0, 1):
        region = slice(near + side * tok, near + (side + 1) * tok)
        bias_ref[region] = jnp.broadcast_to(side_bias[side], (tok, 1))

    def cols(h):
        return slice(h * HD, (h + 1) * HD)

    def forward(h):
        c = cols(h)
        scores = factor * mm(keys[:, c], q_ref[:, c], NT) + bias_ref[...]
        top = jnp.max(scores, axis=0, keepdims=True)
        e = jnp.exp(scores - top)
        inv = 1.0 / jnp.sum(e, axis=0, keepdims=True)
        weights = e * inv
        wts[h] = weights
        att_t[c, :] = mm(vals[:, c], weights.astype(bf16), TN).astype(bf16)
        for side in (0, 1):
            st_out[side, h : h + 1, :] = top - side_bias[side]
            st_out[side, heads + h : heads + h + 1, :] = inv

    def far_weights(side, h):
        c = cols(h)
        scores = factor * mm(keys[:tok, c], qf[side, :, c], NT)
        e = jnp.exp(scores - st_in[side, h : h + 1, :])
        wfar[side, h] = e * st_in[side, heads + h : heads + h + 1, :]

    def core_owns(r):
        return ((blk(r) >> 1) & 1) == core

    def mine(r):
        return (blk(r) >> 1) == me_dp

    def s1_copy(r):
        return remote(
            g1_out.at[r], g1_in.at[r], r_["s1s"].at[0], r_["s1r"].at[r], {"dp": me_dp ^ 1}
        )

    def gy_copy(r, j):
        where = {"dp": me_dp ^ (2 * (j & 1)), "sp": me_sp ^ (2 * (j & 2))}
        return remote(
            gy_out.at[r, y ^ j],
            gy_in.at[r, j - 1],
            r_["gys"].at[0],
            r_["gyr"].at[r],
            where,
        )

    def gx_copy(r, j):
        return remote(
            gx_out.at[r, x ^ j],
            gx_in.at[r, j - 1],
            r_["gxs"].at[0],
            r_["gxr"].at[r],
            {"sp": me_sp ^ j},
        )

    def ag1_copy(r, i):
        return remote(
            fin_out.at[r],
            gfin.at[blk(r) & 1, y, x],
            r_["ag1s"].at[0],
            r_["ag1r"].at[r],
            {"dp": blk(r) >> 1, "sp": 4 * i + x},
        )

    def ag1_sends(r, i):
        return core_owns(r) & jnp.logical_not(mine(r) & (yh == i))

    def ag2_copy(r, j):
        slab = gfin.at[blk(r) & 1, :, x]
        return remote(
            slab, slab, r_["ag2s"].at[0], r_["ag2r"].at[r], {"sp": me_sp ^ j}
        )

    def all_of(some, send, recv):
        return remote(some, some, send, recv, {"sp": me_sp ^ 4})

    def gw_part(r):
        parts[r] = mm(att_t[...], nat[r], NN)

        @pl.when(jnp.logical_not(core_owns(r)))
        def _():
            g1_out[r] = parts[r].astype(bf16)
            s1_copy(r).start()

    def gw_s1(r):
        @pl.when(core_owns(r))
        def _():
            s1_copy(r).wait_recv()
            for i in range(4):
                for k in range(4):
                    rows = slice((4 * i + k) * piece, (4 * i + k + 1) * piece)
                    total = parts[r, rows, :] + g1_in[r, rows, :].astype(f32)
                    parts[r, rows, :] = total
                    gy_out[r, i, k] = total.astype(bf16)
            for j in range(1, 4):
                gy_copy(r, j).start()

    def gw_sy(r):
        @pl.when(core_owns(r))
        def _():
            all_of(gy_in.at[r], r_["gys"].at[0], r_["gyr"].at[r]).wait_recv()
            for k in range(4):
                at = pl.multiple_of(y * (4 * piece) + k * piece, 8)
                total = parts[r, pl.ds(at, piece), :]
                for j in range(3):
                    total = total + gy_in[r, j, k].astype(f32)
                parts[r, k * piece : (k + 1) * piece, :] = total
                gx_out[r, k] = total.astype(bf16)
            for j in range(1, 4):
                gx_copy(r, j).start()

    def gw_sx(r):
        @pl.when(core_owns(r))
        def _():
            all_of(gx_in.at[r], r_["gxs"].at[0], r_["gxr"].at[r]).wait_recv()
            total = parts[r, pl.ds(pl.multiple_of(x * piece, 8), piece), :]
            for j in range(3):
                total = total + gx_in[r, j].astype(f32)
            fin_out[r] = total.astype(bf16)

        for i in (0, 1):

            @pl.when(ag1_sends(r, i))
            def _():
                ag1_copy(r, i).start()

        @pl.when(mine(r))
        def _():
            gfin[blk(r) & 1, y, x] = fin_out[r]

    def gw_ag(r):
        @pl.when(mine(r))
        def _():
            all_of(gx_in.at[0], r_["ag1s"].at[0], r_["ag1r"].at[r]).wait_recv()
            for j in range(1, 4):
                ag2_copy(r, j).start()

    gw_v = r_["gw_v"]

    def gw_end(r):
        @pl.when(mine(r))
        def _():
            all_of(gy_in.at[0], r_["ag2s"].at[0], r_["ag2r"].at[r]).wait_recv()
            at = pl.ds(pl.multiple_of((blk(r) & 1) * w, HD), w)
            for i in range(4):
                for k in range(4):
                    rows = slice((4 * i + k) * piece, (4 * i + k + 1) * piece)
                    gw_v[rows, at] = gfin[blk(r) & 1, i, k].astype(f32)

    trow = text // n_sp

    def tx_copy(j):
        return remote(
            tx_out.at[me_sp ^ j],
            tx_in.at[j - 1],
            r_["txs"].at[0],
            r_["txr"].at[0],
            {"sp": me_sp ^ j},
        )

    def tg_copy(j):
        return remote(
            tg.at[me_sp],
            tg.at[me_sp],
            r_["tgs"].at[0],
            r_["tgr"].at[0],
            {"sp": me_sp ^ j},
        )

    gq_v, gk_v, gv_v, gtk_v, gtv_v = (r_[n] for n in ("gq_v", "gk_v", "gv_v", "gtk_v", "gtv_v"))

    def text_part(h):
        c = cols(h)
        ga = ga_t[c, :]
        wt = wts[h, tok:near, :]
        gp = mm(vals[tok:near, c], ga, NN)
        gs = (wt * (gp - dl_out[h : h + 1, :])).astype(bf16)
        gs_buf[h, tok:near, :] = gs
        gk = (factor * mm(gs, q_ref[:, c], NN)).astype(bf16)
        gv = mm(wt.astype(bf16), ga, NT).astype(bf16)
        for j in range(n_sp):
            rows = slice(j * trow, (j + 1) * trow)
            tx_out[j, :trow, c] = gk[rows]
            tx_out[j, trow:, c] = gv[rows]

    def own_part(h):
        c = cols(h)
        ga = ga_t[c, :]
        delta = dl_out[h : h + 1, :]
        for lo, hi in ((0, tok), (near, near + 2 * tok)):
            gp = mm(vals[lo:hi, c], ga, NN)
            gs_buf[h, lo:hi, :] = (wts[h, lo:hi, :] * (gp - delta)).astype(bf16)
        gq_v[:, c] = (factor * mm(keys[:, c], gs_buf[h], TN)).T.astype(bf16)
        gk_sum[:, c] = mm(gs_buf[h, :tok, :], q_ref[:, c], NN)
        gv_sum[:, c] = mm(wts[h, :tok, :].astype(bf16), ga, NT)

    def far_part(side, h):
        c = cols(h)
        ga = gaf[side, c, :]
        weights = wfar[side, h]
        gp = mm(vals[:tok, c], ga, NN)
        gs = (weights * (gp - dl_in[side, h : h + 1, :])).astype(bf16)
        gk_sum[:, c] += mm(gs, qf[side, :, c], NN)
        gv_sum[:, c] += mm(weights.astype(bf16), ga, NT)

    scale(0)
    z_arrive(0, 0)
    z_arrive(0, 1)
    scale(1)
    scale(7)
    halo_wait_both(("kv", 0))
    forward(0)
    z_arrive(1, 0)
    halo_wait_both(("kv", 1))
    forward(1)
    z_arrive(1, 1)
    scale(2)
    scale(6)
    w_core().wait_recv()
    w_y_all(1).wait_recv()
    w_fwd().start()
    halo_wait_both(("kv", 2))
    forward(2)
    halo_start([4 * heads])
    z_arrive(2, 0)
    for r in (0, 1, 7):
        gw_part(r)
    w_fwd().wait_recv()
    ga_add(0, True)
    ga_add(1)
    ga_add(7)
    for r in (0, 1, 7):
        gw_s1(r)
    z_arrive(2, 1)
    for r in (2, 6):
        gw_part(r)
    ga_add(2)
    ga_add(6)
    for r in (2, 6):
        gw_s1(r)
    scale(3)
    scale(5)
    ga_add(3)
    ga_add(5)
    for r in (3, 5):
        gw_part(r)
    z_arrive(3, 0)
    z_arrive(3, 1)
    scale(4)
    ga_add(4)
    ga_t[...] = acc[...].astype(bf16)
    for h in range(heads):
        c = cols(h)
        dl_out[h : h + 1, :] = jnp.sum(
            ga_t[c, :].astype(f32) * att_t[c, :].astype(f32), axis=0, keepdims=True
        )
    for h in range(heads):
        text_part(h)
    for j in range(1, n_sp):
        tx_copy(j).start()
    for r in (3, 5):
        gw_s1(r)
    gw_part(4)
    for r in (0, 1, 7):
        gw_sy(r)
    halo_start([4 * heads + 1, 3 * heads])
    for r in (2, 6):
        gw_sy(r)
    gw_s1(4)
    halo_start([3 * heads + h for h in range(1, heads)])
    for r in (0, 1, 7):
        gw_sx(r)
    own_part(0)
    for r in (3, 5):
        gw_sy(r)
    for r in (2, 6):
        gw_sx(r)
    own_part(1)
    for r in (0, 1, 7):
        gw_ag(r)
    gw_sy(4)
    own_part(2)
    gq_store = pltpu.make_async_copy(gq_v, r_["gq_out"], r_["os"].at[0])
    gq_store.start()
    halo_wait_both(("st", 0), ("q", 0))
    for h in range(heads):
        for side in (0, 1):
            pl.when(has[side])(functools.partial(far_weights, side, h))
    all_of(tx_in, r_["txs"].at[0], r_["txr"].at[0]).wait_recv()
    total = tx_out[me_sp].astype(f32)
    for j in range(n_sp - 1):
        total = total + tx_in[j].astype(f32)
    tg[me_sp] = total.astype(bf16)
    for j in range(1, n_sp):
        tg_copy(j).start()
    for r in (3, 5):
        gw_sx(r)
    for r in (2, 6):
        gw_ag(r)
    gw_sx(4)
    halo_wait_both(("dl", 0))
    for h in range(heads):
        halo_wait_both(("ga", h))
        for side in (0, 1):
            pl.when(has[side])(functools.partial(far_part, side, h))
        c = cols(h)
        gk_v[:, c] = (factor * gk_sum[:, c]).astype(bf16)
        gv_v[:, c] = gv_sum[:, c].astype(bf16)
        if h == 0:
            for r in (3, 5):
                gw_ag(r)
    stored = [
        pltpu.make_async_copy(gk_v, r_["gk_out"], r_["os"].at[1]),
        pltpu.make_async_copy(gv_v, r_["gv_out"], r_["os"].at[2]),
    ]
    for c in stored:
        c.start()
    gw_ag(4)
    all_of(tg.at[pl.ds(0, n_sp - 1)], r_["tgs"].at[0], r_["tgr"].at[0]).wait_recv()
    for j in range(n_sp):
        rows = slice(j * trow, (j + 1) * trow)
        gtk_v[rows] = tg[j, :trow]
        gtv_v[rows] = tg[j, trow:]
    late = [
        pltpu.make_async_copy(gtk_v, r_["gtk_out"], r_["os"].at[3]),
        pltpu.make_async_copy(gtv_v, r_["gtv_out"], r_["os"].at[4]),
    ]
    for c in late:
        c.start()
    for r in (0, 1, 7, 2, 6, 3, 5, 4):
        gw_end(r)
    gw_store = pltpu.make_async_copy(gw_v, r_["gw_out"], r_["os"].at[5])
    gw_store.start()

    all_of(raw.at[pl.ds(0, n_tp - 1)], r_["zs"].at[0], r_["zr"].at[0, 0, 0]).wait_send()
    w_core().wait_send()

    @pl.when(jnp.logical_not(ends))
    def _():
        w_y_all(1).wait_send()

    @pl.when(ends & gives)
    def _():
        w_y_all(2).wait_send()

    w_fwd().wait_send()
    for side in (0, 1):

        @pl.when(has[side])
        def _():
            blocks = raw.at[pl.ds(0, 4)]
            remote(
                blocks, blocks, r_["hs"].at[side, 0], r_["hr"].at[side, 0], {"sp": side_sp[side]}
            ).wait_send()
            halo(side, 4 * heads).wait_send()
            halo(side, 4 * heads + 1).wait_send()

    for some, n in (
        (g1_out.at[pl.ds(0, 4)], "s1"),
        (gy_in.at[pl.ds(0, 4)], "gy"),
        (gx_in.at[pl.ds(0, 4)], "gx"),
        (gx_in.at[pl.ds(0, 2)], "ag1"),
        (gy_in.at[pl.ds(0, 2)], "ag2"),
        (tx_in, "tx"),
        (tg.at[pl.ds(0, n_sp - 1)], "tg"),
    ):
        all_of(some, r_[n + "s"].at[0], r_[n + "r"].at[0]).wait_send()
    for c in [gq_store] + stored + late + [gw_store]:
        c.wait()


def call(q, k, v, tk, tv, s, w, gate, windows, tile_map, text_count):
    tok, width = q.shape
    text = tk.shape[0]
    heads = width // HD
    cols = w.shape[1]
    total = 3 * tok + text
    block = s.shape[1]
    piece = width // 16
    sm = pl.BlockSpec(memory_space=pltpu.SMEM)
    vm = pl.BlockSpec(memory_space=pltpu.VMEM)
    outs = [
        ("gq", (tok, width), bf16),
        ("gk", (tok, width), bf16),
        ("gv", (tok, width), bf16),
        ("gtk", (text, width), bf16),
        ("gtv", (text, width), bf16),
        ("gw", (width, cols), f32),
    ]
    scratch = [(n + "_v", a, b) for n, a, b in outs] + [
        ("keys", (total, width), bf16),
        ("vals", (total, width), bf16),
        ("qf", (2, tok, width), bf16),
        ("gaf", (2, width, tok), bf16),
        ("st_out", (2, 8, tok), f32),
        ("st_in", (2, 8, tok), f32),
        ("dl_out", (8, tok), f32),
        ("dl_in", (2, 8, tok), f32),
        ("bias", (total, 1), f32),
        ("raw", (8, tok, block), bf16),
        ("nat", (8, tok, block), bf16),
        ("w_all", (4, width, cols), bf16),
        ("acc", (width, tok), f32),
        ("ga_t", (width, tok), bf16),
        ("att_t", (width, tok), bf16),
        ("wts", (heads, total, tok), f32),
        ("wfar", (2, heads, tok, tok), f32),
        ("gs_buf", (heads, total, tok), bf16),
        ("gk_sum", (tok, width), f32),
        ("gv_sum", (tok, width), f32),
        ("parts", (8, width, block), f32),
        ("g1_out", (8, width, block), bf16),
        ("g1_in", (8, width, block), bf16),
        ("gy_out", (8, 4, 4, piece, block), bf16),
        ("gy_in", (8, 3, 4, piece, block), bf16),
        ("gx_out", (8, 4, piece, block), bf16),
        ("gx_in", (8, 3, piece, block), bf16),
        ("fin_out", (8, piece, block), bf16),
        ("gfin", (2, 4, 4, piece, block), bf16),
        ("tx_out", (8, text // 4, width), bf16),
        ("tx_in", (7, text // 4, width), bf16),
        ("tg", (8, text // 4, width), bf16),
    ]
    sems = [
        ("zs", (1,)),
        ("zr", (2, 4, 2)),
        ("ws", (3,)),
        ("wr", (3,)),
        ("hs", (2, 3)),
        ("hr", (2, 2 * heads + 3)),
        ("s1s", (1,)),
        ("s1r", (8,)),
        ("gys", (1,)),
        ("gyr", (8,)),
        ("gxs", (1,)),
        ("gxr", (8,)),
        ("ag1s", (1,)),
        ("ag1r", (8,)),
        ("ag2s", (1,)),
        ("ag2r", (8,)),
        ("txs", (1,)),
        ("txr", (1,)),
        ("tgs", (1,)),
        ("tgr", (1,)),
        ("os", (6,)),
    ]
    args = ["q", "k", "v", "tk", "tv", "s", "w", "gate", "win", "map", "live"]
    names = args + [n + "_out" for n, _, _ in outs] + [n for n, _, _ in scratch]
    names += [n for n, _ in sems]
    return pl.pallas_call(
        functools.partial(kernel, tuple(names)),
        out_shape=[jax.ShapeDtypeStruct(a, b) for _, a, b in outs],
        in_specs=[vm] * 10 + [sm],
        out_specs=[pl.BlockSpec(memory_space=pl.ANY)] * len(outs),
        scratch_shapes=[pltpu.VMEM(a, b) for _, a, b in scratch]
        + [pltpu.SemaphoreType.DMA(n) for _, n in sems],
        compiler_params=pltpu.CompilerParams(
            collective_id=0, has_side_effects=True, vmem_limit_bytes=VMEM
        ),
        name="attention_backward",
    )(q, k, v, tk, tv, s, w, gate, windows, tile_map, text_count)


def copy_kernel(n, *refs):
    srcs, dsts, held = refs[:n], refs[n : 2 * n], refs[2 * n : 3 * n]
    in_sem, out_sem = refs[3 * n :]
    loads = [pltpu.make_async_copy(srcs[i], held[i], in_sem.at[i]) for i in range(n)]
    stores = [pltpu.make_async_copy(held[i], dsts[i], out_sem.at[i]) for i in range(n)]
    for c in loads:
        c.start()
    for i in range(n):
        loads[i].wait()
        stores[i].start()
    for c in stores:
        c.wait()


def copy_call(arrays):
    n = len(arrays)
    hbm = pl.BlockSpec(memory_space=pltpu.HBM)
    return pl.pallas_call(
        functools.partial(copy_kernel, n),
        out_shape=[jax.ShapeDtypeStruct(a.shape, a.dtype) for a in arrays],
        in_specs=[hbm] * n,
        out_specs=[hbm] * n,
        scratch_shapes=[pltpu.VMEM(a.shape, a.dtype) for a in arrays]
        + [pltpu.SemaphoreType.DMA((n,))] * 2,
        compiler_params=pltpu.CompilerParams(vmem_limit_bytes=VMEM),
        name="results",
    )(*arrays)


def per_device(
    query,
    key,
    value,
    text_key,
    text_value,
    grad_out,
    gate,
    out_weight,
    windows,
    tile_map,
    text_count,
):
    outs = call(
        query[0],
        key[0],
        value[0],
        text_key[0],
        text_value[0],
        grad_out[0],
        out_weight,
        gate,
        windows,
        tile_map.T,
        text_count,
    )
    outs = copy_call(outs)
    return tuple(o[None] for o in outs[:5]) + (outs[5],)


def solution(mesh):
    placed = (
        P("dp", "sp", "tp"),
        P("dp", "sp", "tp"),
        P("dp", "sp", "tp"),
        P("dp", None, "tp"),
        P("dp", None, "tp"),
        P("dp", "sp", "tp"),
        P("dp", None),
        P("tp", "dp"),
        P("sp", None),
        P(),
        P("dp"),
    )
    return jax.shard_map(
        per_device,
        mesh=mesh,
        in_specs=placed,
        out_specs=(
            P("dp", "sp", "tp"),
            P("dp", "sp", "tp"),
            P("dp", "sp", "tp"),
            P("dp", None, "tp"),
            P("dp", None, "tp"),
            P("tp", "dp"),
        ),
        check_vma=False,
    )
```

```python
import functools

import jax
import jax.numpy as jnp
from jax import lax
from jax.experimental import pallas as pl
from jax.experimental.pallas import tpu as pltpu
from jax.sharding import PartitionSpec as P

HD = 128
VMEM = 67043328
MESH = pl.DeviceIdType.MESH

NT = (((1,), (1,)), ((), ()))
NN = (((1,), (0,)), ((), ()))
TN = (((0,), (0,)), ((), ()))

bf16, f32 = jnp.bfloat16, jnp.float32


def mm(a, b, dims):
    return lax.dot_general(a, b, dims, preferred_element_type=f32)


def item_k(h):
    return 3 * h


def item_v(h):
    return 3 * h + 1


def item_q(h):
    return 3 * h + 2


def kernel(
    names,
    *refs,
):
    r_ = dict(zip(names, refs, strict=True))
    q_ref, k_ref, v_ref, tk_ref, tv_ref = (r_[n] for n in ("q", "k", "v", "tk", "tv"))
    s_ref, w_ref, gate_ref, win_ref = (r_[n] for n in ("s", "w", "gate", "win"))
    map_ref, live_ref = r_["map"], r_["live"]
    keys, vals, qf, gaf = r_["keys"], r_["vals"], r_["qf"], r_["gaf"]
    st_out, st_in, dl_out, dl_in = r_["st_out"], r_["st_in"], r_["dl_out"], r_["dl_in"]
    raw, nat, w_all, acc = r_["raw"], r_["nat"], r_["w_all"], r_["acc"]
    ga_t, att_t, wts, wfar, gs_buf = r_["ga_t"], r_["att_t"], r_["wts"], r_["wfar"], r_["gs_buf"]
    parts, g1_out, g1_in = r_["parts"], r_["g1_out"], r_["g1_in"]
    gy_out, gy_in, gx_out, gx_in = r_["gy_out"], r_["gy_in"], r_["gx_out"], r_["gx_in"]
    gall, gfin = r_["gall"], r_["gfin"]
    tx_out, tx_in, tg = r_["tx_out"], r_["tx_in"], r_["tg"]
    gk_sum, gv_sum = r_["gk_sum"], r_["gv_sum"]

    factor = HD ** (-0.5)
    tok, width = q_ref.shape
    text = tk_ref.shape[0]
    heads = width // HD
    near = tok + text
    n_tp = n_sp = 8
    me_sp = lax.axis_index("sp")
    me_dp = lax.axis_index("dp")
    me_tp = lax.axis_index("tp")
    x = me_sp & 3
    yh = me_sp >> 2
    core = me_dp & 1
    yl = me_dp >> 1
    w = s_ref.shape[1]
    piece = width // 16
    y = 2 * yh + yl
    half = width // 2
    has = [me_sp >= 1, me_sp + 1 < n_sp]
    side_sp = [me_sp - 1, me_sp + 1]

    partners = [{"tp": (me_tp + 1) & 7}, {"tp": (me_tp + 7) & 7}]
    partners += [{"dp": me_dp ^ 1}, {"dp": me_dp ^ 2}, {"dp": me_dp ^ 2, "sp": me_sp ^ 4}]
    partners += [{"sp": me_sp ^ j} for j in range(1, n_sp)]
    barrier = pltpu.get_barrier_semaphore()
    for where in partners:
        pl.semaphore_signal(barrier, inc=1, device_id=where, device_id_type=MESH)
    pl.semaphore_wait(barrier, len(partners))

    def remote(src, dst, send, recv, where):
        return pltpu.make_async_remote_copy(
            src_ref=src,
            dst_ref=dst,
            send_sem=send,
            recv_sem=recv,
            device_id=where,
            device_id_type=MESH,
        )

    chunk = tok // 2

    def crow(c):
        return pl.ds(c * chunk, chunk)

    def z_copy(up, t, c):
        r = (8 - t) % 8 if up else t
        to = (r + 7) % 8 if up else (r + 1) % 8
        src = s_ref.at[crow(c)] if t == 0 else raw.at[r, crow(c)]
        send = r_["zs"].at[0]
        recv = r_["zr"].at[0 if up else 1, t, c]
        where = {"tp": (me_tp + (1 if up else 7)) & 7}
        return remote(src, raw.at[to, crow(c)], send, recv, where)

    def z_exists(up, t, c):
        return t < 3 or (t == 3 and c == (0 if up else 1))

    def z_arrive(t, i):
        for up in (True, False):
            c = i if up else 1 - i
            if z_exists(up, t, c):
                z_copy(up, t, c).wait_recv()
                if t < 3 and z_exists(up, t + 1, c):
                    z_copy(up, t + 1, c).start()

    def w_core():
        return remote(w_ref, w_all.at[me_dp], r_["ws"].at[0], r_["wr"].at[0], {"dp": me_dp ^ 1})

    ends = (x == 0) | (x == 3)
    gives = jnp.where(x == 0, yh == 1, yh == 0)

    def w_y(i, j):
        rows = pl.ds(j * half, half)
        where = {"dp": me_dp ^ 2, "sp": me_sp ^ (4 * i)}
        return remote(
            w_ref.at[rows],
            w_all.at[me_dp, rows],
            r_["ws"].at[1],
            r_["wr"].at[1],
            where,
        )

    def w_y_all(n):
        held = w_all.at[pl.ds(0, n)]
        return remote(held, held, r_["ws"].at[1], r_["wr"].at[1], {"dp": me_dp ^ 2})

    def w_fwd():
        block = w_all.at[me_dp ^ 2]
        return remote(block, block, r_["ws"].at[2], r_["wr"].at[2], {"dp": me_dp ^ 1})

    def halo(side, item):
        there = 1 - side
        region = pl.ds(near + there * tok, tok)
        if item < 3 * heads:
            h, kind = divmod(item, 3)
            c = pl.ds(h * HD, HD)
            src = (k_ref, v_ref, q_ref)[kind].at[:, c]
            dst = (keys.at[region, c], vals.at[region, c], qf.at[there, :, c])[kind]
        elif item < 4 * heads:
            c = pl.ds((item - 3 * heads) * HD, HD)
            src, dst = ga_t.at[c], gaf.at[there, c]
        elif item == 4 * heads:
            src, dst = st_out.at[side], st_in.at[there]
        else:
            src, dst = dl_out, dl_in.at[there]
        if item < 4 * heads:
            send = 0
            got = (h if kind < 2 else heads) if item < 3 * heads else item - 2 * heads + 1
        else:
            send = 1 + item - 4 * heads
            got = item - 2 * heads + 1
        return remote(
            src, dst, r_["hs"].at[side, send], r_["hr"].at[there, got], {"sp": side_sp[side]}
        )

    def halo_start(items):
        for side in (0, 1):

            @pl.when(has[side])
            def _():
                for item in items:
                    halo(side, item).start()

    def halo_wait(side, what):
        kind, h = what
        if kind in ("st", "dl"):
            halo(1 - side, 4 * heads + (kind == "dl")).wait_recv()
        elif kind == "ga":
            halo(1 - side, 3 * heads + h).wait_recv()
        else:
            some = keys.at[pl.ds(0, 2 * tok), pl.ds(0, HD)] if kind == "kv" else qf.at[side]
            got = r_["hr"].at[side, h if kind == "kv" else heads]
            remote(some, some, r_["hs"].at[side, 0], got, {"sp": me_sp ^ 1}).wait_recv()

    def halo_wait_both(*whats):
        for side in (0, 1):

            @pl.when(has[side])
            def _():
                for what in whats:
                    halo_wait(side, what)

    for c in (0, 1):
        z_copy(True, 0, c).start()
        z_copy(False, 0, 1 - c).start()
    w_core().start()

    @pl.when(jnp.logical_not(ends))
    def _():
        w_y(0, 0).start()
        w_y(1, 1).start()

    @pl.when(ends & gives)
    def _():
        for i in (0, 1):
            for j in (0, 1):
                w_y(i, j).start()

    for h in range(heads):
        halo_start([item_k(h), item_v(h)])
    for h in range(heads):
        halo_start([item_q(h)])

    keys[:tok] = k_ref[...]
    keys[tok:near] = tk_ref[...]
    vals[:tok] = v_ref[...]
    vals[tok:near] = tv_ref[...]
    w_all[me_dp] = w_ref[...]
    for side in (0, 1):

        @pl.when(jnp.logical_not(has[side]))
        def _():
            region = slice(near + side * tok, near + (side + 1) * tok)
            keys[region] = jnp.zeros((tok, width), bf16)
            vals[region] = jnp.zeros((tok, width), bf16)

    def blk(r):
        return (me_tp + r) & 7

    def scale(r):
        gate = gate_ref[:, pl.ds(pl.multiple_of(blk(r) * w, HD), w)].astype(f32)
        src = s_ref[...] if r == 0 else raw[r]
        nat[r] = (src.astype(f32) * gate).astype(bf16)

    def ga_add(r, first=False):
        at = pl.multiple_of((blk(r) & 1) * w, HD)
        term = mm(w_all[blk(r) >> 1, :, pl.ds(at, w)], nat[r], NT)
        if first:
            acc[...] = term
        else:
            acc[...] += term

    slab_of = lax.broadcasted_iota(jnp.int32, (1, n_sp), 1)

    def place_of_slab(slab):
        here = jnp.where(slab_of == slab, map_ref[...].astype(f32), 0.0)
        return jnp.sum(here, axis=1, keepdims=True)

    place = place_of_slab(me_sp)
    reach = win_ref[...].astype(f32)
    side_bias = []
    for side in (0, 1):
        apart = jnp.abs(place - place_of_slab(side_sp[side]))
        seen = (reach[0:1, 0:1] >= 1.0) & (reach[0:1, 1:2] >= apart)
        edge = jnp.where(has[side], 0.0, -1e30).astype(f32)
        side_bias.append(jnp.minimum(jnp.where(seen, 0.0, -1e30).astype(f32), edge))
    place_of = lax.broadcasted_iota(jnp.int32, (text, 1), 0)
    words = jnp.where(place_of < live_ref[0], 0.0, -1e30).astype(f32)
    bias_ref = r_["bias"]
    bias_ref[:tok] = jnp.zeros((tok, 1), f32)
    bias_ref[tok:near] = words
    for side in (0, 1):
        region = slice(near + side * tok, near + (side + 1) * tok)
        bias_ref[region] = jnp.broadcast_to(side_bias[side], (tok, 1))

    def cols(h):
        return slice(h * HD, (h + 1) * HD)

    def forward(h):
        c = cols(h)
        scores = factor * mm(keys[:, c], q_ref[:, c], NT) + bias_ref[...]
        top = jnp.max(scores, axis=0, keepdims=True)
        e = jnp.exp(scores - top)
        inv = 1.0 / jnp.sum(e, axis=0, keepdims=True)
        weights = e * inv
        wts[h] = weights
        att_t[c, :] = mm(vals[:, c], weights.astype(bf16), TN).astype(bf16)
        for side in (0, 1):
            st_out[side, h : h + 1, :] = top - side_bias[side]
            st_out[side, heads + h : heads + h + 1, :] = inv

    def far_weights(side, h):
        c = cols(h)
        scores = factor * mm(keys[:tok, c], qf[side, :, c], NT)
        e = jnp.exp(scores - st_in[side, h : h + 1, :])
        wfar[side, h] = e * st_in[side, heads + h : heads + h + 1, :]

    def core_owns(r):
        return ((blk(r) >> 1) & 1) == core

    def mine(r):
        return (blk(r) >> 1) == me_dp

    def s1_copy(r):
        return remote(
            g1_out.at[r], g1_in.at[r], r_["s1s"].at[0], r_["s1r"].at[r], {"dp": me_dp ^ 1}
        )

    def x_first(r):
        return r in (2, 6)

    def along_x(j):
        return {"sp": me_sp ^ j}

    def along_y(j):
        return {"dp": me_dp ^ (2 * (j & 1)), "sp": me_sp ^ (2 * (j & 2))}

    def place1(r):
        return x if x_first(r) else y

    def place2(r):
        return y if x_first(r) else x

    def gy_copy(r, j):
        where = along_x(j) if x_first(r) else along_y(j)
        return remote(
            gy_out.at[r, place1(r) ^ j],
            gy_in.at[r, j - 1],
            r_["gys"].at[0],
            r_["gyr"].at[r],
            where,
        )

    def gx_copy(r, j):
        where = along_y(j) if x_first(r) else along_x(j)
        return remote(
            gx_out.at[r, place2(r) ^ j],
            gx_in.at[r, j - 1],
            r_["gxs"].at[0],
            r_["gxr"].at[r],
            where,
        )

    def ag1_copy(r, j):
        piece_ = gall.at[r, x]
        return remote(piece_, piece_, r_["ag1s"].at[0], r_["ag1r"].at[r], along_x(j))

    def ag2_copy(r, i):
        return remote(
            gall.at[r],
            gfin.at[blk(r) & 1, y],
            r_["ag2s"].at[0],
            r_["ag2r"].at[r],
            {"dp": blk(r) >> 1, "sp": 4 * i + x},
        )

    def ag2_sends(r, i):
        return core_owns(r) & jnp.logical_not(mine(r) & (yh == i))

    def all_of(some, send, recv):
        return remote(some, some, send, recv, {"sp": me_sp ^ 4})

    def gw_part(r):
        parts[r] = mm(att_t[...], nat[r], NN)

        @pl.when(jnp.logical_not(core_owns(r)))
        def _():
            g1_out[r] = parts[r].astype(bf16)
            s1_copy(r).start()

    def gw_s1(r):
        @pl.when(core_owns(r))
        def _():
            s1_copy(r).wait_recv()
            for i in range(4):
                for k in range(4):
                    rows = slice((4 * i + k) * piece, (4 * i + k + 1) * piece)
                    total = parts[r, rows, :] + g1_in[r, rows, :].astype(f32)
                    parts[r, rows, :] = total
                    gy_out[r, i, k] = total.astype(bf16)
            for j in range(1, 4):
                gy_copy(r, j).start()

    def gw_sy(r):
        @pl.when(core_owns(r))
        def _():
            all_of(gy_in.at[r], r_["gys"].at[0], r_["gyr"].at[r]).wait_recv()
            for k in range(4):
                at = pl.multiple_of(place1(r) * (4 * piece) + k * piece, 8)
                total = parts[r, pl.ds(at, piece), :]
                for j in range(3):
                    total = total + gy_in[r, j, k].astype(f32)
                parts[r, k * piece : (k + 1) * piece, :] = total
                gx_out[r, k] = total.astype(bf16)
            for j in range(1, 4):
                gx_copy(r, j).start()

    def gw_sx(r):
        @pl.when(core_owns(r))
        def _():
            all_of(gx_in.at[r], r_["gxs"].at[0], r_["gxr"].at[r]).wait_recv()
            total = parts[r, pl.ds(pl.multiple_of(place2(r) * piece, 8), piece), :]
            for j in range(3):
                total = total + gx_in[r, j].astype(f32)
            gall[r, x] = total.astype(bf16)
            for j in range(1, 4):
                ag1_copy(r, j).start()

    def gw_ag(r):
        @pl.when(core_owns(r))
        def _():
            all_of(gx_in.at[0], r_["ag1s"].at[0], r_["ag1r"].at[r]).wait_recv()

        for i in (0, 1):

            @pl.when(ag2_sends(r, i))
            def _():
                ag2_copy(r, i).start()

        @pl.when(mine(r))
        def _():
            gfin[blk(r) & 1, y] = gall[r]

    gw_v = r_["gw_v"]

    def gw_end(r):
        @pl.when(mine(r))
        def _():
            all_of(gy_in.at[0], r_["ag2s"].at[0], r_["ag2r"].at[r]).wait_recv()
            at = pl.ds(pl.multiple_of((blk(r) & 1) * w, HD), w)
            for i in range(4):
                for k in range(4):
                    n = 4 * k + i if x_first(r) else 4 * i + k
                    rows = slice(n * piece, (n + 1) * piece)
                    gw_v[rows, at] = gfin[blk(r) & 1, i, k].astype(f32)

    trow = text // n_sp

    def tx_copy(j):
        return remote(
            tx_out.at[me_sp ^ j],
            tx_in.at[j - 1],
            r_["txs"].at[0],
            r_["txr"].at[0],
            {"sp": me_sp ^ j},
        )

    def tg_copy(j):
        return remote(
            tg.at[me_sp],
            tg.at[me_sp],
            r_["tgs"].at[0],
            r_["tgr"].at[0],
            {"sp": me_sp ^ j},
        )

    gq_v, gk_v, gv_v, gtk_v, gtv_v = (r_[n] for n in ("gq_v", "gk_v", "gv_v", "gtk_v", "gtv_v"))

    def text_part(h):
        c = cols(h)
        ga = ga_t[c, :]
        wt = wts[h, tok:near, :]
        gp = mm(vals[tok:near, c], ga, NN)
        gs = (wt * (gp - dl_out[h : h + 1, :])).astype(bf16)
        gs_buf[h, tok:near, :] = gs
        gk = (factor * mm(gs, q_ref[:, c], NN)).astype(bf16)
        gv = mm(wt.astype(bf16), ga, NT).astype(bf16)
        for j in range(n_sp):
            rows = slice(j * trow, (j + 1) * trow)
            tx_out[j, :trow, c] = gk[rows]
            tx_out[j, trow:, c] = gv[rows]

    def own_part(h):
        c = cols(h)
        ga = ga_t[c, :]
        delta = dl_out[h : h + 1, :]
        for lo, hi in ((0, tok), (near, near + 2 * tok)):
            gp = mm(vals[lo:hi, c], ga, NN)
            gs_buf[h, lo:hi, :] = (wts[h, lo:hi, :] * (gp - delta)).astype(bf16)
        gq_v[:, c] = (factor * mm(keys[:, c], gs_buf[h], TN)).T.astype(bf16)
        gk_sum[:, c] = mm(gs_buf[h, :tok, :], q_ref[:, c], NN)
        gv_sum[:, c] = mm(wts[h, :tok, :].astype(bf16), ga, NT)

    def far_part(side, h):
        c = cols(h)
        ga = gaf[side, c, :]
        weights = wfar[side, h]
        gp = mm(vals[:tok, c], ga, NN)
        gs = (weights * (gp - dl_in[side, h : h + 1, :])).astype(bf16)
        gk_sum[:, c] += mm(gs, qf[side, :, c], NN)
        gv_sum[:, c] += mm(weights.astype(bf16), ga, NT)

    scale(0)
    z_arrive(0, 0)
    z_arrive(0, 1)
    scale(1)
    scale(7)
    halo_wait_both(("kv", 0))
    forward(0)
    z_arrive(1, 0)
    halo_wait_both(("kv", 1))
    forward(1)
    z_arrive(1, 1)
    scale(2)
    scale(6)
    w_core().wait_recv()
    w_y_all(1).wait_recv()
    w_fwd().start()
    halo_wait_both(("kv", 2))
    forward(2)
    halo_start([4 * heads])
    for r in (0, 1, 7):
        gw_part(r)
    z_arrive(2, 0)
    w_fwd().wait_recv()
    ga_add(0, True)
    ga_add(1)
    ga_add(7)
    for r in (0, 1, 7):
        gw_s1(r)
    for r in (2, 6):
        gw_part(r)
    ga_add(2)
    ga_add(6)
    z_arrive(2, 1)
    scale(3)
    scale(5)
    ga_add(3)
    ga_add(5)
    for r in (3, 5):
        gw_part(r)
    for r in (2, 6):
        gw_s1(r)
    z_arrive(3, 0)
    scale(4)
    gw_part(4)
    ga_add(4)
    ga_t[...] = acc[...].astype(bf16)
    for h in range(heads):
        c = cols(h)
        dl_out[h : h + 1, :] = jnp.sum(
            ga_t[c, :].astype(f32) * att_t[c, :].astype(f32), axis=0, keepdims=True
        )
    for r in (3, 5):
        gw_s1(r)
    for h in range(heads):
        text_part(h)
    gw_s1(4)
    for r in (0, 1, 7):
        gw_sy(r)
    for j in range(1, n_sp):
        tx_copy(j).start()
    for r in (2, 6):
        gw_sy(r)
    halo_start([4 * heads + 1, 3 * heads])
    own_part(0)
    for r in (0, 1, 7):
        gw_sx(r)
    for r in (3, 5):
        gw_sy(r)
    halo_start([3 * heads + h for h in range(1, heads)])
    own_part(1)
    gw_sy(4)
    own_part(2)
    gq_store = pltpu.make_async_copy(gq_v, r_["gq_out"], r_["os"].at[0])
    gq_store.start()
    halo_wait_both(("st", 0), ("q", 0))
    for h in range(heads):
        for side in (0, 1):
            pl.when(has[side])(functools.partial(far_weights, side, h))
    for r in (2, 6):
        gw_sx(r)
    for r in (0, 1, 7):
        gw_ag(r)
    all_of(tx_in, r_["txs"].at[0], r_["txr"].at[0]).wait_recv()
    total = tx_out[me_sp].astype(f32)
    for j in range(n_sp - 1):
        total = total + tx_in[j].astype(f32)
    tg[me_sp] = total.astype(bf16)
    for r in (3, 5):
        gw_sx(r)
    for j in range(1, n_sp):
        tg_copy(j).start()
    for r in (2, 6):
        gw_ag(r)
    gw_sx(4)
    halo_wait_both(("dl", 0))
    for h in range(heads):
        halo_wait_both(("ga", h))
        for side in (0, 1):
            pl.when(has[side])(functools.partial(far_part, side, h))
        c = cols(h)
        gk_v[:, c] = (factor * gk_sum[:, c]).astype(bf16)
        gv_v[:, c] = gv_sum[:, c].astype(bf16)
        if h == 0:
            for r in (3, 5):
                gw_ag(r)
        if h == 1:
            gw_ag(4)
    stored = [
        pltpu.make_async_copy(gk_v, r_["gk_out"], r_["os"].at[1]),
        pltpu.make_async_copy(gv_v, r_["gv_out"], r_["os"].at[2]),
    ]
    for c in stored:
        c.start()
    all_of(tg.at[pl.ds(0, n_sp - 1)], r_["tgs"].at[0], r_["tgr"].at[0]).wait_recv()
    for j in range(n_sp):
        rows = slice(j * trow, (j + 1) * trow)
        gtk_v[rows] = tg[j, :trow]
        gtv_v[rows] = tg[j, trow:]
    late = [
        pltpu.make_async_copy(gtk_v, r_["gtk_out"], r_["os"].at[3]),
        pltpu.make_async_copy(gtv_v, r_["gtv_out"], r_["os"].at[4]),
    ]
    for c in late:
        c.start()
    for r in (0, 1, 7, 2, 6, 3, 5, 4):
        gw_end(r)
    gw_store = pltpu.make_async_copy(gw_v, r_["gw_out"], r_["os"].at[5])
    gw_store.start()

    all_of(raw.at[pl.ds(0, n_tp - 1)], r_["zs"].at[0], r_["zr"].at[0, 0, 0]).wait_send()
    w_core().wait_send()

    @pl.when(jnp.logical_not(ends))
    def _():
        w_y_all(1).wait_send()

    @pl.when(ends & gives)
    def _():
        w_y_all(2).wait_send()

    w_fwd().wait_send()
    for side in (0, 1):

        @pl.when(has[side])
        def _():
            blocks = raw.at[pl.ds(0, 4)]
            remote(
                blocks, blocks, r_["hs"].at[side, 0], r_["hr"].at[side, 0], {"sp": side_sp[side]}
            ).wait_send()
            halo(side, 4 * heads).wait_send()
            halo(side, 4 * heads + 1).wait_send()

    for some, n in (
        (g1_out.at[pl.ds(0, 4)], "s1"),
        (gy_in.at[pl.ds(0, 4)], "gy"),
        (gx_in.at[pl.ds(0, 4)], "gx"),
        (gx_in.at[pl.ds(0, 4)], "ag1"),
        (gy_in.at[pl.ds(0, 2)], "ag2"),
        (tx_in, "tx"),
        (tg.at[pl.ds(0, n_sp - 1)], "tg"),
    ):
        all_of(some, r_[n + "s"].at[0], r_[n + "r"].at[0]).wait_send()
    for c in [gq_store] + stored + late + [gw_store]:
        c.wait()


def call(q, k, v, tk, tv, s, w, gate, windows, tile_map, text_count):
    tok, width = q.shape
    text = tk.shape[0]
    heads = width // HD
    cols = w.shape[1]
    total = 3 * tok + text
    block = s.shape[1]
    piece = width // 16
    sm = pl.BlockSpec(memory_space=pltpu.SMEM)
    vm = pl.BlockSpec(memory_space=pltpu.VMEM)
    outs = [
        ("gq", (tok, width), bf16),
        ("gk", (tok, width), bf16),
        ("gv", (tok, width), bf16),
        ("gtk", (text, width), bf16),
        ("gtv", (text, width), bf16),
        ("gw", (width, cols), f32),
    ]
    scratch = [(n + "_v", a, b) for n, a, b in outs] + [
        ("keys", (total, width), bf16),
        ("vals", (total, width), bf16),
        ("qf", (2, tok, width), bf16),
        ("gaf", (2, width, tok), bf16),
        ("st_out", (2, 8, tok), f32),
        ("st_in", (2, 8, tok), f32),
        ("dl_out", (8, tok), f32),
        ("dl_in", (2, 8, tok), f32),
        ("bias", (total, 1), f32),
        ("raw", (8, tok, block), bf16),
        ("nat", (8, tok, block), bf16),
        ("w_all", (4, width, cols), bf16),
        ("acc", (width, tok), f32),
        ("ga_t", (width, tok), bf16),
        ("att_t", (width, tok), bf16),
        ("wts", (heads, total, tok), f32),
        ("wfar", (2, heads, tok, tok), f32),
        ("gs_buf", (heads, total, tok), bf16),
        ("gk_sum", (tok, width), f32),
        ("gv_sum", (tok, width), f32),
        ("parts", (8, width, block), f32),
        ("g1_out", (8, width, block), bf16),
        ("g1_in", (8, width, block), bf16),
        ("gy_out", (8, 4, 4, piece, block), bf16),
        ("gy_in", (8, 3, 4, piece, block), bf16),
        ("gx_out", (8, 4, piece, block), bf16),
        ("gx_in", (8, 3, piece, block), bf16),
        ("gall", (8, 4, piece, block), bf16),
        ("gfin", (2, 4, 4, piece, block), bf16),
        ("tx_out", (8, text // 4, width), bf16),
        ("tx_in", (7, text // 4, width), bf16),
        ("tg", (8, text // 4, width), bf16),
    ]
    sems = [
        ("zs", (1,)),
        ("zr", (2, 4, 2)),
        ("ws", (3,)),
        ("wr", (3,)),
        ("hs", (2, 3)),
        ("hr", (2, 2 * heads + 3)),
        ("s1s", (1,)),
        ("s1r", (8,)),
        ("gys", (1,)),
        ("gyr", (8,)),
        ("gxs", (1,)),
        ("gxr", (8,)),
        ("ag1s", (1,)),
        ("ag1r", (8,)),
        ("ag2s", (1,)),
        ("ag2r", (8,)),
        ("txs", (1,)),
        ("txr", (1,)),
        ("tgs", (1,)),
        ("tgr", (1,)),
        ("os", (6,)),
    ]
    args = ["q", "k", "v", "tk", "tv", "s", "w", "gate", "win", "map", "live"]
    names = args + [n + "_out" for n, _, _ in outs] + [n for n, _, _ in scratch]
    names += [n for n, _ in sems]
    return pl.pallas_call(
        functools.partial(kernel, tuple(names)),
        out_shape=[jax.ShapeDtypeStruct(a, b) for _, a, b in outs],
        in_specs=[vm] * 10 + [sm],
        out_specs=[pl.BlockSpec(memory_space=pl.ANY)] * len(outs),
        scratch_shapes=[pltpu.VMEM(a, b) for _, a, b in scratch]
        + [pltpu.SemaphoreType.DMA(n) for _, n in sems],
        compiler_params=pltpu.CompilerParams(
            collective_id=0, has_side_effects=True, vmem_limit_bytes=VMEM
        ),
        name="attention_backward",
    )(q, k, v, tk, tv, s, w, gate, windows, tile_map, text_count)


def copy_kernel(n, *refs):
    srcs, dsts, held = refs[:n], refs[n : 2 * n], refs[2 * n : 3 * n]
    in_sem, out_sem = refs[3 * n :]
    loads = [pltpu.make_async_copy(srcs[i], held[i], in_sem.at[i]) for i in range(n)]
    stores = [pltpu.make_async_copy(held[i], dsts[i], out_sem.at[i]) for i in range(n)]
    for c in loads:
        c.start()
    for i in range(n):
        loads[i].wait()
        stores[i].start()
    for c in stores:
        c.wait()


def copy_call(arrays):
    n = len(arrays)
    hbm = pl.BlockSpec(memory_space=pltpu.HBM)
    return pl.pallas_call(
        functools.partial(copy_kernel, n),
        out_shape=[jax.ShapeDtypeStruct(a.shape, a.dtype) for a in arrays],
        in_specs=[hbm] * n,
        out_specs=[hbm] * n,
        scratch_shapes=[pltpu.VMEM(a.shape, a.dtype) for a in arrays]
        + [pltpu.SemaphoreType.DMA((n,))] * 2,
        compiler_params=pltpu.CompilerParams(vmem_limit_bytes=VMEM),
        name="results",
    )(*arrays)


def per_device(
    query,
    key,
    value,
    text_key,
    text_value,
    grad_out,
    gate,
    out_weight,
    windows,
    tile_map,
    text_count,
):
    outs = call(
        query[0],
        key[0],
        value[0],
        text_key[0],
        text_value[0],
        grad_out[0],
        out_weight,
        gate,
        windows,
        tile_map.T,
        text_count,
    )
    outs = copy_call(outs)
    return tuple(o[None] for o in outs[:5]) + (outs[5],)


def solution(mesh):
    placed = (
        P("dp", "sp", "tp"),
        P("dp", "sp", "tp"),
        P("dp", "sp", "tp"),
        P("dp", None, "tp"),
        P("dp", None, "tp"),
        P("dp", "sp", "tp"),
        P("dp", None),
        P("tp", "dp"),
        P("sp", None),
        P(),
        P("dp"),
    )
    return jax.shard_map(
        per_device,
        mesh=mesh,
        in_specs=placed,
        out_specs=(
            P("dp", "sp", "tp"),
            P("dp", "sp", "tp"),
            P("dp", "sp", "tp"),
            P("dp", None, "tp"),
            P("dp", None, "tp"),
            P("tp", "dp"),
        ),
        check_vma=False,
    )
```

```python
import functools

import jax
import jax.numpy as jnp
from jax import lax
from jax.experimental import pallas as pl
from jax.experimental.pallas import tpu as pltpu
from jax.sharding import PartitionSpec as P

HD = 128
VMEM = 67043328
MESH = pl.DeviceIdType.MESH

NT = (((1,), (1,)), ((), ()))
NN = (((1,), (0,)), ((), ()))
TN = (((0,), (0,)), ((), ()))

bf16, f32 = jnp.bfloat16, jnp.float32


def mm(a, b, dims):
    return lax.dot_general(a, b, dims, preferred_element_type=f32)


def item_k(h):
    return 3 * h


def item_v(h):
    return 3 * h + 1


def item_q(h):
    return 3 * h + 2


def kernel(
    names,
    *refs,
):
    r_ = dict(zip(names, refs, strict=True))
    q_ref, s_ref, gate_ref, win_ref = (r_[n] for n in ("q_v", "s_v", "gate", "win"))
    map_ref, live_ref = r_["map"], r_["live"]
    keys, vals, qf, gaf = r_["keys"], r_["vals"], r_["qf"], r_["gaf"]
    st_out, st_in, dl_out, dl_in = r_["st_out"], r_["st_in"], r_["dl_out"], r_["dl_in"]
    raw, nat, w_all, acc = r_["raw"], r_["nat"], r_["w_all"], r_["acc"]
    ga_t, att_t, wts, wfar, gs_buf = r_["ga_t"], r_["att_t"], r_["wts"], r_["wfar"], r_["gs_buf"]
    parts, g1_out, g1_in = r_["parts"], r_["g1_out"], r_["g1_in"]
    gy_out, gy_in, gx_out, gx_in = r_["gy_out"], r_["gy_in"], r_["gx_out"], r_["gx_in"]
    gall, gfin = r_["gall"], r_["gfin"]
    tx_out, tx_in, tg = r_["tx_out"], r_["tx_in"], r_["tg"]
    ty_out, ty_in, t_own = r_["ty_out"], r_["ty_in"], r_["t_own"]
    gk_sum, gv_sum = r_["gk_sum"], r_["gv_sum"]

    factor = HD ** (-0.5)
    tok, width = q_ref.shape
    text = r_["tk"].shape[0]
    heads = width // HD
    near = tok + text
    n_tp = n_sp = 8
    me_sp = lax.axis_index("sp")
    me_dp = lax.axis_index("dp")
    me_tp = lax.axis_index("tp")
    x = me_sp & 3
    yh = me_sp >> 2
    core = me_dp & 1
    yl = me_dp >> 1
    w = s_ref.shape[1]
    piece = width // 16
    y = 2 * yh + yl
    half = width // 2
    has = [me_sp >= 1, me_sp + 1 < n_sp]
    side_sp = [me_sp - 1, me_sp + 1]

    partners = [{"tp": (me_tp + 1) & 7}, {"tp": (me_tp + 7) & 7}]
    partners += [{"dp": me_dp ^ 1}, {"dp": me_dp ^ 2}, {"dp": me_dp ^ 2, "sp": me_sp ^ 4}]
    partners += [{"sp": me_sp ^ j} for j in range(1, n_sp)]
    barrier = pltpu.get_barrier_semaphore()
    for where in partners:
        pl.semaphore_signal(barrier, inc=1, device_id=where, device_id_type=MESH)

    w_ref = w_all.at[me_dp]
    loads = {
        n: pltpu.make_async_copy(r_[n], to, r_["ls"].at[i])
        for i, (n, to) in enumerate(
            [
                ("s", s_ref),
                ("w", w_ref),
                ("k", keys.at[pl.ds(0, tok)]),
                ("v", vals.at[pl.ds(0, tok)]),
                ("q", q_ref),
                ("tk", keys.at[pl.ds(tok, text)]),
                ("tv", vals.at[pl.ds(tok, text)]),
            ]
        )
    }
    for c in loads.values():
        c.start()
    pl.semaphore_wait(barrier, len(partners))

    def remote(src, dst, send, recv, where):
        return pltpu.make_async_remote_copy(
            src_ref=src,
            dst_ref=dst,
            send_sem=send,
            recv_sem=recv,
            device_id=where,
            device_id_type=MESH,
        )

    chunk = tok // 2

    def crow(c):
        return pl.ds(c * chunk, chunk)

    def z_copy(up, t, c):
        r = (8 - t) % 8 if up else t
        to = (r + 7) % 8 if up else (r + 1) % 8
        src = s_ref.at[crow(c)] if t == 0 else raw.at[r, crow(c)]
        send = r_["zs"].at[0]
        recv = r_["zr"].at[0 if up else 1, t, c]
        where = {"tp": (me_tp + (1 if up else 7)) & 7}
        return remote(src, raw.at[to, crow(c)], send, recv, where)

    def z_exists(up, t, c):
        return t < 3 or (t == 3 and c == (0 if up else 1))

    def z_arrive(t, i):
        for up in (True, False):
            c = i if up else 1 - i
            if z_exists(up, t, c):
                z_copy(up, t, c).wait_recv()
                if t < 3 and z_exists(up, t + 1, c):
                    z_copy(up, t + 1, c).start()

    def w_core():
        return remote(w_ref, w_all.at[me_dp], r_["ws"].at[0], r_["wr"].at[0], {"dp": me_dp ^ 1})

    ends = (x == 0) | (x == 3)
    gives = jnp.where(x == 0, yh == 1, yh == 0)

    def w_y(i, j):
        rows = pl.ds(j * half, half)
        where = {"dp": me_dp ^ 2, "sp": me_sp ^ (4 * i)}
        return remote(
            w_ref.at[rows],
            w_all.at[me_dp, rows],
            r_["ws"].at[1],
            r_["wr"].at[1],
            where,
        )

    def w_y_all(n):
        held = w_all.at[pl.ds(0, n)]
        return remote(held, held, r_["ws"].at[1], r_["wr"].at[1], {"dp": me_dp ^ 2})

    def w_fwd():
        block = w_all.at[me_dp ^ 2]
        return remote(block, block, r_["ws"].at[2], r_["wr"].at[2], {"dp": me_dp ^ 1})

    def halo(side, item):
        there = 1 - side
        region = pl.ds(near + there * tok, tok)
        if item < 3 * heads:
            h, kind = divmod(item, 3)
            c = pl.ds(h * HD, HD)
            src = (keys.at[pl.ds(0, tok), c], vals.at[pl.ds(0, tok), c], q_ref.at[:, c])[kind]
            dst = (keys.at[region, c], vals.at[region, c], qf.at[there, :, c])[kind]
        elif item < 4 * heads:
            c = pl.ds((item - 3 * heads) * HD, HD)
            src, dst = ga_t.at[c], gaf.at[there, c]
        elif item == 4 * heads:
            src, dst = st_out.at[side], st_in.at[there]
        else:
            src, dst = dl_out, dl_in.at[there]
        if item < 4 * heads:
            send = 0
            got = (h if kind < 2 else heads) if item < 3 * heads else item - 2 * heads + 1
        else:
            send = 1 + item - 4 * heads
            got = item - 2 * heads + 1
        return remote(
            src, dst, r_["hs"].at[side, send], r_["hr"].at[there, got], {"sp": side_sp[side]}
        )

    def halo_start(items):
        for side in (0, 1):

            @pl.when(has[side])
            def _():
                for item in items:
                    halo(side, item).start()

    def halo_wait(side, what):
        kind, h = what
        if kind in ("st", "dl"):
            halo(1 - side, 4 * heads + (kind == "dl")).wait_recv()
        elif kind == "ga":
            halo(1 - side, 3 * heads + h).wait_recv()
        else:
            some = keys.at[pl.ds(0, 2 * tok), pl.ds(0, HD)] if kind == "kv" else qf.at[side]
            got = r_["hr"].at[side, h if kind == "kv" else heads]
            remote(some, some, r_["hs"].at[side, 0], got, {"sp": me_sp ^ 1}).wait_recv()

    def halo_wait_both(*whats):
        for side in (0, 1):

            @pl.when(has[side])
            def _():
                for what in whats:
                    halo_wait(side, what)

    loads["s"].wait()
    for c in (0, 1):
        z_copy(True, 0, c).start()
        z_copy(False, 0, 1 - c).start()
    loads["w"].wait()
    w_core().start()

    @pl.when(jnp.logical_not(ends))
    def _():
        w_y(0, 0).start()
        w_y(1, 1).start()

    @pl.when(ends & gives)
    def _():
        for i in (0, 1):
            for j in (0, 1):
                w_y(i, j).start()

    loads["k"].wait()
    loads["v"].wait()
    for h in range(heads):
        halo_start([item_k(h), item_v(h)])
    loads["q"].wait()
    for h in range(heads):
        halo_start([item_q(h)])
    loads["tk"].wait()
    loads["tv"].wait()
    for side in (0, 1):

        @pl.when(jnp.logical_not(has[side]))
        def _():
            region = slice(near + side * tok, near + (side + 1) * tok)
            keys[region] = jnp.zeros((tok, width), bf16)
            vals[region] = jnp.zeros((tok, width), bf16)

    def blk(r):
        return (me_tp + r) & 7

    def scale(r):
        gate = gate_ref[:, pl.ds(pl.multiple_of(blk(r) * w, HD), w)].astype(f32)
        src = s_ref[...] if r == 0 else raw[r]
        nat[r] = (src.astype(f32) * gate).astype(bf16)

    def ga_add(r, first=False):
        at = pl.multiple_of((blk(r) & 1) * w, HD)
        term = mm(w_all[blk(r) >> 1, :, pl.ds(at, w)], nat[r], NT)
        if first:
            acc[...] = term
        else:
            acc[...] += term

    slab_of = lax.broadcasted_iota(jnp.int32, (1, n_sp), 1)

    def place_of_slab(slab):
        here = jnp.where(slab_of == slab, map_ref[...].astype(f32), 0.0)
        return jnp.sum(here, axis=1, keepdims=True)

    place = place_of_slab(me_sp)
    reach = win_ref[...].astype(f32)
    side_bias = []
    for side in (0, 1):
        apart = jnp.abs(place - place_of_slab(side_sp[side]))
        seen = (reach[0:1, 0:1] >= 1.0) & (reach[0:1, 1:2] >= apart)
        edge = jnp.where(has[side], 0.0, -1e30).astype(f32)
        side_bias.append(jnp.minimum(jnp.where(seen, 0.0, -1e30).astype(f32), edge))
    place_of = lax.broadcasted_iota(jnp.int32, (text, 1), 0)
    words = jnp.where(place_of < live_ref[0], 0.0, -1e30).astype(f32)
    bias_ref = r_["bias"]
    bias_ref[:tok] = jnp.zeros((tok, 1), f32)
    bias_ref[tok:near] = words
    for side in (0, 1):
        region = slice(near + side * tok, near + (side + 1) * tok)
        bias_ref[region] = jnp.broadcast_to(side_bias[side], (tok, 1))

    def cols(h):
        return slice(h * HD, (h + 1) * HD)

    def forward(h):
        c = cols(h)
        scores = factor * mm(keys[:, c], q_ref[:, c], NT) + bias_ref[...]
        top = jnp.max(scores, axis=0, keepdims=True)
        e = jnp.exp(scores - top)
        inv = 1.0 / jnp.sum(e, axis=0, keepdims=True)
        weights = e * inv
        wts[h] = weights
        att_t[c, :] = mm(vals[:, c], weights.astype(bf16), TN).astype(bf16)
        for side in (0, 1):
            st_out[side, h : h + 1, :] = top - side_bias[side]
            st_out[side, heads + h : heads + h + 1, :] = inv

    def far_weights(side, h):
        c = cols(h)
        scores = factor * mm(keys[:tok, c], qf[side, :, c], NT)
        e = jnp.exp(scores - st_in[side, h : h + 1, :])
        wfar[side, h] = e * st_in[side, heads + h : heads + h + 1, :]

    def core_owns(r):
        return ((blk(r) >> 1) & 1) == core

    def mine(r):
        return (blk(r) >> 1) == me_dp

    def s1_copy(r):
        return remote(
            g1_out.at[r], g1_in.at[r], r_["s1s"].at[0], r_["s1r"].at[r], {"dp": me_dp ^ 1}
        )

    def x_first(r):
        return r in (2, 6)

    def along_x(j):
        return {"sp": me_sp ^ j}

    def along_y(j):
        return {"dp": me_dp ^ (2 * (j & 1)), "sp": me_sp ^ (2 * (j & 2))}

    def place1(r):
        return x if x_first(r) else y

    def place2(r):
        return y if x_first(r) else x

    def gy_copy(r, j):
        where = along_x(j) if x_first(r) else along_y(j)
        return remote(
            gy_out.at[r, place1(r) ^ j],
            gy_in.at[r, j - 1],
            r_["gys"].at[0],
            r_["gyr"].at[r],
            where,
        )

    def gx_copy(r, j):
        where = along_y(j) if x_first(r) else along_x(j)
        return remote(
            gx_out.at[r, place2(r) ^ j],
            gx_in.at[r, j - 1],
            r_["gxs"].at[0],
            r_["gxr"].at[r],
            where,
        )

    def ag1_copy(r, j):
        piece_ = gall.at[r, x]
        return remote(piece_, piece_, r_["ag1s"].at[0], r_["ag1r"].at[r], along_x(j))

    def ag2_copy(r, i):
        return remote(
            gall.at[r],
            gfin.at[blk(r) & 1, y],
            r_["ag2s"].at[0],
            r_["ag2r"].at[r],
            {"dp": blk(r) >> 1, "sp": 4 * i + x},
        )

    def ag2_sends(r, i):
        return core_owns(r) & jnp.logical_not(mine(r) & (yh == i))

    def all_of(some, send, recv):
        return remote(some, some, send, recv, {"sp": me_sp ^ 4})

    def gw_part(r):
        parts[r] = mm(att_t[...], nat[r], NN)

        @pl.when(jnp.logical_not(core_owns(r)))
        def _():
            g1_out[r] = parts[r].astype(bf16)
            s1_copy(r).start()

    def gw_s1(r):
        @pl.when(core_owns(r))
        def _():
            s1_copy(r).wait_recv()
            for i in range(4):
                for k in range(4):
                    rows = slice((4 * i + k) * piece, (4 * i + k + 1) * piece)
                    total = parts[r, rows, :] + g1_in[r, rows, :].astype(f32)
                    parts[r, rows, :] = total
                    gy_out[r, i, k] = total.astype(bf16)
            for j in range(1, 4):
                gy_copy(r, j).start()

    def gw_sy(r):
        @pl.when(core_owns(r))
        def _():
            all_of(gy_in.at[r], r_["gys"].at[0], r_["gyr"].at[r]).wait_recv()
            for k in range(4):
                at = pl.multiple_of(place1(r) * (4 * piece) + k * piece, 8)
                total = parts[r, pl.ds(at, piece), :]
                for j in range(3):
                    total = total + gy_in[r, j, k].astype(f32)
                parts[r, k * piece : (k + 1) * piece, :] = total
                gx_out[r, k] = total.astype(bf16)
            for j in range(1, 4):
                gx_copy(r, j).start()

    def gw_sx(r):
        @pl.when(core_owns(r))
        def _():
            all_of(gx_in.at[r], r_["gxs"].at[0], r_["gxr"].at[r]).wait_recv()
            total = parts[r, pl.ds(pl.multiple_of(place2(r) * piece, 8), piece), :]
            for j in range(3):
                total = total + gx_in[r, j].astype(f32)
            gall[r, x] = total.astype(bf16)
            for j in range(1, 4):
                ag1_copy(r, j).start()

    def gw_ag(r):
        @pl.when(core_owns(r))
        def _():
            all_of(gx_in.at[0], r_["ag1s"].at[0], r_["ag1r"].at[r]).wait_recv()

        for i in (0, 1):

            @pl.when(ag2_sends(r, i))
            def _():
                ag2_copy(r, i).start()

        @pl.when(mine(r))
        def _():
            gfin[blk(r) & 1, y] = gall[r]

    gw_v = r_["gw_v"]

    def gw_end(r):
        @pl.when(mine(r))
        def _():
            all_of(gy_in.at[0], r_["ag2s"].at[0], r_["ag2r"].at[r]).wait_recv()
            at = pl.ds(pl.multiple_of((blk(r) & 1) * w, HD), w)
            for i in range(4):
                for k in range(4):
                    n = 4 * k + i if x_first(r) else 4 * i + k
                    rows = slice(n * piece, (n + 1) * piece)
                    gw_v[rows, at] = gfin[blk(r) & 1, i, k].astype(f32)

    trow = text // n_sp

    def tx_copy(j):
        return remote(
            tx_out.at[x ^ j], tx_in.at[j - 1], r_["txs"].at[0], r_["txr"].at[0], along_x(j)
        )

    def ty_copy():
        return remote(ty_out, ty_in, r_["tys"].at[0], r_["tyr"].at[0], {"sp": me_sp ^ 4})

    def tg_copy():
        slot = tg.at[x, yh]
        return remote(slot, slot, r_["tgs"].at[0], r_["tgr"].at[0], {"sp": me_sp ^ 4})

    def tz_copy(j):
        return remote(tg.at[x], tg.at[x], r_["tzs"].at[0], r_["tzr"].at[0], along_x(j))

    def text_1():
        all_of(tx_in, r_["txs"].at[0], r_["txr"].at[0]).wait_recv()

        def over_x(i):
            total = tx_out[x, i].astype(f32)
            for j in range(3):
                total = total + tx_in[j, i].astype(f32)
            return total

        ty_out[...] = over_x(1 - yh).astype(bf16)
        ty_copy().start()
        t_own[...] = over_x(yh)

    def text_2():
        ty_copy().wait_recv()
        tg[x, yh] = (t_own[...] + ty_in[...].astype(f32)).astype(bf16)
        tg_copy().start()

    def text_3():
        tg_copy().wait_recv()
        for j in range(1, 4):
            tz_copy(j).start()

    def text_4():
        all_of(tx_in, r_["tzs"].at[0], r_["tzr"].at[0]).wait_recv()
        for i in range(4):
            for k in range(2):
                rows = slice((2 * i + k) * trow, (2 * i + k + 1) * trow)
                gtk_v[rows] = tg[i, k, :trow]
                gtv_v[rows] = tg[i, k, trow:]

    gq_v, gk_v, gv_v, gtk_v, gtv_v = (r_[n] for n in ("gq_v", "gk_v", "gv_v", "gtk_v", "gtv_v"))

    def text_part(h):
        c = cols(h)
        ga = ga_t[c, :]
        wt = wts[h, tok:near, :]
        gp = mm(vals[tok:near, c], ga, NN)
        gs = (wt * (gp - dl_out[h : h + 1, :])).astype(bf16)
        gs_buf[h, tok:near, :] = gs
        gk = (factor * mm(gs, q_ref[:, c], NN)).astype(bf16)
        gv = mm(wt.astype(bf16), ga, NT).astype(bf16)
        for j in range(n_sp):
            rows = slice(j * trow, (j + 1) * trow)
            tx_out[j // 2, j % 2, :trow, c] = gk[rows]
            tx_out[j // 2, j % 2, trow:, c] = gv[rows]

    def own_part(h):
        c = cols(h)
        ga = ga_t[c, :]
        delta = dl_out[h : h + 1, :]
        for lo, hi in ((0, tok), (near, near + 2 * tok)):
            gp = mm(vals[lo:hi, c], ga, NN)
            gs_buf[h, lo:hi, :] = (wts[h, lo:hi, :] * (gp - delta)).astype(bf16)
        gq_v[:, c] = (factor * mm(keys[:, c], gs_buf[h], TN)).T.astype(bf16)
        gk_sum[:, c] = mm(gs_buf[h, :tok, :], q_ref[:, c], NN)
        gv_sum[:, c] = mm(wts[h, :tok, :].astype(bf16), ga, NT)

    def far_part(side, h):
        c = cols(h)
        ga = gaf[side, c, :]
        weights = wfar[side, h]
        gp = mm(vals[:tok, c], ga, NN)
        gs = (weights * (gp - dl_in[side, h : h + 1, :])).astype(bf16)
        gk_sum[:, c] += mm(gs, qf[side, :, c], NN)
        gv_sum[:, c] += mm(weights.astype(bf16), ga, NT)

    scale(0)
    z_arrive(0, 0)
    z_arrive(0, 1)
    scale(1)
    scale(7)
    halo_wait_both(("kv", 0))
    forward(0)
    z_arrive(1, 0)
    halo_wait_both(("kv", 1))
    forward(1)
    z_arrive(1, 1)
    scale(2)
    scale(6)
    w_core().wait_recv()
    w_y_all(1).wait_recv()
    w_fwd().start()
    halo_wait_both(("kv", 2))
    forward(2)
    halo_start([4 * heads])
    for r in (0, 1, 7):
        gw_part(r)
    z_arrive(2, 0)
    gw_s1(0)
    gw_s1(1)
    w_fwd().wait_recv()
    ga_add(0, True)
    gw_s1(7)
    for r in (2, 6):
        gw_part(r)
    ga_add(1)
    ga_add(7)
    ga_add(2)
    z_arrive(2, 1)
    ga_add(6)
    scale(3)
    scale(5)
    ga_add(3)
    ga_add(5)
    for r in (3, 5):
        gw_part(r)
    for r in (2, 6):
        gw_s1(r)
    z_arrive(3, 0)
    scale(4)
    gw_part(4)
    ga_add(4)
    ga_t[...] = acc[...].astype(bf16)
    for h in range(heads):
        c = cols(h)
        dl_out[h : h + 1, :] = jnp.sum(
            ga_t[c, :].astype(f32) * att_t[c, :].astype(f32), axis=0, keepdims=True
        )
    for r in (3, 5):
        gw_s1(r)
    for h in range(heads):
        text_part(h)
    gw_s1(4)
    for r in (0, 1, 7):
        gw_sy(r)
    for j in range(1, 4):
        tx_copy(j).start()
    for r in (2, 6):
        gw_sy(r)
    halo_start([4 * heads + 1, 3 * heads])
    own_part(0)
    for r in (0, 1, 7):
        gw_sx(r)
    for r in (3, 5):
        gw_sy(r)
    halo_start([3 * heads + 1])
    own_part(1)
    gw_sy(4)
    halo_start([3 * heads + 2])
    own_part(2)
    text_1()
    halo_wait_both(("st", 0), ("q", 0))
    for h in range(heads):
        for side in (0, 1):
            pl.when(has[side])(functools.partial(far_weights, side, h))
    for r in (2, 6):
        gw_sx(r)
    for r in (0, 1, 7):
        gw_ag(r)
    text_2()
    for r in (3, 5):
        gw_sx(r)

    def far_head(h):
        halo_wait_both(("ga", h))
        for side in (0, 1):
            pl.when(has[side])(functools.partial(far_part, side, h))
        c = cols(h)
        gk_v[:, c] = (factor * gk_sum[:, c]).astype(bf16)
        gv_v[:, c] = gv_sum[:, c].astype(bf16)

    halo_wait_both(("dl", 0))
    far_head(0)
    gw_sx(4)
    for r in (2, 6):
        gw_ag(r)
    far_head(1)
    for r in (3, 5):
        gw_ag(r)
    text_3()
    gw_ag(4)
    far_head(2)
    text_4()
    for r in (0, 1, 7, 2, 6, 3, 5, 4):
        gw_end(r)

    all_of(raw.at[pl.ds(0, n_tp - 1)], r_["zs"].at[0], r_["zr"].at[0, 0, 0]).wait_send()
    w_core().wait_send()

    @pl.when(jnp.logical_not(ends))
    def _():
        w_y_all(1).wait_send()

    @pl.when(ends & gives)
    def _():
        w_y_all(2).wait_send()

    w_fwd().wait_send()
    for side in (0, 1):

        @pl.when(has[side])
        def _():
            blocks = raw.at[pl.ds(0, 4)]
            remote(
                blocks, blocks, r_["hs"].at[side, 0], r_["hr"].at[side, 0], {"sp": side_sp[side]}
            ).wait_send()
            halo(side, 4 * heads).wait_send()
            halo(side, 4 * heads + 1).wait_send()

    for some, n in (
        (g1_out.at[pl.ds(0, 4)], "s1"),
        (gy_in.at[pl.ds(0, 4)], "gy"),
        (gx_in.at[pl.ds(0, 4)], "gx"),
        (gx_in.at[pl.ds(0, 4)], "ag1"),
        (gy_in.at[pl.ds(0, 2)], "ag2"),
        (tx_in, "tx"),
        (ty_out, "ty"),
        (ty_out, "tg"),
        (tx_in, "tz"),
    ):
        all_of(some, r_[n + "s"].at[0], r_[n + "r"].at[0]).wait_send()


def call(q, k, v, tk, tv, s, w, gate, windows, tile_map, text_count):
    tok, width = q.shape
    text = tk.shape[0]
    heads = width // HD
    cols = w.shape[1]
    hbm = pl.BlockSpec(memory_space=pltpu.HBM)
    total = 3 * tok + text
    block = s.shape[1]
    piece = width // 16
    sm = pl.BlockSpec(memory_space=pltpu.SMEM)
    vm = pl.BlockSpec(memory_space=pltpu.VMEM)
    outs = [
        ("gq", (tok, width), bf16),
        ("gk", (tok, width), bf16),
        ("gv", (tok, width), bf16),
        ("gtk", (text, width), bf16),
        ("gtv", (text, width), bf16),
        ("gw", (width, cols), f32),
    ]
    scratch = [
        ("q_v", (tok, width), bf16),
        ("s_v", (tok, block), bf16),
        ("keys", (total, width), bf16),
        ("vals", (total, width), bf16),
        ("qf", (2, tok, width), bf16),
        ("gaf", (2, width, tok), bf16),
        ("st_out", (2, 8, tok), f32),
        ("st_in", (2, 8, tok), f32),
        ("dl_out", (8, tok), f32),
        ("dl_in", (2, 8, tok), f32),
        ("bias", (total, 1), f32),
        ("raw", (8, tok, block), bf16),
        ("nat", (8, tok, block), bf16),
        ("w_all", (4, width, cols), bf16),
        ("acc", (width, tok), f32),
        ("ga_t", (width, tok), bf16),
        ("att_t", (width, tok), bf16),
        ("wts", (heads, total, tok), f32),
        ("wfar", (2, heads, tok, tok), f32),
        ("gs_buf", (heads, total, tok), bf16),
        ("gk_sum", (tok, width), f32),
        ("gv_sum", (tok, width), f32),
        ("parts", (8, width, block), f32),
        ("g1_out", (8, width, block), bf16),
        ("g1_in", (8, width, block), bf16),
        ("gy_out", (8, 4, 4, piece, block), bf16),
        ("gy_in", (8, 3, 4, piece, block), bf16),
        ("gx_out", (8, 4, piece, block), bf16),
        ("gx_in", (8, 3, piece, block), bf16),
        ("gall", (8, 4, piece, block), bf16),
        ("gfin", (2, 4, 4, piece, block), bf16),
        ("tx_out", (4, 2, text // 4, width), bf16),
        ("tx_in", (3, 2, text // 4, width), bf16),
        ("ty_out", (text // 4, width), bf16),
        ("ty_in", (text // 4, width), bf16),
        ("t_own", (text // 4, width), f32),
        ("tg", (4, 2, text // 4, width), bf16),
    ]
    sems = [
        ("zs", (1,)),
        ("zr", (2, 4, 2)),
        ("ws", (3,)),
        ("wr", (3,)),
        ("hs", (2, 3)),
        ("hr", (2, 2 * heads + 3)),
        ("s1s", (1,)),
        ("s1r", (8,)),
        ("gys", (1,)),
        ("gyr", (8,)),
        ("gxs", (1,)),
        ("gxr", (8,)),
        ("ag1s", (1,)),
        ("ag1r", (8,)),
        ("ag2s", (1,)),
        ("ag2r", (8,)),
        ("txs", (1,)),
        ("txr", (1,)),
        ("tys", (1,)),
        ("tyr", (1,)),
        ("tzs", (1,)),
        ("tzr", (1,)),
        ("tgs", (1,)),
        ("tgr", (1,)),
        ("ls", (7,)),
    ]
    args = ["q", "k", "v", "tk", "tv", "s", "w", "gate", "win", "map", "live"]
    names = args + [n + "_v" for n, _, _ in outs] + [n for n, _, _ in scratch]
    names += [n for n, _ in sems]
    return pl.pallas_call(
        functools.partial(kernel, tuple(names)),
        out_shape=[pltpu.VMEM(a, b) for _, a, b in outs],
        in_specs=[hbm] * 7 + [vm] * 3 + [sm],
        out_specs=[vm] * len(outs),
        scratch_shapes=[pltpu.VMEM(a, b) for _, a, b in scratch]
        + [pltpu.SemaphoreType.DMA(n) for _, n in sems],
        compiler_params=pltpu.CompilerParams(
            collective_id=0, has_side_effects=True, vmem_limit_bytes=56 << 20
        ),
        name="attention_backward",
    )(q, k, v, tk, tv, s, w, gate, windows, tile_map, text_count)


def copy_kernel(n, *refs):
    srcs, dsts, sem = refs[:n], refs[n : 2 * n], refs[2 * n]
    stores = [pltpu.make_async_copy(srcs[i], dsts[i], sem.at[i]) for i in range(n)]
    for c in stores:
        c.start()
    for c in stores:
        c.wait()


def copy_call(arrays):
    n = len(arrays)
    return pl.pallas_call(
        functools.partial(copy_kernel, n),
        out_shape=[jax.ShapeDtypeStruct(a.shape, a.dtype) for a in arrays],
        in_specs=[pl.BlockSpec(memory_space=pltpu.VMEM)] * n,
        out_specs=[pl.BlockSpec(memory_space=pltpu.HBM)] * n,
        scratch_shapes=[pltpu.SemaphoreType.DMA((n,))],
        compiler_params=pltpu.CompilerParams(vmem_limit_bytes=4 << 20),
        name="results",
    )(*arrays)


def per_device(
    query,
    key,
    value,
    text_key,
    text_value,
    grad_out,
    gate,
    out_weight,
    windows,
    tile_map,
    text_count,
):
    outs = call(
        query[0],
        key[0],
        value[0],
        text_key[0],
        text_value[0],
        grad_out[0],
        out_weight,
        gate,
        windows,
        tile_map.T,
        text_count,
    )
    outs = copy_call(outs)
    return tuple(o[None] for o in outs[:5]) + (outs[5],)


def solution(mesh):
    placed = (
        P("dp", "sp", "tp"),
        P("dp", "sp", "tp"),
        P("dp", "sp", "tp"),
        P("dp", None, "tp"),
        P("dp", None, "tp"),
        P("dp", "sp", "tp"),
        P("dp", None),
        P("tp", "dp"),
        P("sp", None),
        P(),
        P("dp"),
    )
    return jax.shard_map(
        per_device,
        mesh=mesh,
        in_specs=placed,
        out_specs=(
            P("dp", "sp", "tp"),
            P("dp", "sp", "tp"),
            P("dp", "sp", "tp"),
            P("dp", None, "tp"),
            P("dp", None, "tp"),
            P("tp", "dp"),
        ),
        check_vma=False,
    )
```

```python
import functools

import jax
import jax.numpy as jnp
from jax import lax
from jax.experimental import pallas as pl
from jax.experimental.pallas import tpu as pltpu
from jax.sharding import PartitionSpec as P

HD = 128
VMEM = 67043328
MESH = pl.DeviceIdType.MESH

NT = (((1,), (1,)), ((), ()))
NN = (((1,), (0,)), ((), ()))
TN = (((0,), (0,)), ((), ()))

bf16, f32 = jnp.bfloat16, jnp.float32


def mm(a, b, dims):
    return lax.dot_general(a, b, dims, preferred_element_type=f32)


def item_k(h):
    return 3 * h


def item_v(h):
    return 3 * h + 1


def item_q(h):
    return 3 * h + 2


def kernel(
    names,
    *refs,
):
    r_ = dict(zip(names, refs, strict=True))
    q_ref, s_ref, gate_ref, win_ref = (r_[n] for n in ("q_v", "s_v", "gate", "win"))
    map_ref, live_ref = r_["map"], r_["live"]
    keys, vals, qf, gaf = r_["keys"], r_["vals"], r_["qf"], r_["gaf"]
    st_out, st_in, dl_out, dl_in = r_["st_out"], r_["st_in"], r_["dl_out"], r_["dl_in"]
    raw, nat, w_all, acc = r_["raw"], r_["nat"], r_["w_all"], r_["acc"]
    ga_t, att_t, wts, wfar, gs_buf = r_["ga_t"], r_["att_t"], r_["wts"], r_["wfar"], r_["gs_buf"]
    parts, g1_out, g1_in = r_["parts"], r_["g1_out"], r_["g1_in"]
    gy_out, gy_in, gx_out, gx_in = r_["gy_out"], r_["gy_in"], r_["gx_out"], r_["gx_in"]
    gall, gfin = r_["gall"], r_["gfin"]
    tx_out, tx_in, tg = r_["tx_out"], r_["tx_in"], r_["tg"]
    ty_out, ty_in, t_own = r_["ty_out"], r_["ty_in"], r_["t_own"]
    gk_sum, gv_sum = r_["gk_sum"], r_["gv_sum"]

    factor = HD ** (-0.5)
    tok, width = q_ref.shape
    text = r_["tk"].shape[0]
    heads = width // HD
    near = tok + text
    n_tp = n_sp = 8
    me_sp = lax.axis_index("sp")
    me_dp = lax.axis_index("dp")
    me_tp = lax.axis_index("tp")
    x = me_sp & 3
    yh = me_sp >> 2
    core = me_dp & 1
    yl = me_dp >> 1
    w = s_ref.shape[1]
    piece = width // 16
    y = 2 * yh + yl
    half = width // 2
    has = [me_sp >= 1, me_sp + 1 < n_sp]
    side_sp = [me_sp - 1, me_sp + 1]

    partners = [{"tp": (me_tp + 1) & 7}, {"tp": (me_tp + 7) & 7}]
    partners += [{"dp": me_dp ^ 1}, {"dp": me_dp ^ 2}, {"dp": me_dp ^ 2, "sp": me_sp ^ 4}]
    partners += [{"sp": me_sp ^ j} for j in range(1, n_sp)]
    barrier = pltpu.get_barrier_semaphore()
    for where in partners:
        pl.semaphore_signal(barrier, inc=1, device_id=where, device_id_type=MESH)

    w_ref = w_all.at[me_dp]
    loads = {
        n: pltpu.make_async_copy(r_[n], to, r_["ls"].at[i])
        for i, (n, to) in enumerate(
            [
                ("s", s_ref),
                ("w", w_ref),
                ("k", keys.at[pl.ds(0, tok)]),
                ("v", vals.at[pl.ds(0, tok)]),
                ("q", q_ref),
                ("tk", keys.at[pl.ds(tok, text)]),
                ("tv", vals.at[pl.ds(tok, text)]),
            ]
        )
    }
    for c in loads.values():
        c.start()
    pl.semaphore_wait(barrier, len(partners))

    def remote(src, dst, send, recv, where):
        return pltpu.make_async_remote_copy(
            src_ref=src,
            dst_ref=dst,
            send_sem=send,
            recv_sem=recv,
            device_id=where,
            device_id_type=MESH,
        )

    chunk = tok // 2

    def crow(c):
        return pl.ds(c * chunk, chunk)

    def z_copy(up, t, c):
        r = (8 - t) % 8 if up else t
        to = (r + 7) % 8 if up else (r + 1) % 8
        src = s_ref.at[crow(c)] if t == 0 else raw.at[r, crow(c)]
        send = r_["zs"].at[0]
        recv = r_["zr"].at[0 if up else 1, t, c]
        where = {"tp": (me_tp + (1 if up else 7)) & 7}
        return remote(src, raw.at[to, crow(c)], send, recv, where)

    def z_exists(up, t, c):
        return t < 3 or (t == 3 and c == (0 if up else 1))

    def z_arrive(t, i):
        for up in (True, False):
            c = i if up else 1 - i
            if z_exists(up, t, c):
                z_copy(up, t, c).wait_recv()
                if t < 3 and z_exists(up, t + 1, c):
                    z_copy(up, t + 1, c).start()

    def w_core():
        return remote(w_ref, w_all.at[me_dp], r_["ws"].at[0], r_["wr"].at[0], {"dp": me_dp ^ 1})

    ends = (x == 0) | (x == 3)
    gives = jnp.where(x == 0, yh == 1, yh == 0)

    def w_y(i, j):
        rows = pl.ds(j * half, half)
        where = {"dp": me_dp ^ 2, "sp": me_sp ^ (4 * i)}
        return remote(
            w_ref.at[rows],
            w_all.at[me_dp, rows],
            r_["ws"].at[1],
            r_["wr"].at[1],
            where,
        )

    def w_y_all(n):
        held = w_all.at[pl.ds(0, n)]
        return remote(held, held, r_["ws"].at[1], r_["wr"].at[1], {"dp": me_dp ^ 2})

    def w_fwd():
        block = w_all.at[me_dp ^ 2]
        return remote(block, block, r_["ws"].at[2], r_["wr"].at[2], {"dp": me_dp ^ 1})

    def halo(side, item):
        there = 1 - side
        region = pl.ds(near + there * tok, tok)
        if item < 3 * heads:
            h, kind = divmod(item, 3)
            c = pl.ds(h * HD, HD)
            src = (keys.at[pl.ds(0, tok), c], vals.at[pl.ds(0, tok), c], q_ref.at[:, c])[kind]
            dst = (keys.at[region, c], vals.at[region, c], qf.at[there, :, c])[kind]
        elif item < 4 * heads:
            c = pl.ds((item - 3 * heads) * HD, HD)
            src, dst = ga_t.at[c], gaf.at[there, c]
        elif item == 4 * heads:
            src, dst = st_out.at[side], st_in.at[there]
        else:
            src, dst = dl_out, dl_in.at[there]
        if item < 4 * heads:
            send = 0
            got = (h if kind < 2 else heads) if item < 3 * heads else item - 2 * heads + 1
        else:
            send = 1 + item - 4 * heads
            got = item - 2 * heads + 1
        return remote(
            src, dst, r_["hs"].at[side, send], r_["hr"].at[there, got], {"sp": side_sp[side]}
        )

    def halo_start(items):
        for side in (0, 1):

            @pl.when(has[side])
            def _():
                for item in items:
                    halo(side, item).start()

    def halo_wait(side, what):
        kind, h = what
        if kind in ("st", "dl"):
            halo(1 - side, 4 * heads + (kind == "dl")).wait_recv()
        elif kind == "ga":
            halo(1 - side, 3 * heads + h).wait_recv()
        else:
            some = keys.at[pl.ds(0, 2 * tok), pl.ds(0, HD)] if kind == "kv" else qf.at[side]
            got = r_["hr"].at[side, h if kind == "kv" else heads]
            remote(some, some, r_["hs"].at[side, 0], got, {"sp": me_sp ^ 1}).wait_recv()

    def halo_wait_both(*whats):
        for side in (0, 1):

            @pl.when(has[side])
            def _():
                for what in whats:
                    halo_wait(side, what)

    loads["s"].wait()
    for c in (0, 1):
        z_copy(True, 0, c).start()
        z_copy(False, 0, 1 - c).start()
    loads["w"].wait()
    w_core().start()

    @pl.when(jnp.logical_not(ends))
    def _():
        w_y(0, 0).start()
        w_y(1, 1).start()

    @pl.when(ends & gives)
    def _():
        for i in (0, 1):
            for j in (0, 1):
                w_y(i, j).start()

    loads["k"].wait()
    loads["v"].wait()
    for h in range(heads):
        halo_start([item_k(h), item_v(h)])
    loads["q"].wait()
    for h in range(heads):
        halo_start([item_q(h)])
    loads["tk"].wait()
    loads["tv"].wait()
    for side in (0, 1):

        @pl.when(jnp.logical_not(has[side]))
        def _():
            region = slice(near + side * tok, near + (side + 1) * tok)
            keys[region] = jnp.zeros((tok, width), bf16)
            vals[region] = jnp.zeros((tok, width), bf16)

    def blk(r):
        return (me_tp + r) & 7

    def scale(r):
        gate = gate_ref[:, pl.ds(pl.multiple_of(blk(r) * w, HD), w)].astype(f32)
        src = s_ref[...] if r == 0 else raw[r]
        nat[r] = (src.astype(f32) * gate).astype(bf16)

    def ga_add(r, first=False):
        at = pl.multiple_of((blk(r) & 1) * w, HD)
        term = mm(w_all[blk(r) >> 1, :, pl.ds(at, w)], nat[r], NT)
        if first:
            acc[...] = term
        else:
            acc[...] += term

    slab_of = lax.broadcasted_iota(jnp.int32, (1, n_sp), 1)

    def place_of_slab(slab):
        here = jnp.where(slab_of == slab, map_ref[...].astype(f32), 0.0)
        return jnp.sum(here, axis=1, keepdims=True)

    place = place_of_slab(me_sp)
    reach = win_ref[...].astype(f32)
    side_bias = []
    for side in (0, 1):
        apart = jnp.abs(place - place_of_slab(side_sp[side]))
        seen = (reach[0:1, 0:1] >= 1.0) & (reach[0:1, 1:2] >= apart)
        edge = jnp.where(has[side], 0.0, -1e30).astype(f32)
        side_bias.append(jnp.minimum(jnp.where(seen, 0.0, -1e30).astype(f32), edge))
    place_of = lax.broadcasted_iota(jnp.int32, (text, 1), 0)
    words = jnp.where(place_of < live_ref[0], 0.0, -1e30).astype(f32)
    bias_ref = r_["bias"]
    bias_ref[:tok] = jnp.zeros((tok, 1), f32)
    bias_ref[tok:near] = words
    for side in (0, 1):
        region = slice(near + side * tok, near + (side + 1) * tok)
        bias_ref[region] = jnp.broadcast_to(side_bias[side], (tok, 1))

    def cols(h):
        return slice(h * HD, (h + 1) * HD)

    def forward(h):
        c = cols(h)
        scores = factor * mm(keys[:, c], q_ref[:, c], NT) + bias_ref[...]
        top = jnp.max(scores, axis=0, keepdims=True)
        e = jnp.exp(scores - top)
        inv = 1.0 / jnp.sum(e, axis=0, keepdims=True)
        weights = e * inv
        wts[h] = weights
        att_t[c, :] = mm(vals[:, c], weights.astype(bf16), TN).astype(bf16)
        for side in (0, 1):
            st_out[side, h : h + 1, :] = top - side_bias[side]
            st_out[side, heads + h : heads + h + 1, :] = inv

    def far_weights(side, h):
        c = cols(h)
        scores = factor * mm(keys[:tok, c], qf[side, :, c], NT)
        e = jnp.exp(scores - st_in[side, h : h + 1, :])
        wfar[side, h] = e * st_in[side, heads + h : heads + h + 1, :]

    def core_owns(r):
        return ((blk(r) >> 1) & 1) == core

    def mine(r):
        return (blk(r) >> 1) == me_dp

    def s1_copy(r):
        return remote(
            g1_out.at[r], g1_in.at[r], r_["s1s"].at[0], r_["s1r"].at[r], {"dp": me_dp ^ 1}
        )

    def x_first(r):
        return r in (2, 6)

    def along_x(j):
        return {"sp": me_sp ^ j}

    def along_y(j):
        return {"dp": me_dp ^ (2 * (j & 1)), "sp": me_sp ^ (2 * (j & 2))}

    def place1(r):
        return x if x_first(r) else y

    def place2(r):
        return y if x_first(r) else x

    def gy_copy(r, j):
        where = along_x(j) if x_first(r) else along_y(j)
        return remote(
            gy_out.at[r, place1(r) ^ j],
            gy_in.at[r, j - 1],
            r_["gys"].at[0],
            r_["gyr"].at[r],
            where,
        )

    def gx_copy(r, j):
        where = along_y(j) if x_first(r) else along_x(j)
        return remote(
            gx_out.at[r, place2(r) ^ j],
            gx_in.at[r, j - 1],
            r_["gxs"].at[0],
            r_["gxr"].at[r],
            where,
        )

    def ag1_copy(r, j):
        piece_ = gall.at[r, x]
        return remote(piece_, piece_, r_["ag1s"].at[0], r_["ag1r"].at[r], along_x(j))

    def ag2_copy(r, i):
        return remote(
            gall.at[r],
            gfin.at[blk(r) & 1, y],
            r_["ag2s"].at[0],
            r_["ag2r"].at[r],
            {"dp": blk(r) >> 1, "sp": 4 * i + x},
        )

    def ag2_sends(r, i):
        return core_owns(r) & jnp.logical_not(mine(r) & (yh == i))

    def all_of(some, send, recv):
        return remote(some, some, send, recv, {"sp": me_sp ^ 4})

    def gw_part(r):
        parts[r] = mm(att_t[...], nat[r], NN)

        @pl.when(jnp.logical_not(core_owns(r)))
        def _():
            g1_out[r] = parts[r].astype(bf16)
            s1_copy(r).start()

    def gw_s1(r):
        @pl.when(core_owns(r))
        def _():
            s1_copy(r).wait_recv()
            for i in range(4):
                for k in range(4):
                    rows = slice((4 * i + k) * piece, (4 * i + k + 1) * piece)
                    total = parts[r, rows, :] + g1_in[r, rows, :].astype(f32)
                    parts[r, rows, :] = total
                    gy_out[r, i, k] = total.astype(bf16)
            for j in range(1, 4):
                gy_copy(r, j).start()

    def gw_sy(r):
        @pl.when(core_owns(r))
        def _():
            all_of(gy_in.at[r], r_["gys"].at[0], r_["gyr"].at[r]).wait_recv()
            for k in range(4):
                at = pl.multiple_of(place1(r) * (4 * piece) + k * piece, 8)
                total = parts[r, pl.ds(at, piece), :]
                for j in range(3):
                    total = total + gy_in[r, j, k].astype(f32)
                parts[r, k * piece : (k + 1) * piece, :] = total
                gx_out[r, k] = total.astype(bf16)
            for j in range(1, 4):
                gx_copy(r, j).start()

    def gw_sx(r):
        @pl.when(core_owns(r))
        def _():
            all_of(gx_in.at[r], r_["gxs"].at[0], r_["gxr"].at[r]).wait_recv()
            total = parts[r, pl.ds(pl.multiple_of(place2(r) * piece, 8), piece), :]
            for j in range(3):
                total = total + gx_in[r, j].astype(f32)
            gall[r, x] = total.astype(bf16)
            for j in range(1, 4):
                ag1_copy(r, j).start()

    def gw_ag(r):
        @pl.when(core_owns(r))
        def _():
            all_of(gx_in.at[0], r_["ag1s"].at[0], r_["ag1r"].at[r]).wait_recv()

        for i in (0, 1):

            @pl.when(ag2_sends(r, i))
            def _():
                ag2_copy(r, i).start()

        @pl.when(mine(r))
        def _():
            gfin[blk(r) & 1, y] = gall[r]

    gw_v = r_["gw_v"]

    def gw_end(r):
        @pl.when(mine(r))
        def _():
            all_of(gy_in.at[0], r_["ag2s"].at[0], r_["ag2r"].at[r]).wait_recv()
            at = pl.ds(pl.multiple_of((blk(r) & 1) * w, HD), w)
            for i in range(4):
                for k in range(4):
                    n = 4 * k + i if x_first(r) else 4 * i + k
                    rows = slice(n * piece, (n + 1) * piece)
                    gw_v[rows, at] = gfin[blk(r) & 1, i, k].astype(f32)

    trow = text // n_sp

    def tx_copy(j):
        return remote(
            tx_out.at[x ^ j], tx_in.at[j - 1], r_["txs"].at[0], r_["txr"].at[0], along_x(j)
        )

    def ty_copy():
        return remote(ty_out, ty_in, r_["tys"].at[0], r_["tyr"].at[0], {"sp": me_sp ^ 4})

    def tg_copy():
        slot = tg.at[x, yh]
        return remote(slot, slot, r_["tgs"].at[0], r_["tgr"].at[0], {"sp": me_sp ^ 4})

    def tz_copy(i, j):
        slot = tg.at[x, i]
        return remote(slot, slot, r_["tzs"].at[0], r_["tzr"].at[0], along_x(j))

    def text_1():
        all_of(tx_in, r_["txs"].at[0], r_["txr"].at[0]).wait_recv()

        def over_x(i):
            total = tx_out[x, i].astype(f32)
            for j in range(3):
                total = total + tx_in[j, i].astype(f32)
            return total

        ty_out[...] = over_x(1 - yh).astype(bf16)
        ty_copy().start()
        t_own[...] = over_x(yh)

    def text_2():
        ty_copy().wait_recv()
        tg[x, yh] = (t_own[...] + ty_in[...].astype(f32)).astype(bf16)
        tg_copy().start()
        for j in range(1, 4):
            tz_copy(yh, j).start()

    def text_3():
        tg_copy().wait_recv()
        for j in range(1, 4):
            tz_copy(1 - yh, j).start()

    def text_4():
        all_of(tx_in, r_["tzs"].at[0], r_["tzr"].at[0]).wait_recv()
        for i in range(4):
            for k in range(2):
                rows = slice((2 * i + k) * trow, (2 * i + k + 1) * trow)
                gtk_v[rows] = tg[i, k, :trow]
                gtv_v[rows] = tg[i, k, trow:]

    gq_v, gk_v, gv_v, gtk_v, gtv_v = (r_[n] for n in ("gq_v", "gk_v", "gv_v", "gtk_v", "gtv_v"))

    def text_part(h):
        c = cols(h)
        ga = ga_t[c, :]
        wt = wts[h, tok:near, :]
        gp = mm(vals[tok:near, c], ga, NN)
        gs = (wt * (gp - dl_out[h : h + 1, :])).astype(bf16)
        gs_buf[h, tok:near, :] = gs
        gk = (factor * mm(gs, q_ref[:, c], NN)).astype(bf16)
        gv = mm(wt.astype(bf16), ga, NT).astype(bf16)
        for j in range(n_sp):
            rows = slice(j * trow, (j + 1) * trow)
            tx_out[j // 2, j % 2, :trow, c] = gk[rows]
            tx_out[j // 2, j % 2, trow:, c] = gv[rows]

    def own_part(h):
        c = cols(h)
        ga = ga_t[c, :]
        delta = dl_out[h : h + 1, :]
        for lo, hi in ((0, tok), (near, near + 2 * tok)):
            gp = mm(vals[lo:hi, c], ga, NN)
            gs_buf[h, lo:hi, :] = (wts[h, lo:hi, :] * (gp - delta)).astype(bf16)
        gq_v[:, c] = (factor * mm(keys[:, c], gs_buf[h], TN)).T.astype(bf16)
        gk_sum[:, c] = mm(gs_buf[h, :tok, :], q_ref[:, c], NN)
        gv_sum[:, c] = mm(wts[h, :tok, :].astype(bf16), ga, NT)

    def far_part(side, h):
        c = cols(h)
        ga = gaf[side, c, :]
        weights = wfar[side, h]
        gp = mm(vals[:tok, c], ga, NN)
        gs = (weights * (gp - dl_in[side, h : h + 1, :])).astype(bf16)
        gk_sum[:, c] += mm(gs, qf[side, :, c], NN)
        gv_sum[:, c] += mm(weights.astype(bf16), ga, NT)

    scale(0)
    z_arrive(0, 0)
    z_arrive(0, 1)
    scale(1)
    scale(7)
    halo_wait_both(("kv", 0))
    forward(0)
    z_arrive(1, 0)
    halo_wait_both(("kv", 1))
    forward(1)
    z_arrive(1, 1)
    scale(2)
    scale(6)
    w_core().wait_recv()
    w_y_all(1).wait_recv()
    w_fwd().start()
    halo_wait_both(("kv", 2))
    forward(2)
    halo_start([4 * heads])
    for r in (0, 1, 7):
        gw_part(r)
    z_arrive(2, 0)
    gw_s1(0)
    gw_s1(1)
    w_fwd().wait_recv()
    ga_add(0, True)
    gw_s1(7)
    for r in (2, 6):
        gw_part(r)
    ga_add(1)
    ga_add(7)
    ga_add(2)
    z_arrive(2, 1)
    ga_add(6)
    scale(3)
    scale(5)
    ga_add(3)
    ga_add(5)
    for r in (3, 5):
        gw_part(r)
    for r in (2, 6):
        gw_s1(r)
    z_arrive(3, 0)
    scale(4)
    gw_part(4)
    ga_add(4)
    ga_t[...] = acc[...].astype(bf16)
    for h in range(heads):
        c = cols(h)
        dl_out[h : h + 1, :] = jnp.sum(
            ga_t[c, :].astype(f32) * att_t[c, :].astype(f32), axis=0, keepdims=True
        )
    for r in (3, 5):
        gw_s1(r)
    for h in range(heads):
        text_part(h)
    gw_s1(4)
    for r in (0, 1, 7):
        gw_sy(r)
    def far_head(h):
        halo_wait_both(("ga", h))
        for side in (0, 1):
            pl.when(has[side])(functools.partial(far_part, side, h))
        c = cols(h)
        gk_v[:, c] = (factor * gk_sum[:, c]).astype(bf16)
        gv_v[:, c] = gv_sum[:, c].astype(bf16)

    for j in range(1, 4):
        tx_copy(j).start()
    for r in (2, 6):
        gw_sy(r)
    own_part(0)
    for r in (0, 1, 7):
        gw_sx(r)
    for r in (3, 5):
        gw_sy(r)
    halo_start([4 * heads + 1, 3 * heads])
    own_part(1)
    gw_sy(4)
    own_part(2)
    halo_start([3 * heads + 1])
    for r in (2, 6):
        gw_sx(r)
    text_1()
    halo_wait_both(("st", 0), ("q", 0))
    for h in range(heads):
        for side in (0, 1):
            pl.when(has[side])(functools.partial(far_weights, side, h))
    for r in (3, 5):
        gw_sx(r)
    gw_sx(4)
    halo_start([3 * heads + 2])
    text_2()
    for r in (0, 1, 7):
        gw_ag(r)
    for r in (2, 6):
        gw_ag(r)
    halo_wait_both(("dl", 0))
    far_head(0)
    for r in (3, 5):
        gw_ag(r)
    gw_ag(4)
    text_3()
    far_head(1)
    far_head(2)
    text_4()
    for r in (0, 1, 7, 2, 6, 3, 5, 4):
        gw_end(r)

    all_of(raw.at[pl.ds(0, n_tp - 1)], r_["zs"].at[0], r_["zr"].at[0, 0, 0]).wait_send()
    w_core().wait_send()

    @pl.when(jnp.logical_not(ends))
    def _():
        w_y_all(1).wait_send()

    @pl.when(ends & gives)
    def _():
        w_y_all(2).wait_send()

    w_fwd().wait_send()
    for side in (0, 1):

        @pl.when(has[side])
        def _():
            blocks = raw.at[pl.ds(0, 4)]
            remote(
                blocks, blocks, r_["hs"].at[side, 0], r_["hr"].at[side, 0], {"sp": side_sp[side]}
            ).wait_send()
            halo(side, 4 * heads).wait_send()
            halo(side, 4 * heads + 1).wait_send()

    for some, n in (
        (g1_out.at[pl.ds(0, 4)], "s1"),
        (gy_in.at[pl.ds(0, 4)], "gy"),
        (gx_in.at[pl.ds(0, 4)], "gx"),
        (gx_in.at[pl.ds(0, 4)], "ag1"),
        (gy_in.at[pl.ds(0, 2)], "ag2"),
        (tx_in, "tx"),
        (ty_out, "ty"),
        (ty_out, "tg"),
        (tx_in, "tz"),
    ):
        all_of(some, r_[n + "s"].at[0], r_[n + "r"].at[0]).wait_send()


def call(q, k, v, tk, tv, s, w, gate, windows, tile_map, text_count):
    tok, width = q.shape
    text = tk.shape[0]
    heads = width // HD
    cols = w.shape[1]
    hbm = pl.BlockSpec(memory_space=pltpu.HBM)
    total = 3 * tok + text
    block = s.shape[1]
    piece = width // 16
    sm = pl.BlockSpec(memory_space=pltpu.SMEM)
    vm = pl.BlockSpec(memory_space=pltpu.VMEM)
    outs = [
        ("gq", (tok, width), bf16),
        ("gk", (tok, width), bf16),
        ("gv", (tok, width), bf16),
        ("gtk", (text, width), bf16),
        ("gtv", (text, width), bf16),
        ("gw", (width, cols), f32),
    ]
    scratch = [
        ("q_v", (tok, width), bf16),
        ("s_v", (tok, block), bf16),
        ("keys", (total, width), bf16),
        ("vals", (total, width), bf16),
        ("qf", (2, tok, width), bf16),
        ("gaf", (2, width, tok), bf16),
        ("st_out", (2, 8, tok), f32),
        ("st_in", (2, 8, tok), f32),
        ("dl_out", (8, tok), f32),
        ("dl_in", (2, 8, tok), f32),
        ("bias", (total, 1), f32),
        ("raw", (8, tok, block), bf16),
        ("nat", (8, tok, block), bf16),
        ("w_all", (4, width, cols), bf16),
        ("acc", (width, tok), f32),
        ("ga_t", (width, tok), bf16),
        ("att_t", (width, tok), bf16),
        ("wts", (heads, total, tok), f32),
        ("wfar", (2, heads, tok, tok), f32),
        ("gs_buf", (heads, total, tok), bf16),
        ("gk_sum", (tok, width), f32),
        ("gv_sum", (tok, width), f32),
        ("parts", (8, width, block), f32),
        ("g1_out", (8, width, block), bf16),
        ("g1_in", (8, width, block), bf16),
        ("gy_out", (8, 4, 4, piece, block), bf16),
        ("gy_in", (8, 3, 4, piece, block), bf16),
        ("gx_out", (8, 4, piece, block), bf16),
        ("gx_in", (8, 3, piece, block), bf16),
        ("gall", (8, 4, piece, block), bf16),
        ("gfin", (2, 4, 4, piece, block), bf16),
        ("tx_out", (4, 2, text // 4, width), bf16),
        ("tx_in", (3, 2, text // 4, width), bf16),
        ("ty_out", (text // 4, width), bf16),
        ("ty_in", (text // 4, width), bf16),
        ("t_own", (text // 4, width), f32),
        ("tg", (4, 2, text // 4, width), bf16),
    ]
    sems = [
        ("zs", (1,)),
        ("zr", (2, 4, 2)),
        ("ws", (3,)),
        ("wr", (3,)),
        ("hs", (2, 3)),
        ("hr", (2, 2 * heads + 3)),
        ("s1s", (1,)),
        ("s1r", (8,)),
        ("gys", (1,)),
        ("gyr", (8,)),
        ("gxs", (1,)),
        ("gxr", (8,)),
        ("ag1s", (1,)),
        ("ag1r", (8,)),
        ("ag2s", (1,)),
        ("ag2r", (8,)),
        ("txs", (1,)),
        ("txr", (1,)),
        ("tys", (1,)),
        ("tyr", (1,)),
        ("tzs", (1,)),
        ("tzr", (1,)),
        ("tgs", (1,)),
        ("tgr", (1,)),
        ("ls", (7,)),
    ]
    args = ["q", "k", "v", "tk", "tv", "s", "w", "gate", "win", "map", "live"]
    names = args + [n + "_v" for n, _, _ in outs] + [n for n, _, _ in scratch]
    names += [n for n, _ in sems]
    return pl.pallas_call(
        functools.partial(kernel, tuple(names)),
        out_shape=[pltpu.VMEM(a, b) for _, a, b in outs],
        in_specs=[hbm] * 7 + [vm] * 3 + [sm],
        out_specs=[vm] * len(outs),
        scratch_shapes=[pltpu.VMEM(a, b) for _, a, b in scratch]
        + [pltpu.SemaphoreType.DMA(n) for _, n in sems],
        compiler_params=pltpu.CompilerParams(
            collective_id=0, has_side_effects=True, vmem_limit_bytes=56 << 20
        ),
        name="attention_backward",
    )(q, k, v, tk, tv, s, w, gate, windows, tile_map, text_count)


def copy_kernel(n, *refs):
    srcs, dsts, sem = refs[:n], refs[n : 2 * n], refs[2 * n]
    stores = [pltpu.make_async_copy(srcs[i], dsts[i], sem.at[i]) for i in range(n)]
    for c in stores:
        c.start()
    for c in stores:
        c.wait()


def copy_call(arrays):
    n = len(arrays)
    return pl.pallas_call(
        functools.partial(copy_kernel, n),
        out_shape=[jax.ShapeDtypeStruct(a.shape, a.dtype) for a in arrays],
        in_specs=[pl.BlockSpec(memory_space=pltpu.VMEM)] * n,
        out_specs=[pl.BlockSpec(memory_space=pltpu.HBM)] * n,
        scratch_shapes=[pltpu.SemaphoreType.DMA((n,))],
        compiler_params=pltpu.CompilerParams(vmem_limit_bytes=4 << 20),
        name="results",
    )(*arrays)


def per_device(
    query,
    key,
    value,
    text_key,
    text_value,
    grad_out,
    gate,
    out_weight,
    windows,
    tile_map,
    text_count,
):
    outs = call(
        query[0],
        key[0],
        value[0],
        text_key[0],
        text_value[0],
        grad_out[0],
        out_weight,
        gate,
        windows,
        tile_map.T,
        text_count,
    )
    outs = copy_call(outs)
    return tuple(o[None] for o in outs[:5]) + (outs[5],)


def solution(mesh):
    placed = (
        P("dp", "sp", "tp"),
        P("dp", "sp", "tp"),
        P("dp", "sp", "tp"),
        P("dp", None, "tp"),
        P("dp", None, "tp"),
        P("dp", "sp", "tp"),
        P("dp", None),
        P("tp", "dp"),
        P("sp", None),
        P(),
        P("dp"),
    )
    return jax.shard_map(
        per_device,
        mesh=mesh,
        in_specs=placed,
        out_specs=(
            P("dp", "sp", "tp"),
            P("dp", "sp", "tp"),
            P("dp", "sp", "tp"),
            P("dp", None, "tp"),
            P("dp", None, "tp"),
            P("tp", "dp"),
        ),
        check_vma=False,
    )
```

```python
import functools

import jax
import jax.numpy as jnp
from jax import lax
from jax.experimental import pallas as pl
from jax.experimental.pallas import tpu as pltpu
from jax.sharding import PartitionSpec as P

HD = 128
VMEM = 67043328
MESH = pl.DeviceIdType.MESH

NT = (((1,), (1,)), ((), ()))
NN = (((1,), (0,)), ((), ()))
TN = (((0,), (0,)), ((), ()))

bf16, f32 = jnp.bfloat16, jnp.float32


def mm(a, b, dims):
    return lax.dot_general(a, b, dims, preferred_element_type=f32)


def item_k(h):
    return 3 * h


def item_v(h):
    return 3 * h + 1


def item_q(h):
    return 3 * h + 2


def kernel(
    names,
    *refs,
):
    r_ = dict(zip(names, refs, strict=True))
    q_ref, s_ref, gate_ref, win_ref = (r_[n] for n in ("q_v", "s_v", "gate", "win"))
    map_ref, live_ref = r_["map"], r_["live"]
    keys, vals, qf, gaf = r_["keys"], r_["vals"], r_["qf"], r_["gaf"]
    st_out, st_in, dl_out, dl_in = r_["st_out"], r_["st_in"], r_["dl_out"], r_["dl_in"]
    raw, nat, w_all, acc = r_["raw"], r_["nat"], r_["w_all"], r_["acc"]
    ga_t, att_t, wts, wfar, gs_buf = r_["ga_t"], r_["att_t"], r_["wts"], r_["wfar"], r_["gs_buf"]
    parts, g1_out, g1_in = r_["parts"], r_["g1_out"], r_["g1_in"]
    gy_out, gy_in, gx_out, gx_in = r_["gy_out"], r_["gy_in"], r_["gx_out"], r_["gx_in"]
    gall, gfin = r_["gall"], r_["gfin"]
    tx_out, tx_in, tg = r_["tx_out"], r_["tx_in"], r_["tg"]
    ty_out, ty_in, t_own = r_["ty_out"], r_["ty_in"], r_["t_own"]
    gk_sum, gv_sum = r_["gk_sum"], r_["gv_sum"]

    factor = HD ** (-0.5)
    tok, width = q_ref.shape
    text = r_["tk"].shape[0]
    heads = width // HD
    near = tok + text
    n_tp = n_sp = 8
    me_sp = lax.axis_index("sp")
    me_dp = lax.axis_index("dp")
    me_tp = lax.axis_index("tp")
    x = me_sp & 3
    yh = me_sp >> 2
    core = me_dp & 1
    yl = me_dp >> 1
    w = s_ref.shape[1]
    piece = width // 16
    y = 2 * yh + yl
    half = width // 2
    has = [me_sp >= 1, me_sp + 1 < n_sp]
    side_sp = [me_sp - 1, me_sp + 1]

    partners = [{"tp": (me_tp + 1) & 7}, {"tp": (me_tp + 7) & 7}]
    partners += [{"dp": me_dp ^ 1}, {"dp": me_dp ^ 2}, {"dp": me_dp ^ 2, "sp": me_sp ^ 4}]
    partners += [{"sp": me_sp ^ j} for j in range(1, n_sp)]
    barrier = pltpu.get_barrier_semaphore()
    for where in partners:
        pl.semaphore_signal(barrier, inc=1, device_id=where, device_id_type=MESH)

    w_ref = w_all.at[me_dp]
    loads = {
        n: pltpu.make_async_copy(r_[n], to, r_["ls"].at[i])
        for i, (n, to) in enumerate(
            [
                ("s", s_ref),
                ("w", w_ref),
                ("k", keys.at[pl.ds(0, tok)]),
                ("v", vals.at[pl.ds(0, tok)]),
                ("q", q_ref),
                ("tk", keys.at[pl.ds(tok, text)]),
                ("tv", vals.at[pl.ds(tok, text)]),
            ]
        )
    }
    for c in loads.values():
        c.start()
    pl.semaphore_wait(barrier, len(partners))

    def remote(src, dst, send, recv, where):
        return pltpu.make_async_remote_copy(
            src_ref=src,
            dst_ref=dst,
            send_sem=send,
            recv_sem=recv,
            device_id=where,
            device_id_type=MESH,
        )

    chunk = tok // 2

    def crow(c):
        return pl.ds(c * chunk, chunk)

    def z_copy(up, t, c):
        r = (8 - t) % 8 if up else t
        to = (r + 7) % 8 if up else (r + 1) % 8
        src = s_ref.at[crow(c)] if t == 0 else raw.at[r, crow(c)]
        send = r_["zs"].at[0]
        recv = r_["zr"].at[0 if up else 1, t, c]
        where = {"tp": (me_tp + (1 if up else 7)) & 7}
        return remote(src, raw.at[to, crow(c)], send, recv, where)

    def z_exists(up, t, c):
        return t < 3 or (t == 3 and c == (0 if up else 1))

    def z_arrive(t, i):
        for up in (True, False):
            c = i if up else 1 - i
            if z_exists(up, t, c):
                z_copy(up, t, c).wait_recv()
                if t < 3 and z_exists(up, t + 1, c):
                    z_copy(up, t + 1, c).start()

    def w_core():
        return remote(w_ref, w_all.at[me_dp], r_["ws"].at[0], r_["wr"].at[0], {"dp": me_dp ^ 1})

    ends = (x == 0) | (x == 3)
    gives = jnp.where(x == 0, yh == 1, yh == 0)

    def w_y(i, j):
        rows = pl.ds(j * half, half)
        where = {"dp": me_dp ^ 2, "sp": me_sp ^ (4 * i)}
        return remote(
            w_ref.at[rows],
            w_all.at[me_dp, rows],
            r_["ws"].at[1],
            r_["wr"].at[1],
            where,
        )

    def w_y_all(n):
        held = w_all.at[pl.ds(0, n)]
        return remote(held, held, r_["ws"].at[1], r_["wr"].at[1], {"dp": me_dp ^ 2})

    def w_fwd():
        block = w_all.at[me_dp ^ 2]
        return remote(block, block, r_["ws"].at[2], r_["wr"].at[2], {"dp": me_dp ^ 1})

    def halo(side, item):
        there = 1 - side
        region = pl.ds(near + there * tok, tok)
        if item < 3 * heads:
            h, kind = divmod(item, 3)
            c = pl.ds(h * HD, HD)
            src = (keys.at[pl.ds(0, tok), c], vals.at[pl.ds(0, tok), c], q_ref.at[:, c])[kind]
            dst = (keys.at[region, c], vals.at[region, c], qf.at[there, :, c])[kind]
        elif item < 4 * heads:
            c = pl.ds((item - 3 * heads) * HD, HD)
            src, dst = ga_t.at[c], gaf.at[there, c]
        elif item == 4 * heads:
            src, dst = st_out.at[side], st_in.at[there]
        else:
            src, dst = dl_out, dl_in.at[there]
        if item < 4 * heads:
            send = 0
            got = (h if kind < 2 else heads) if item < 3 * heads else item - 2 * heads + 1
        else:
            send = 1 + item - 4 * heads
            got = item - 2 * heads + 1
        return remote(
            src, dst, r_["hs"].at[side, send], r_["hr"].at[there, got], {"sp": side_sp[side]}
        )

    def halo_start(items):
        for side in (0, 1):

            @pl.when(has[side])
            def _():
                for item in items:
                    halo(side, item).start()

    def halo_wait(side, what):
        kind, h = what
        if kind in ("st", "dl"):
            halo(1 - side, 4 * heads + (kind == "dl")).wait_recv()
        elif kind == "ga":
            halo(1 - side, 3 * heads + h).wait_recv()
        else:
            some = keys.at[pl.ds(0, 2 * tok), pl.ds(0, HD)] if kind == "kv" else qf.at[side]
            got = r_["hr"].at[side, h if kind == "kv" else heads]
            remote(some, some, r_["hs"].at[side, 0], got, {"sp": me_sp ^ 1}).wait_recv()

    def halo_wait_both(*whats):
        for side in (0, 1):

            @pl.when(has[side])
            def _():
                for what in whats:
                    halo_wait(side, what)

    loads["s"].wait()
    for c in (0, 1):
        z_copy(True, 0, c).start()
        z_copy(False, 0, 1 - c).start()
    loads["w"].wait()
    w_core().start()

    @pl.when(jnp.logical_not(ends))
    def _():
        w_y(0, 0).start()
        w_y(1, 1).start()

    @pl.when(ends & gives)
    def _():
        for i in (0, 1):
            for j in (0, 1):
                w_y(i, j).start()

    loads["k"].wait()
    loads["v"].wait()
    for h in range(heads):
        halo_start([item_k(h), item_v(h)])
    loads["q"].wait()
    for h in range(heads):
        halo_start([item_q(h)])
    loads["tk"].wait()
    loads["tv"].wait()
    for side in (0, 1):

        @pl.when(jnp.logical_not(has[side]))
        def _():
            region = slice(near + side * tok, near + (side + 1) * tok)
            keys[region] = jnp.zeros((tok, width), bf16)
            vals[region] = jnp.zeros((tok, width), bf16)

    def blk(r):
        return (me_tp + r) & 7

    def scale(r):
        gate = gate_ref[:, pl.ds(pl.multiple_of(blk(r) * w, HD), w)].astype(f32)
        src = s_ref[...] if r == 0 else raw[r]
        nat[r] = (src.astype(f32) * gate).astype(bf16)

    def ga_add(r, first=False):
        at = pl.multiple_of((blk(r) & 1) * w, HD)
        term = mm(w_all[blk(r) >> 1, :, pl.ds(at, w)], nat[r], NT)
        if first:
            acc[...] = term
        else:
            acc[...] += term

    slab_of = lax.broadcasted_iota(jnp.int32, (1, n_sp), 1)

    def place_of_slab(slab):
        here = jnp.where(slab_of == slab, map_ref[...].astype(f32), 0.0)
        return jnp.sum(here, axis=1, keepdims=True)

    place = place_of_slab(me_sp)
    reach = win_ref[...].astype(f32)
    side_bias = []
    for side in (0, 1):
        apart = jnp.abs(place - place_of_slab(side_sp[side]))
        seen = (reach[0:1, 0:1] >= 1.0) & (reach[0:1, 1:2] >= apart)
        edge = jnp.where(has[side], 0.0, -1e30).astype(f32)
        side_bias.append(jnp.minimum(jnp.where(seen, 0.0, -1e30).astype(f32), edge))
    place_of = lax.broadcasted_iota(jnp.int32, (text, 1), 0)
    words = jnp.where(place_of < live_ref[0], 0.0, -1e30).astype(f32)
    bias_ref, st_near = r_["bias"], r_["st_near"]
    bias_ref[:tok] = jnp.zeros((tok, 1), f32)
    bias_ref[tok:near] = words
    for side in (0, 1):
        region = slice(near + side * tok, near + (side + 1) * tok)
        bias_ref[region] = jnp.broadcast_to(side_bias[side], (tok, 1))

    def cols(h):
        return slice(h * HD, (h + 1) * HD)

    def near_scores(h):
        c = cols(h)
        scores = factor * mm(keys[:near, c], q_ref[:, c], NT) + bias_ref[:near]
        top = jnp.max(scores, axis=0, keepdims=True)
        e = jnp.exp(scores - top)
        wts[h, :near, :] = e
        st_near[h : h + 1, :] = top
        st_near[heads + h : heads + h + 1, :] = jnp.sum(e, axis=0, keepdims=True)

    def forward(h):
        c = cols(h)
        scores = factor * mm(keys[near:, c], q_ref[:, c], NT) + bias_ref[near:]
        top_near = st_near[h : h + 1, :]
        top = jnp.maximum(top_near, jnp.max(scores, axis=0, keepdims=True))
        e = jnp.exp(scores - top)
        fix = jnp.exp(top_near - top)
        total = jnp.sum(e, axis=0, keepdims=True) + fix * st_near[heads + h : heads + h + 1, :]
        inv = 1.0 / total
        w_near = wts[h, :near, :] * (fix * inv)
        w_far = e * inv
        wts[h, :near, :] = w_near
        wts[h, near:, :] = w_far
        att = mm(vals[:near, c], w_near.astype(bf16), TN) + mm(vals[near:, c], w_far.astype(bf16), TN)
        att_t[c, :] = att.astype(bf16)
        for side in (0, 1):
            st_out[side, h : h + 1, :] = top - side_bias[side]
            st_out[side, heads + h : heads + h + 1, :] = inv

    def far_weights(side, h):
        c = cols(h)
        scores = factor * mm(keys[:tok, c], qf[side, :, c], NT)
        e = jnp.exp(scores - st_in[side, h : h + 1, :])
        wfar[side, h] = e * st_in[side, heads + h : heads + h + 1, :]

    def core_owns(r):
        return ((blk(r) >> 1) & 1) == core

    def mine(r):
        return (blk(r) >> 1) == me_dp

    def s1_copy(r):
        return remote(
            g1_out.at[r], g1_in.at[r], r_["s1s"].at[0], r_["s1r"].at[r], {"dp": me_dp ^ 1}
        )

    def x_first(r):
        return r in (2, 6)

    def along_x(j):
        return {"sp": me_sp ^ j}

    def along_y(j):
        return {"dp": me_dp ^ (2 * (j & 1)), "sp": me_sp ^ (2 * (j & 2))}

    def place1(r):
        return x if x_first(r) else y

    def place2(r):
        return y if x_first(r) else x

    def gy_copy(r, j):
        where = along_x(j) if x_first(r) else along_y(j)
        return remote(
            gy_out.at[r, place1(r) ^ j],
            gy_in.at[r, j - 1],
            r_["gys"].at[0],
            r_["gyr"].at[r],
            where,
        )

    def gx_copy(r, j):
        where = along_y(j) if x_first(r) else along_x(j)
        return remote(
            gx_out.at[r, place2(r) ^ j],
            gx_in.at[r, j - 1],
            r_["gxs"].at[0],
            r_["gxr"].at[r],
            where,
        )

    def ag1_copy(r, j):
        piece_ = gall.at[r, x]
        return remote(piece_, piece_, r_["ag1s"].at[0], r_["ag1r"].at[r], along_x(j))

    def ag2_copy(r, i):
        return remote(
            gall.at[r],
            gfin.at[blk(r) & 1, y],
            r_["ag2s"].at[0],
            r_["ag2r"].at[r],
            {"dp": blk(r) >> 1, "sp": 4 * i + x},
        )

    def ag2_sends(r, i):
        return core_owns(r) & jnp.logical_not(mine(r) & (yh == i))

    def all_of(some, send, recv):
        return remote(some, some, send, recv, {"sp": me_sp ^ 4})

    def gw_part(r):
        parts[r] = mm(att_t[...], nat[r], NN)

        @pl.when(jnp.logical_not(core_owns(r)))
        def _():
            g1_out[r] = parts[r].astype(bf16)
            s1_copy(r).start()

    def gw_s1(r):
        @pl.when(core_owns(r))
        def _():
            s1_copy(r).wait_recv()
            for i in range(4):
                for k in range(4):
                    rows = slice((4 * i + k) * piece, (4 * i + k + 1) * piece)
                    total = parts[r, rows, :] + g1_in[r, rows, :].astype(f32)
                    parts[r, rows, :] = total
                    gy_out[r, i, k] = total.astype(bf16)
            for j in range(1, 4):
                gy_copy(r, j).start()

    def gw_sy(r):
        @pl.when(core_owns(r))
        def _():
            all_of(gy_in.at[r], r_["gys"].at[0], r_["gyr"].at[r]).wait_recv()
            for k in range(4):
                at = pl.multiple_of(place1(r) * (4 * piece) + k * piece, 8)
                total = parts[r, pl.ds(at, piece), :]
                for j in range(3):
                    total = total + gy_in[r, j, k].astype(f32)
                parts[r, k * piece : (k + 1) * piece, :] = total
                gx_out[r, k] = total.astype(bf16)
            for j in range(1, 4):
                gx_copy(r, j).start()

    def gw_sx(r):
        @pl.when(core_owns(r))
        def _():
            all_of(gx_in.at[r], r_["gxs"].at[0], r_["gxr"].at[r]).wait_recv()
            total = parts[r, pl.ds(pl.multiple_of(place2(r) * piece, 8), piece), :]
            for j in range(3):
                total = total + gx_in[r, j].astype(f32)
            gall[r, x] = total.astype(bf16)
            for j in range(1, 4):
                ag1_copy(r, j).start()

    def gw_ag(r):
        @pl.when(core_owns(r))
        def _():
            all_of(gx_in.at[0], r_["ag1s"].at[0], r_["ag1r"].at[r]).wait_recv()

        for i in (0, 1):

            @pl.when(ag2_sends(r, i))
            def _():
                ag2_copy(r, i).start()

        @pl.when(mine(r))
        def _():
            gfin[blk(r) & 1, y] = gall[r]

    gw_v = r_["gw_v"]

    def gw_end(r):
        @pl.when(mine(r))
        def _():
            all_of(gy_in.at[0], r_["ag2s"].at[0], r_["ag2r"].at[r]).wait_recv()
            at = pl.ds(pl.multiple_of((blk(r) & 1) * w, HD), w)
            for i in range(4):
                for k in range(4):
                    n = 4 * k + i if x_first(r) else 4 * i + k
                    rows = slice(n * piece, (n + 1) * piece)
                    gw_v[rows, at] = gfin[blk(r) & 1, i, k].astype(f32)

    trow = text // n_sp

    def tx_copy(j):
        return remote(
            tx_out.at[x ^ j], tx_in.at[j - 1], r_["txs"].at[0], r_["txr"].at[0], along_x(j)
        )

    def ty_copy():
        return remote(ty_out, ty_in, r_["tys"].at[0], r_["tyr"].at[0], {"sp": me_sp ^ 4})

    def tg_copy():
        slot = tg.at[x, yh]
        return remote(slot, slot, r_["tgs"].at[0], r_["tgr"].at[0], {"sp": me_sp ^ 4})

    def tz_copy(i, j):
        slot = tg.at[x, i]
        return remote(slot, slot, r_["tzs"].at[0], r_["tzr"].at[0], along_x(j))

    def text_1():
        all_of(tx_in, r_["txs"].at[0], r_["txr"].at[0]).wait_recv()

        def over_x(i):
            total = tx_out[x, i].astype(f32)
            for j in range(3):
                total = total + tx_in[j, i].astype(f32)
            return total

        ty_out[...] = over_x(1 - yh).astype(bf16)
        ty_copy().start()
        t_own[...] = over_x(yh)

    def text_2():
        ty_copy().wait_recv()
        tg[x, yh] = (t_own[...] + ty_in[...].astype(f32)).astype(bf16)
        tg_copy().start()
        for j in range(1, 4):
            tz_copy(yh, j).start()

    def text_3():
        tg_copy().wait_recv()
        for j in range(1, 4):
            tz_copy(1 - yh, j).start()

    def text_4():
        all_of(tx_in, r_["tzs"].at[0], r_["tzr"].at[0]).wait_recv()
        for i in range(4):
            for k in range(2):
                rows = slice((2 * i + k) * trow, (2 * i + k + 1) * trow)
                gtk_v[rows] = tg[i, k, :trow]
                gtv_v[rows] = tg[i, k, trow:]

    gq_v, gk_v, gv_v, gtk_v, gtv_v = (r_[n] for n in ("gq_v", "gk_v", "gv_v", "gtk_v", "gtv_v"))

    def text_part(h):
        c = cols(h)
        ga = ga_t[c, :]
        wt = wts[h, tok:near, :]
        gp = mm(vals[tok:near, c], ga, NN)
        gs = (wt * (gp - dl_out[h : h + 1, :])).astype(bf16)
        gs_buf[h, tok:near, :] = gs
        gk = (factor * mm(gs, q_ref[:, c], NN)).astype(bf16)
        gv = mm(wt.astype(bf16), ga, NT).astype(bf16)
        for j in range(n_sp):
            rows = slice(j * trow, (j + 1) * trow)
            tx_out[j // 2, j % 2, :trow, c] = gk[rows]
            tx_out[j // 2, j % 2, trow:, c] = gv[rows]

    def own_part(h):
        c = cols(h)
        ga = ga_t[c, :]
        delta = dl_out[h : h + 1, :]
        for lo, hi in ((0, tok), (near, near + 2 * tok)):
            gp = mm(vals[lo:hi, c], ga, NN)
            gs_buf[h, lo:hi, :] = (wts[h, lo:hi, :] * (gp - delta)).astype(bf16)
        gq_v[:, c] = (factor * mm(keys[:, c], gs_buf[h], TN)).T.astype(bf16)
        gk_sum[:, c] = mm(gs_buf[h, :tok, :], q_ref[:, c], NN)
        gv_sum[:, c] = mm(wts[h, :tok, :].astype(bf16), ga, NT)

    def far_part(side, h):
        c = cols(h)
        ga = gaf[side, c, :]
        weights = wfar[side, h]
        gp = mm(vals[:tok, c], ga, NN)
        gs = (weights * (gp - dl_in[side, h : h + 1, :])).astype(bf16)
        gk_sum[:, c] += mm(gs, qf[side, :, c], NN)
        gv_sum[:, c] += mm(weights.astype(bf16), ga, NT)

    scale(0)
    for h in range(heads):
        near_scores(h)
    z_arrive(0, 0)
    z_arrive(0, 1)
    scale(1)
    scale(7)
    halo_wait_both(("kv", 0))
    forward(0)
    z_arrive(1, 0)
    halo_wait_both(("kv", 1))
    forward(1)
    z_arrive(1, 1)
    scale(2)
    scale(6)
    w_core().wait_recv()
    w_y_all(1).wait_recv()
    w_fwd().start()
    halo_wait_both(("kv", 2))
    forward(2)
    halo_start([4 * heads])
    for r in (0, 1, 7):
        gw_part(r)
    z_arrive(2, 0)
    for r in (2, 6):
        gw_part(r)
    for r in (0, 1, 7):
        gw_s1(r)
    w_fwd().wait_recv()
    ga_add(0, True)
    ga_add(1)
    for r in (2, 6):
        gw_s1(r)
    ga_add(7)
    ga_add(2)
    z_arrive(2, 1)
    scale(3)
    scale(5)
    for r in (3, 5):
        gw_part(r)
    ga_add(6)
    ga_add(3)
    ga_add(5)
    z_arrive(3, 0)
    scale(4)
    gw_part(4)
    for r in (3, 5):
        gw_s1(r)
    ga_add(4)
    ga_t[...] = acc[...].astype(bf16)
    for h in range(heads):
        c = cols(h)
        dl_out[h : h + 1, :] = jnp.sum(
            ga_t[c, :].astype(f32) * att_t[c, :].astype(f32), axis=0, keepdims=True
        )
    gw_s1(4)
    for h in range(heads):
        text_part(h)
    for r in (0, 1, 7):
        gw_sy(r)
    def far_head(h):
        halo_wait_both(("ga", h))
        for side in (0, 1):
            pl.when(has[side])(functools.partial(far_part, side, h))
        c = cols(h)
        gk_v[:, c] = (factor * gk_sum[:, c]).astype(bf16)
        gv_v[:, c] = gv_sum[:, c].astype(bf16)

    for j in range(1, 4):
        tx_copy(j).start()
    for r in (2, 6):
        gw_sy(r)
    own_part(0)
    own_part(1)
    for r in (3, 5):
        gw_sy(r)
    for r in (0, 1, 7):
        gw_sx(r)
    halo_start([4 * heads + 1, 3 * heads])
    gw_sy(4)
    own_part(2)
    halo_start([3 * heads + 1])
    for r in (2, 6):
        gw_sx(r)
    text_1()
    halo_wait_both(("st", 0), ("q", 0))
    for h in range(heads):
        for side in (0, 1):
            pl.when(has[side])(functools.partial(far_weights, side, h))
    for r in (3, 5):
        gw_sx(r)
    gw_sx(4)
    halo_start([3 * heads + 2])
    text_2()
    for r in (0, 1, 7):
        gw_ag(r)
    for r in (2, 6):
        gw_ag(r)
    halo_wait_both(("dl", 0))
    far_head(0)
    for r in (3, 5):
        gw_ag(r)
    gw_ag(4)
    text_3()
    far_head(1)
    far_head(2)
    text_4()
    for r in (0, 1, 7, 2, 6, 3, 5, 4):
        gw_end(r)

    all_of(raw.at[pl.ds(0, n_tp - 1)], r_["zs"].at[0], r_["zr"].at[0, 0, 0]).wait_send()
    w_core().wait_send()

    @pl.when(jnp.logical_not(ends))
    def _():
        w_y_all(1).wait_send()

    @pl.when(ends & gives)
    def _():
        w_y_all(2).wait_send()

    w_fwd().wait_send()
    for side in (0, 1):

        @pl.when(has[side])
        def _():
            blocks = raw.at[pl.ds(0, 4)]
            remote(
                blocks, blocks, r_["hs"].at[side, 0], r_["hr"].at[side, 0], {"sp": side_sp[side]}
            ).wait_send()
            halo(side, 4 * heads).wait_send()
            halo(side, 4 * heads + 1).wait_send()

    for some, n in (
        (g1_out.at[pl.ds(0, 4)], "s1"),
        (gy_in.at[pl.ds(0, 4)], "gy"),
        (gx_in.at[pl.ds(0, 4)], "gx"),
        (gx_in.at[pl.ds(0, 4)], "ag1"),
        (gy_in.at[pl.ds(0, 2)], "ag2"),
        (tx_in, "tx"),
        (ty_out, "ty"),
        (ty_out, "tg"),
        (tx_in, "tz"),
    ):
        all_of(some, r_[n + "s"].at[0], r_[n + "r"].at[0]).wait_send()


def call(q, k, v, tk, tv, s, w, gate, windows, tile_map, text_count):
    tok, width = q.shape
    text = tk.shape[0]
    heads = width // HD
    cols = w.shape[1]
    hbm = pl.BlockSpec(memory_space=pltpu.HBM)
    total = 3 * tok + text
    block = s.shape[1]
    piece = width // 16
    sm = pl.BlockSpec(memory_space=pltpu.SMEM)
    vm = pl.BlockSpec(memory_space=pltpu.VMEM)
    outs = [
        ("gq", (tok, width), bf16),
        ("gk", (tok, width), bf16),
        ("gv", (tok, width), bf16),
        ("gtk", (text, width), bf16),
        ("gtv", (text, width), bf16),
        ("gw", (width, cols), f32),
    ]
    scratch = [
        ("q_v", (tok, width), bf16),
        ("s_v", (tok, block), bf16),
        ("keys", (total, width), bf16),
        ("vals", (total, width), bf16),
        ("qf", (2, tok, width), bf16),
        ("gaf", (2, width, tok), bf16),
        ("st_out", (2, 8, tok), f32),
        ("st_in", (2, 8, tok), f32),
        ("dl_out", (8, tok), f32),
        ("dl_in", (2, 8, tok), f32),
        ("bias", (total, 1), f32),
        ("st_near", (8, tok), f32),
        ("raw", (8, tok, block), bf16),
        ("nat", (8, tok, block), bf16),
        ("w_all", (4, width, cols), bf16),
        ("acc", (width, tok), f32),
        ("ga_t", (width, tok), bf16),
        ("att_t", (width, tok), bf16),
        ("wts", (heads, total, tok), f32),
        ("wfar", (2, heads, tok, tok), f32),
        ("gs_buf", (heads, total, tok), bf16),
        ("gk_sum", (tok, width), f32),
        ("gv_sum", (tok, width), f32),
        ("parts", (8, width, block), f32),
        ("g1_out", (8, width, block), bf16),
        ("g1_in", (8, width, block), bf16),
        ("gy_out", (8, 4, 4, piece, block), bf16),
        ("gy_in", (8, 3, 4, piece, block), bf16),
        ("gx_out", (8, 4, piece, block), bf16),
        ("gx_in", (8, 3, piece, block), bf16),
        ("gall", (8, 4, piece, block), bf16),
        ("gfin", (2, 4, 4, piece, block), bf16),
        ("tx_out", (4, 2, text // 4, width), bf16),
        ("tx_in", (3, 2, text // 4, width), bf16),
        ("ty_out", (text // 4, width), bf16),
        ("ty_in", (text // 4, width), bf16),
        ("t_own", (text // 4, width), f32),
        ("tg", (4, 2, text // 4, width), bf16),
    ]
    sems = [
        ("zs", (1,)),
        ("zr", (2, 4, 2)),
        ("ws", (3,)),
        ("wr", (3,)),
        ("hs", (2, 3)),
        ("hr", (2, 2 * heads + 3)),
        ("s1s", (1,)),
        ("s1r", (8,)),
        ("gys", (1,)),
        ("gyr", (8,)),
        ("gxs", (1,)),
        ("gxr", (8,)),
        ("ag1s", (1,)),
        ("ag1r", (8,)),
        ("ag2s", (1,)),
        ("ag2r", (8,)),
        ("txs", (1,)),
        ("txr", (1,)),
        ("tys", (1,)),
        ("tyr", (1,)),
        ("tzs", (1,)),
        ("tzr", (1,)),
        ("tgs", (1,)),
        ("tgr", (1,)),
        ("ls", (7,)),
    ]
    args = ["q", "k", "v", "tk", "tv", "s", "w", "gate", "win", "map", "live"]
    names = args + [n + "_v" for n, _, _ in outs] + [n for n, _, _ in scratch]
    names += [n for n, _ in sems]
    return pl.pallas_call(
        functools.partial(kernel, tuple(names)),
        out_shape=[pltpu.VMEM(a, b) for _, a, b in outs],
        in_specs=[hbm] * 7 + [vm] * 3 + [sm],
        out_specs=[vm] * len(outs),
        scratch_shapes=[pltpu.VMEM(a, b) for _, a, b in scratch]
        + [pltpu.SemaphoreType.DMA(n) for _, n in sems],
        compiler_params=pltpu.CompilerParams(
            collective_id=0, has_side_effects=True, vmem_limit_bytes=56 << 20
        ),
        name="attention_backward",
    )(q, k, v, tk, tv, s, w, gate, windows, tile_map, text_count)


def copy_kernel(n, *refs):
    srcs, dsts, sem = refs[:n], refs[n : 2 * n], refs[2 * n]
    stores = [pltpu.make_async_copy(srcs[i], dsts[i], sem.at[i]) for i in range(n)]
    for c in stores:
        c.start()
    for c in stores:
        c.wait()


def copy_call(arrays):
    n = len(arrays)
    return pl.pallas_call(
        functools.partial(copy_kernel, n),
        out_shape=[jax.ShapeDtypeStruct(a.shape, a.dtype) for a in arrays],
        in_specs=[pl.BlockSpec(memory_space=pltpu.VMEM)] * n,
        out_specs=[pl.BlockSpec(memory_space=pltpu.HBM)] * n,
        scratch_shapes=[pltpu.SemaphoreType.DMA((n,))],
        compiler_params=pltpu.CompilerParams(vmem_limit_bytes=4 << 20),
        name="results",
    )(*arrays)


def per_device(
    query,
    key,
    value,
    text_key,
    text_value,
    grad_out,
    gate,
    out_weight,
    windows,
    tile_map,
    text_count,
):
    outs = call(
        query[0],
        key[0],
        value[0],
        text_key[0],
        text_value[0],
        grad_out[0],
        out_weight,
        gate,
        windows,
        tile_map.T,
        text_count,
    )
    outs = copy_call(outs)
    return tuple(o[None] for o in outs[:5]) + (outs[5],)


def solution(mesh):
    placed = (
        P("dp", "sp", "tp"),
        P("dp", "sp", "tp"),
        P("dp", "sp", "tp"),
        P("dp", None, "tp"),
        P("dp", None, "tp"),
        P("dp", "sp", "tp"),
        P("dp", None),
        P("tp", "dp"),
        P("sp", None),
        P(),
        P("dp"),
    )
    return jax.shard_map(
        per_device,
        mesh=mesh,
        in_specs=placed,
        out_specs=(
            P("dp", "sp", "tp"),
            P("dp", "sp", "tp"),
            P("dp", "sp", "tp"),
            P("dp", None, "tp"),
            P("dp", None, "tp"),
            P("tp", "dp"),
        ),
        check_vma=False,
    )
```

```python
import functools

import jax
import jax.numpy as jnp
from jax import lax
from jax.experimental import pallas as pl
from jax.experimental.pallas import tpu as pltpu
from jax.sharding import PartitionSpec as P

HD = 128
VMEM = 67043328
MESH = pl.DeviceIdType.MESH

NT = (((1,), (1,)), ((), ()))
NN = (((1,), (0,)), ((), ()))
TN = (((0,), (0,)), ((), ()))

bf16, f32 = jnp.bfloat16, jnp.float32


def mm(a, b, dims):
    return lax.dot_general(a, b, dims, preferred_element_type=f32)


def item_k(h):
    return 3 * h


def item_v(h):
    return 3 * h + 1


def item_q(h):
    return 3 * h + 2


def kernel(
    names,
    *refs,
):
    r_ = dict(zip(names, refs, strict=True))
    q_ref, s_ref, gate_ref, win_ref = (r_[n] for n in ("q_v", "s_v", "gate", "win"))
    map_ref, live_ref = r_["map"], r_["live"]
    keys, vals, qf, gaf = r_["keys"], r_["vals"], r_["qf"], r_["gaf"]
    st_out, st_in, dl_out, dl_in = r_["st_out"], r_["st_in"], r_["dl_out"], r_["dl_in"]
    raw, nat, w_all, acc = r_["raw"], r_["nat"], r_["w_all"], r_["acc"]
    ga_t, att_t, wts, wfar, gs_buf = r_["ga_t"], r_["att_t"], r_["wts"], r_["wfar"], r_["gs_buf"]
    parts, g1_out, g1_in = r_["parts"], r_["g1_out"], r_["g1_in"]
    gy_out, gy_in, gx_out, gx_in = r_["gy_out"], r_["gy_in"], r_["gx_out"], r_["gx_in"]
    gall, gfin = r_["gall"], r_["gfin"]
    tx_out, tx_in, tg = r_["tx_out"], r_["tx_in"], r_["tg"]
    ty_out, ty_in, t_own = r_["ty_out"], r_["ty_in"], r_["t_own"]
    gk_sum, gv_sum = r_["gk_sum"], r_["gv_sum"]

    factor = HD ** (-0.5)
    tok, width = q_ref.shape
    text = r_["tk"].shape[0]
    heads = width // HD
    near = tok + text
    n_tp = n_sp = 8
    me_sp = lax.axis_index("sp")
    me_dp = lax.axis_index("dp")
    me_tp = lax.axis_index("tp")
    x = me_sp & 3
    yh = me_sp >> 2
    core = me_dp & 1
    yl = me_dp >> 1
    w = s_ref.shape[1]
    piece = width // 16
    y = 2 * yh + yl
    half = width // 2
    has = [me_sp >= 1, me_sp + 1 < n_sp]
    side_sp = [me_sp - 1, me_sp + 1]

    partners = [{"tp": (me_tp + 1) & 7}, {"tp": (me_tp + 7) & 7}]
    partners += [{"dp": me_dp ^ 1}, {"dp": me_dp ^ 2}, {"dp": me_dp ^ 2, "sp": me_sp ^ 4}]
    partners += [{"sp": me_sp ^ j} for j in range(1, n_sp)]
    barrier = pltpu.get_barrier_semaphore()
    for where in partners:
        pl.semaphore_signal(barrier, inc=1, device_id=where, device_id_type=MESH)

    w_ref = w_all.at[me_dp]
    loads = {
        n: pltpu.make_async_copy(r_[n], to, r_["ls"].at[i])
        for i, (n, to) in enumerate(
            [
                ("s", s_ref),
                ("w", w_ref),
                ("k", keys.at[pl.ds(0, tok)]),
                ("v", vals.at[pl.ds(0, tok)]),
                ("q", q_ref),
                ("tk", keys.at[pl.ds(tok, text)]),
                ("tv", vals.at[pl.ds(tok, text)]),
            ]
        )
    }
    for c in loads.values():
        c.start()
    pl.semaphore_wait(barrier, len(partners))

    def remote(src, dst, send, recv, where):
        return pltpu.make_async_remote_copy(
            src_ref=src,
            dst_ref=dst,
            send_sem=send,
            recv_sem=recv,
            device_id=where,
            device_id_type=MESH,
        )

    chunk = tok // 2

    def crow(c):
        return pl.ds(c * chunk, chunk)

    def z_copy(up, t, c):
        r = (8 - t) % 8 if up else t
        to = (r + 7) % 8 if up else (r + 1) % 8
        src = s_ref.at[crow(c)] if t == 0 else raw.at[r, crow(c)]
        send = r_["zs"].at[0]
        recv = r_["zr"].at[0 if up else 1, t, c]
        where = {"tp": (me_tp + (1 if up else 7)) & 7}
        return remote(src, raw.at[to, crow(c)], send, recv, where)

    def z_exists(up, t, c):
        return t < 3 or (t == 3 and c == (0 if up else 1))

    def z_arrive(t, i):
        for up in (True, False):
            c = i if up else 1 - i
            if z_exists(up, t, c):
                z_copy(up, t, c).wait_recv()
                if t < 3 and z_exists(up, t + 1, c):
                    z_copy(up, t + 1, c).start()

    def w_core():
        return remote(w_ref, w_all.at[me_dp], r_["ws"].at[0], r_["wr"].at[0], {"dp": me_dp ^ 1})

    ends = (x == 0) | (x == 3)
    gives = jnp.where(x == 0, yh == 1, yh == 0)

    def w_y(i, j):
        rows = pl.ds(j * half, half)
        where = {"dp": me_dp ^ 2, "sp": me_sp ^ (4 * i)}
        return remote(
            w_ref.at[rows],
            w_all.at[me_dp, rows],
            r_["ws"].at[1],
            r_["wr"].at[1],
            where,
        )

    def w_y_all(n):
        held = w_all.at[pl.ds(0, n)]
        return remote(held, held, r_["ws"].at[1], r_["wr"].at[1], {"dp": me_dp ^ 2})

    def w_fwd():
        block = w_all.at[me_dp ^ 2]
        return remote(block, block, r_["ws"].at[2], r_["wr"].at[2], {"dp": me_dp ^ 1})

    def halo(side, item):
        there = 1 - side
        region = pl.ds(near + there * tok, tok)
        if item < 3 * heads:
            h, kind = divmod(item, 3)
            c = pl.ds(h * HD, HD)
            src = (keys.at[pl.ds(0, tok), c], vals.at[pl.ds(0, tok), c], q_ref.at[:, c])[kind]
            dst = (keys.at[region, c], vals.at[region, c], qf.at[there, :, c])[kind]
        elif item < 4 * heads:
            c = pl.ds((item - 3 * heads) * HD, HD)
            src, dst = ga_t.at[c], gaf.at[there, c]
        elif item == 4 * heads:
            src, dst = st_out.at[side], st_in.at[there]
        else:
            src, dst = dl_out, dl_in.at[there]
        if item < 4 * heads:
            send = 0
            got = (h if kind < 2 else heads) if item < 3 * heads else item - 2 * heads + 1
        else:
            send = 1 + item - 4 * heads
            got = item - 2 * heads + 1
        return remote(
            src, dst, r_["hs"].at[side, send], r_["hr"].at[there, got], {"sp": side_sp[side]}
        )

    def halo_start(items):
        for side in (0, 1):

            @pl.when(has[side])
            def _():
                for item in items:
                    halo(side, item).start()

    def halo_wait(side, what):
        kind, h = what
        if kind in ("st", "dl"):
            halo(1 - side, 4 * heads + (kind == "dl")).wait_recv()
        elif kind == "ga":
            halo(1 - side, 3 * heads + h).wait_recv()
        else:
            some = keys.at[pl.ds(0, 2 * tok), pl.ds(0, HD)] if kind == "kv" else qf.at[side]
            got = r_["hr"].at[side, h if kind == "kv" else heads]
            remote(some, some, r_["hs"].at[side, 0], got, {"sp": me_sp ^ 1}).wait_recv()

    def halo_wait_both(*whats):
        for side in (0, 1):

            @pl.when(has[side])
            def _():
                for what in whats:
                    halo_wait(side, what)

    loads["s"].wait()
    for c in (0, 1):
        z_copy(True, 0, c).start()
        z_copy(False, 0, 1 - c).start()
    loads["w"].wait()
    w_core().start()

    @pl.when(jnp.logical_not(ends))
    def _():
        w_y(0, 0).start()
        w_y(1, 1).start()

    @pl.when(ends & gives)
    def _():
        for i in (0, 1):
            for j in (0, 1):
                w_y(i, j).start()

    loads["k"].wait()
    loads["v"].wait()
    for h in range(heads):
        halo_start([item_k(h), item_v(h)])
    loads["q"].wait()
    for h in range(heads):
        halo_start([item_q(h)])
    loads["tk"].wait()
    loads["tv"].wait()
    for side in (0, 1):

        @pl.when(jnp.logical_not(has[side]))
        def _():
            region = slice(near + side * tok, near + (side + 1) * tok)
            keys[region] = jnp.zeros((tok, width), bf16)
            vals[region] = jnp.zeros((tok, width), bf16)

    def blk(r):
        return (me_tp + r) & 7

    def scale(r):
        gate = gate_ref[:, pl.ds(pl.multiple_of(blk(r) * w, HD), w)].astype(f32)
        src = s_ref[...] if r == 0 else raw[r]
        nat[r] = (src.astype(f32) * gate).astype(bf16)

    def ga_add(r, first=False):
        at = pl.multiple_of((blk(r) & 1) * w, HD)
        term = mm(w_all[blk(r) >> 1, :, pl.ds(at, w)], nat[r], NT)
        if first:
            acc[...] = term
        else:
            acc[...] += term

    slab_of = lax.broadcasted_iota(jnp.int32, (1, n_sp), 1)

    def place_of_slab(slab):
        here = jnp.where(slab_of == slab, map_ref[...].astype(f32), 0.0)
        return jnp.sum(here, axis=1, keepdims=True)

    place = place_of_slab(me_sp)
    reach = win_ref[...].astype(f32)
    side_bias = []
    for side in (0, 1):
        apart = jnp.abs(place - place_of_slab(side_sp[side]))
        seen = (reach[0:1, 0:1] >= 1.0) & (reach[0:1, 1:2] >= apart)
        edge = jnp.where(has[side], 0.0, -1e30).astype(f32)
        side_bias.append(jnp.minimum(jnp.where(seen, 0.0, -1e30).astype(f32), edge))
    place_of = lax.broadcasted_iota(jnp.int32, (text, 1), 0)
    words = jnp.where(place_of < live_ref[0], 0.0, -1e30).astype(f32)
    bias_ref, st_near = r_["bias"], r_["st_near"]
    bias_ref[:tok] = jnp.zeros((tok, 1), f32)
    bias_ref[tok:near] = words
    for side in (0, 1):
        region = slice(near + side * tok, near + (side + 1) * tok)
        bias_ref[region] = jnp.broadcast_to(side_bias[side], (tok, 1))

    def cols(h):
        return slice(h * HD, (h + 1) * HD)

    def near_scores(h):
        c = cols(h)
        scores = factor * mm(keys[:near, c], q_ref[:, c], NT) + bias_ref[:near]
        top = jnp.max(scores, axis=0, keepdims=True)
        e = jnp.exp(scores - top)
        wts[h, :near, :] = e
        st_near[h : h + 1, :] = top
        st_near[heads + h : heads + h + 1, :] = jnp.sum(e, axis=0, keepdims=True)

    def forward(h):
        c = cols(h)
        scores = factor * mm(keys[near:, c], q_ref[:, c], NT) + bias_ref[near:]
        top_near = st_near[h : h + 1, :]
        top = jnp.maximum(top_near, jnp.max(scores, axis=0, keepdims=True))
        e = jnp.exp(scores - top)
        fix = jnp.exp(top_near - top)
        total = jnp.sum(e, axis=0, keepdims=True) + fix * st_near[heads + h : heads + h + 1, :]
        inv = 1.0 / total
        w_near = wts[h, :near, :] * (fix * inv)
        w_far = e * inv
        wts[h, :near, :] = w_near
        wts[h, near:, :] = w_far
        att = mm(vals[:near, c], w_near.astype(bf16), TN) + mm(vals[near:, c], w_far.astype(bf16), TN)
        att_t[c, :] = att.astype(bf16)
        for side in (0, 1):
            st_out[side, h : h + 1, :] = top - side_bias[side]
            st_out[side, heads + h : heads + h + 1, :] = inv

    def far_weights(side, h):
        c = cols(h)
        scores = factor * mm(keys[:tok, c], qf[side, :, c], NT)
        e = jnp.exp(scores - st_in[side, h : h + 1, :])
        wfar[side, h] = e * st_in[side, heads + h : heads + h + 1, :]

    def own_slot(r):
        return 2 * (blk(r) >> 2) + (blk(r) & 1)

    def core_owns(r):
        return ((blk(r) >> 1) & 1) == core

    def mine(r):
        return (blk(r) >> 1) == me_dp

    def s1_copy(r):
        return remote(
            g1_out.at[r], g1_in.at[r], r_["s1s"].at[0], r_["s1r"].at[own_slot(r)], {"dp": me_dp ^ 1}
        )

    def x_first(r):
        return r in (2, 6)

    def along_x(j):
        return {"sp": me_sp ^ j}

    def along_y(j):
        return {"dp": me_dp ^ (2 * (j & 1)), "sp": me_sp ^ (2 * (j & 2))}

    def place1(r):
        return x if x_first(r) else y

    def place2(r):
        return y if x_first(r) else x

    def gy_copy(r, j):
        where = along_x(j) if x_first(r) else along_y(j)
        return remote(
            gy_out.at[r, place1(r) ^ j],
            gy_in.at[r, j - 1],
            r_["gys"].at[0],
            r_["gyr"].at[own_slot(r)],
            where,
        )

    def gx_copy(r, j):
        where = along_y(j) if x_first(r) else along_x(j)
        return remote(
            gx_out.at[r, place2(r) ^ j],
            gx_in.at[r, j - 1],
            r_["gxs"].at[0],
            r_["gxr"].at[own_slot(r)],
            where,
        )

    def ag1_copy(r, j):
        piece_ = gall.at[r, x]
        return remote(piece_, piece_, r_["ag1s"].at[0], r_["ag1r"].at[own_slot(r)], along_x(j))

    def ag2_copy(r, i):
        return remote(
            gall.at[r],
            gfin.at[blk(r) & 1, y],
            r_["ag2s"].at[0],
            r_["ag2r"].at[blk(r) & 1],
            {"dp": blk(r) >> 1, "sp": 4 * i + x},
        )

    def ag2_sends(r, i):
        return core_owns(r) & jnp.logical_not(mine(r) & (yh == i))

    def all_of(some, send, recv):
        return remote(some, some, send, recv, {"sp": me_sp ^ 4})

    def gw_part(r):
        parts[r] = mm(att_t[...], nat[r], NN)

        @pl.when(jnp.logical_not(core_owns(r)))
        def _():
            g1_out[r] = parts[r].astype(bf16)
            s1_copy(r).start()

    def gw_s1(r):
        @pl.when(core_owns(r))
        def _():
            s1_copy(r).wait_recv()
            for i in range(4):
                for k in range(4):
                    rows = slice((4 * i + k) * piece, (4 * i + k + 1) * piece)
                    total = parts[r, rows, :] + g1_in[r, rows, :].astype(f32)
                    parts[r, rows, :] = total
                    gy_out[r, i, k] = total.astype(bf16)
            for j in range(1, 4):
                gy_copy(r, j).start()

    def gw_sy(r):
        @pl.when(core_owns(r))
        def _():
            all_of(gy_in.at[r], r_["gys"].at[0], r_["gyr"].at[own_slot(r)]).wait_recv()
            for k in range(4):
                at = pl.multiple_of(place1(r) * (4 * piece) + k * piece, 8)
                total = parts[r, pl.ds(at, piece), :]
                for j in range(3):
                    total = total + gy_in[r, j, k].astype(f32)
                parts[r, k * piece : (k + 1) * piece, :] = total
                gx_out[r, k] = total.astype(bf16)
            for j in range(1, 4):
                gx_copy(r, j).start()

    def gw_sx(r):
        @pl.when(core_owns(r))
        def _():
            all_of(gx_in.at[r], r_["gxs"].at[0], r_["gxr"].at[own_slot(r)]).wait_recv()
            total = parts[r, pl.ds(pl.multiple_of(place2(r) * piece, 8), piece), :]
            for j in range(3):
                total = total + gx_in[r, j].astype(f32)
            gall[r, x] = total.astype(bf16)
            for j in range(1, 4):
                ag1_copy(r, j).start()

    def gw_ag(r):
        @pl.when(core_owns(r))
        def _():
            all_of(gx_in.at[0], r_["ag1s"].at[0], r_["ag1r"].at[own_slot(r)]).wait_recv()

        for i in (0, 1):

            @pl.when(ag2_sends(r, i))
            def _():
                ag2_copy(r, i).start()

        @pl.when(mine(r))
        def _():
            gfin[blk(r) & 1, y] = gall[r]

    gw_v = r_["gw_v"]

    def gw_end(r):
        @pl.when(mine(r))
        def _():
            all_of(gy_in.at[0], r_["ag2s"].at[0], r_["ag2r"].at[blk(r) & 1]).wait_recv()
            at = pl.ds(pl.multiple_of((blk(r) & 1) * w, HD), w)
            for i in range(4):
                for k in range(4):
                    n = 4 * k + i if x_first(r) else 4 * i + k
                    rows = slice(n * piece, (n + 1) * piece)
                    gw_v[rows, at] = gfin[blk(r) & 1, i, k].astype(f32)

    trow = text // n_sp

    def tx_copy(j):
        return remote(
            tx_out.at[x ^ j], tx_in.at[j - 1], r_["txs"].at[0], r_["txr"].at[0], along_x(j)
        )

    def ty_copy():
        return remote(ty_out, ty_in, r_["tys"].at[0], r_["tyr"].at[0], {"sp": me_sp ^ 4})

    def tg_copy():
        slot = tg.at[x, yh]
        return remote(slot, slot, r_["tgs"].at[0], r_["tgr"].at[0], {"sp": me_sp ^ 4})

    def tz_copy(i, j):
        slot = tg.at[x, i]
        return remote(slot, slot, r_["tzs"].at[0], r_["tzr"].at[0], along_x(j))

    def text_1():
        all_of(tx_in, r_["txs"].at[0], r_["txr"].at[0]).wait_recv()

        def over_x(i):
            total = tx_out[x, i].astype(f32)
            for j in range(3):
                total = total + tx_in[j, i].astype(f32)
            return total

        ty_out[...] = over_x(1 - yh).astype(bf16)
        ty_copy().start()
        t_own[...] = over_x(yh)

    def text_2():
        ty_copy().wait_recv()
        tg[x, yh] = (t_own[...] + ty_in[...].astype(f32)).astype(bf16)
        tg_copy().start()
        for j in range(1, 4):
            tz_copy(yh, j).start()

    def text_3():
        tg_copy().wait_recv()
        for j in range(1, 4):
            tz_copy(1 - yh, j).start()

    def text_4():
        all_of(tx_in, r_["tzs"].at[0], r_["tzr"].at[0]).wait_recv()
        for i in range(4):
            for k in range(2):
                rows = slice((2 * i + k) * trow, (2 * i + k + 1) * trow)
                gtk_v[rows] = tg[i, k, :trow]
                gtv_v[rows] = tg[i, k, trow:]

    gq_v, gk_v, gv_v, gtk_v, gtv_v = (r_[n] for n in ("gq_v", "gk_v", "gv_v", "gtk_v", "gtv_v"))

    def text_part(h):
        c = cols(h)
        ga = ga_t[c, :]
        wt = wts[h, tok:near, :]
        gp = mm(vals[tok:near, c], ga, NN)
        gs = (wt * (gp - dl_out[h : h + 1, :])).astype(bf16)
        gs_buf[h, tok:near, :] = gs
        gk = (factor * mm(gs, q_ref[:, c], NN)).astype(bf16)
        gv = mm(wt.astype(bf16), ga, NT).astype(bf16)
        for j in range(n_sp):
            rows = slice(j * trow, (j + 1) * trow)
            tx_out[j // 2, j % 2, :trow, c] = gk[rows]
            tx_out[j // 2, j % 2, trow:, c] = gv[rows]

    def own_part(h):
        c = cols(h)
        ga = ga_t[c, :]
        delta = dl_out[h : h + 1, :]
        for lo, hi in ((0, tok), (near, near + 2 * tok)):
            gp = mm(vals[lo:hi, c], ga, NN)
            gs_buf[h, lo:hi, :] = (wts[h, lo:hi, :] * (gp - delta)).astype(bf16)
        gq_v[:, c] = (factor * mm(keys[:, c], gs_buf[h], TN)).T.astype(bf16)
        gk_sum[:, c] = mm(gs_buf[h, :tok, :], q_ref[:, c], NN)
        gv_sum[:, c] = mm(wts[h, :tok, :].astype(bf16), ga, NT)

    def far_part(side, h):
        c = cols(h)
        ga = gaf[side, c, :]
        weights = wfar[side, h]
        gp = mm(vals[:tok, c], ga, NN)
        gs = (weights * (gp - dl_in[side, h : h + 1, :])).astype(bf16)
        gk_sum[:, c] += mm(gs, qf[side, :, c], NN)
        gv_sum[:, c] += mm(weights.astype(bf16), ga, NT)

    scale(0)
    for h in range(heads):
        near_scores(h)
    z_arrive(0, 0)
    z_arrive(0, 1)
    scale(1)
    scale(7)
    halo_wait_both(("kv", 0))
    forward(0)
    z_arrive(1, 0)
    halo_wait_both(("kv", 1))
    forward(1)
    z_arrive(1, 1)
    scale(2)
    scale(6)
    w_core().wait_recv()
    w_y_all(1).wait_recv()
    w_fwd().start()
    halo_wait_both(("kv", 2))
    forward(2)
    halo_start([4 * heads])
    for r in (0, 1, 7):
        gw_part(r)
    z_arrive(2, 0)
    for r in (2, 6):
        gw_part(r)
    for r in (0, 1, 7):
        gw_s1(r)
    w_fwd().wait_recv()
    ga_add(0, True)
    ga_add(1)
    for r in (2, 6):
        gw_s1(r)
    ga_add(7)
    ga_add(2)
    z_arrive(2, 1)
    scale(3)
    scale(5)
    for r in (3, 5):
        gw_part(r)
    ga_add(6)
    ga_add(3)
    ga_add(5)
    z_arrive(3, 0)
    scale(4)
    gw_part(4)
    for r in (3, 5):
        gw_s1(r)
    ga_add(4)
    ga_t[...] = acc[...].astype(bf16)
    for h in range(heads):
        c = cols(h)
        dl_out[h : h + 1, :] = jnp.sum(
            ga_t[c, :].astype(f32) * att_t[c, :].astype(f32), axis=0, keepdims=True
        )
    gw_s1(4)
    for h in range(heads):
        text_part(h)
    for r in (0, 1, 7):
        gw_sy(r)
    def far_head(h):
        halo_wait_both(("ga", h))
        for side in (0, 1):
            pl.when(has[side])(functools.partial(far_part, side, h))
        c = cols(h)
        gk_v[:, c] = (factor * gk_sum[:, c]).astype(bf16)
        gv_v[:, c] = gv_sum[:, c].astype(bf16)

    for j in range(1, 4):
        tx_copy(j).start()
    for r in (2, 6):
        gw_sy(r)
    own_part(0)
    own_part(1)
    for r in (3, 5):
        gw_sy(r)
    for r in (0, 1, 7):
        gw_sx(r)
    halo_start([4 * heads + 1, 3 * heads])
    gw_sy(4)
    own_part(2)
    halo_start([3 * heads + 1])
    for r in (2, 6):
        gw_sx(r)
    text_1()
    halo_wait_both(("st", 0), ("q", 0))
    for h in range(heads):
        for side in (0, 1):
            pl.when(has[side])(functools.partial(far_weights, side, h))
    for r in (3, 5):
        gw_sx(r)
    gw_sx(4)
    halo_start([3 * heads + 2])
    text_2()
    for r in (0, 1, 7):
        gw_ag(r)
    for r in (2, 6):
        gw_ag(r)
    halo_wait_both(("dl", 0))
    far_head(0)
    for r in (3, 5):
        gw_ag(r)
    gw_ag(4)
    text_3()
    far_head(1)
    far_head(2)
    text_4()
    for r in (0, 1, 7, 2, 6, 3, 5, 4):
        gw_end(r)

    all_of(raw.at[pl.ds(0, n_tp - 1)], r_["zs"].at[0], r_["zr"].at[0, 0, 0]).wait_send()
    w_core().wait_send()

    @pl.when(jnp.logical_not(ends))
    def _():
        w_y_all(1).wait_send()

    @pl.when(ends & gives)
    def _():
        w_y_all(2).wait_send()

    w_fwd().wait_send()
    for side in (0, 1):

        @pl.when(has[side])
        def _():
            blocks = raw.at[pl.ds(0, 4)]
            remote(
                blocks, blocks, r_["hs"].at[side, 0], r_["hr"].at[side, 0], {"sp": side_sp[side]}
            ).wait_send()
            halo(side, 4 * heads).wait_send()
            halo(side, 4 * heads + 1).wait_send()

    for some, n in (
        (g1_out.at[pl.ds(0, 4)], "s1"),
        (gy_in.at[pl.ds(0, 4)], "gy"),
        (gx_in.at[pl.ds(0, 4)], "gx"),
        (gx_in.at[pl.ds(0, 4)], "ag1"),
        (gy_in.at[pl.ds(0, 2)], "ag2"),
        (tx_in, "tx"),
        (ty_out, "ty"),
        (ty_out, "tg"),
        (tx_in, "tz"),
    ):
        all_of(some, r_[n + "s"].at[0], r_[n + "r"].at[0]).wait_send()


def call(q, k, v, tk, tv, s, w, gate, windows, tile_map, text_count):
    tok, width = q.shape
    text = tk.shape[0]
    heads = width // HD
    cols = w.shape[1]
    hbm = pl.BlockSpec(memory_space=pltpu.HBM)
    total = 3 * tok + text
    block = s.shape[1]
    piece = width // 16
    sm = pl.BlockSpec(memory_space=pltpu.SMEM)
    vm = pl.BlockSpec(memory_space=pltpu.VMEM)
    outs = [
        ("gq", (tok, width), bf16),
        ("gk", (tok, width), bf16),
        ("gv", (tok, width), bf16),
        ("gtk", (text, width), bf16),
        ("gtv", (text, width), bf16),
        ("gw", (width, cols), f32),
    ]
    scratch = [
        ("q_v", (tok, width), bf16),
        ("s_v", (tok, block), bf16),
        ("keys", (total, width), bf16),
        ("vals", (total, width), bf16),
        ("qf", (2, tok, width), bf16),
        ("gaf", (2, width, tok), bf16),
        ("st_out", (2, 8, tok), f32),
        ("st_in", (2, 8, tok), f32),
        ("dl_out", (8, tok), f32),
        ("dl_in", (2, 8, tok), f32),
        ("bias", (total, 1), f32),
        ("st_near", (8, tok), f32),
        ("raw", (8, tok, block), bf16),
        ("nat", (8, tok, block), bf16),
        ("w_all", (4, width, cols), bf16),
        ("acc", (width, tok), f32),
        ("ga_t", (width, tok), bf16),
        ("att_t", (width, tok), bf16),
        ("wts", (heads, total, tok), f32),
        ("wfar", (2, heads, tok, tok), f32),
        ("gs_buf", (heads, total, tok), bf16),
        ("gk_sum", (tok, width), f32),
        ("gv_sum", (tok, width), f32),
        ("parts", (8, width, block), f32),
        ("g1_out", (8, width, block), bf16),
        ("g1_in", (8, width, block), bf16),
        ("gy_out", (8, 4, 4, piece, block), bf16),
        ("gy_in", (8, 3, 4, piece, block), bf16),
        ("gx_out", (8, 4, piece, block), bf16),
        ("gx_in", (8, 3, piece, block), bf16),
        ("gall", (8, 4, piece, block), bf16),
        ("gfin", (2, 4, 4, piece, block), bf16),
        ("tx_out", (4, 2, text // 4, width), bf16),
        ("tx_in", (3, 2, text // 4, width), bf16),
        ("ty_out", (text // 4, width), bf16),
        ("ty_in", (text // 4, width), bf16),
        ("t_own", (text // 4, width), f32),
        ("tg", (4, 2, text // 4, width), bf16),
    ]
    sems = [
        ("zs", (1,)),
        ("zr", (2, 4, 2)),
        ("ws", (3,)),
        ("wr", (3,)),
        ("hs", (2, 3)),
        ("hr", (2, 2 * heads + 3)),
        ("s1s", (1,)),
        ("s1r", (4,)),
        ("gys", (1,)),
        ("gyr", (4,)),
        ("gxs", (1,)),
        ("gxr", (4,)),
        ("ag1s", (1,)),
        ("ag1r", (4,)),
        ("ag2s", (1,)),
        ("ag2r", (2,)),
        ("txs", (1,)),
        ("txr", (1,)),
        ("tys", (1,)),
        ("tyr", (1,)),
        ("tzs", (1,)),
        ("tzr", (1,)),
        ("tgs", (1,)),
        ("tgr", (1,)),
        ("ls", (7,)),
    ]
    args = ["q", "k", "v", "tk", "tv", "s", "w", "gate", "win", "map", "live"]
    names = args + [n + "_v" for n, _, _ in outs] + [n for n, _, _ in scratch]
    names += [n for n, _ in sems]
    return pl.pallas_call(
        functools.partial(kernel, tuple(names)),
        out_shape=[pltpu.VMEM(a, b) for _, a, b in outs],
        in_specs=[hbm] * 7 + [vm] * 3 + [sm],
        out_specs=[vm] * len(outs),
        scratch_shapes=[pltpu.VMEM(a, b) for _, a, b in scratch]
        + [pltpu.SemaphoreType.DMA(n) for _, n in sems],
        compiler_params=pltpu.CompilerParams(
            collective_id=0, has_side_effects=True, vmem_limit_bytes=56 << 20
        ),
        name="attention_backward",
    )(q, k, v, tk, tv, s, w, gate, windows, tile_map, text_count)


def copy_kernel(n, *refs):
    srcs, dsts, sem = refs[:n], refs[n : 2 * n], refs[2 * n]
    stores = [pltpu.make_async_copy(srcs[i], dsts[i], sem.at[i]) for i in range(n)]
    for c in stores:
        c.start()
    for c in stores:
        c.wait()


def copy_call(arrays):
    n = len(arrays)
    return pl.pallas_call(
        functools.partial(copy_kernel, n),
        out_shape=[jax.ShapeDtypeStruct(a.shape, a.dtype) for a in arrays],
        in_specs=[pl.BlockSpec(memory_space=pltpu.VMEM)] * n,
        out_specs=[pl.BlockSpec(memory_space=pltpu.HBM)] * n,
        scratch_shapes=[pltpu.SemaphoreType.DMA((n,))],
        compiler_params=pltpu.CompilerParams(vmem_limit_bytes=4 << 20),
        name="results",
    )(*arrays)


def per_device(
    query,
    key,
    value,
    text_key,
    text_value,
    grad_out,
    gate,
    out_weight,
    windows,
    tile_map,
    text_count,
):
    outs = call(
        query[0],
        key[0],
        value[0],
        text_key[0],
        text_value[0],
        grad_out[0],
        out_weight,
        gate,
        windows,
        tile_map.T,
        text_count,
    )
    outs = copy_call(outs)
    return tuple(o[None] for o in outs[:5]) + (outs[5],)


def solution(mesh):
    placed = (
        P("dp", "sp", "tp"),
        P("dp", "sp", "tp"),
        P("dp", "sp", "tp"),
        P("dp", None, "tp"),
        P("dp", None, "tp"),
        P("dp", "sp", "tp"),
        P("dp", None),
        P("tp", "dp"),
        P("sp", None),
        P(),
        P("dp"),
    )
    return jax.shard_map(
        per_device,
        mesh=mesh,
        in_specs=placed,
        out_specs=(
            P("dp", "sp", "tp"),
            P("dp", "sp", "tp"),
            P("dp", "sp", "tp"),
            P("dp", None, "tp"),
            P("dp", None, "tp"),
            P("tp", "dp"),
        ),
        check_vma=False,
    )
```
